128 devices in a mesh: seq: 16 (over z, x), tp: 8 (over y, core).
Axes of the slice: x: 4, y: 4, z: 4, core: 2. Of those that a mesh axis runs over, the one named last changes fastest.
Arguments:
- inner_x: bfloat16 [8192, 5120], P('seq', 'tp'), may hold values from -6 to 6
- gate_z: bfloat16 [8192, 5120], P('seq', 'tp'), may hold values from -6 to 6
- proj_bc: bfloat16 [8192, 256], P('seq'), may hold values from -6 to 6
- dt_raw: bfloat16 [8192, 80], P('seq', 'tp'), may hold values from -6 to 10
- a_log: float32 [80], P('tp'), may hold values from -12 to 0
- dt_bias: float32 [80], P('tp'), may hold values from -4 to -2
- d_skip: float32 [80], P('tp'), may hold values from 0.5 to 1.5
- conv_x: float32 [4, 5120], P(None, 'tp'), may hold values from -3 to 3
- bias_x: float32 [5120], P('tp'), may hold values from -3 to 3
- conv_bc: float32 [4, 256], replicated, may hold values from -3 to 3
- bias_bc: float32 [256], replicated, may hold values from -3 to 3
- norm_gain: float32 [5120], P('tp'), may hold values from 0.5 to 1.5
- w_out: bfloat16 [5120, 2560], P('tp', 'seq'), may hold values from -0.078125 to 0.078125
- d_out: bfloat16 [8192, 2560], P('seq', 'tp'), may hold values from -6 to 6
Outputs:
- output: bfloat16 [8192, 2560], P('seq', 'tp')
- grad_x: float32 [8192, 5120], P('seq', 'tp')
- grad_z: float32 [8192, 5120], P('seq', 'tp')
- grad_bc: float32 [8192, 256], P('seq')
- grad_dt: float32 [8192, 80], P('seq', 'tp')
- grad_w: float32 [5120, 2560], P('tp', 'seq')
The draws below stay inside these ranges and needn't reach their ends.
All inputs are finite; a program needn't handle non-finite values.
Results may differ from the reference program's by a relative error of at most 0.013.
Values may be sent and summed in bfloat16 or wider, within the bound.
A program may use at most 192 MiB of HBM per device.

```python
import jax
import jax.numpy as jnp
from jax import lax

D = 2560
HEADS = 80
STATE = 128
KERNEL = 4
BLOCK = 256
INNER = 5120
STREAM_LENGTH = 8192
N_TP = 8


def draw_a_log(key, part):
    key_order, key_slow, key_fast = jax.random.split(jax.random.fold_in(key, 11), 3)
    ranking = jax.random.permutation(key_order, HEADS)
    keeping = ranking >= HEADS // 2
    slow_log = jnp.log(2.0 / STREAM_LENGTH) + jax.random.uniform(key_slow, (HEADS,), jnp.float32) * jnp.log(10.0)
    fast_log = jnp.log(0.3) + jax.random.uniform(key_fast, (HEADS,), jnp.float32) * jnp.log(3.0)
    return jnp.where(keeping, slow_log, fast_log).astype(jnp.float32)


def draw_dt_raw(key, part):
    key_ground, key_spots, key_raise = jax.random.split(jax.random.fold_in(key, 23), 3)
    expected_answer = jnp.clip(jax.random.normal(key_ground, (STREAM_LENGTH, HEADS), jnp.float32), -6.0, 6.0)
    marker_indices = jax.random.randint(key_spots, (8,), 0, STREAM_LENGTH)
    cluster_batches = jnp.any(jnp.arange(STREAM_LENGTH)[:, None] == marker_indices[None, :], axis=1)
    elevated_entries = jax.random.uniform(key_raise, (HEADS,), jnp.float32, 2.0, 4.0)
    return (expected_answer + jnp.where(cluster_batches[:, None], elevated_entries[None, :], 0.0)).astype(jnp.bfloat16)


def strengthened(values, own_key, source, target, blocks, factor):
    owner, partner = [(jnp.arange(values.shape[axis_at]) // (values.shape[axis_at] // blocks)).reshape([-1 if axis == axis_at else 1 for axis in range(values.ndim)]) for axis_at in (source, target)]
    chosen = jax.random.permutation(own_key, blocks)[partner]
    strong = (owner == chosen) | (owner == (partner + blocks // 2) % blocks)
    return jnp.where(strong, factor * values, values)


def shard_levels(stream_key, shape, cuts, least, largest):
    def one(position, shards_of):
        heights = jax.random.uniform(jax.random.fold_in(jax.random.fold_in(stream_key, 6), position), (shards_of,), jnp.float32, least / len(cuts), largest / len(cuts))
        return jnp.repeat(jnp.exp(heights), shape[position] // shards_of).reshape((-1,) + (1,) * (len(shape) - position - 1))

    loudness = one(*cuts[0])
    for cut in cuts[1:]:
        loudness = loudness * one(*cut)
    return loudness


def normal_values(key, extent, deviation, bound, cuts=(), kind=jnp.bfloat16):
    array = jax.random.normal(key, extent, jnp.float32) * deviation
    if len(cuts) > 0:
        array = shard_levels(key, extent, cuts, -0.22, 0.18) * array
    return jnp.clip(array, min=-bound, max=bound).astype(kind)


def heavy_noise(stream_key, dims, scale, most, cuts, heavy, kind=jnp.bfloat16):
    result = scale * jax.random.normal(stream_key, dims, jnp.float32)
    if cuts:
        result = result * shard_levels(stream_key, dims, cuts, -0.22, 0.18)
    return jnp.clip(strengthened(result, jax.random.fold_in(stream_key, 3), *heavy), -most, most).astype(kind)


def setup_inputs(seed: int = 0) -> dict:
    key_of = jax.random.split(jax.random.key(seed), 15)
    return {
        "inner_x": normal_values(key_of[0], (STREAM_LENGTH, INNER), 1.0, 6.0, ((0, 16), (1, 8))),
        "gate_z": normal_values(key_of[1], (STREAM_LENGTH, INNER), 1.0, 6.0, ((0, 16), (1, 8))),
        "proj_bc": normal_values(key_of[2], (STREAM_LENGTH, 2 * STATE), 1.0, 6.0, ((0, 16),)),
        "dt_raw": draw_dt_raw(jax.random.fold_in(key_of[14], 71), 0),
        "a_log": draw_a_log(jax.random.fold_in(key_of[14], 71), 0),
        "dt_bias": jnp.clip(-4.0 + 2.0 * jax.random.uniform(key_of[5], (HEADS,), jnp.float32) ** shard_levels(key_of[5], (HEADS,), ((0, 8),), -0.2, 0.2), -4.0, -2.0),
        "d_skip": jnp.clip(0.5 + 1.0 * jax.random.uniform(key_of[6], (HEADS,), jnp.float32) ** shard_levels(key_of[6], (HEADS,), ((0, 8),), -0.2, 0.2), 0.5, 1.5),
        "conv_x": normal_values(key_of[7], (KERNEL, INNER), KERNEL ** -0.5, 3.0, ((1, 8),), jnp.float32),
        "bias_x": normal_values(key_of[8], (INNER,), 0.5, 3.0, ((0, 8),), jnp.float32),
        "conv_bc": normal_values(key_of[9], (KERNEL, 2 * STATE), KERNEL ** -0.5, 3.0, (), jnp.float32),
        "bias_bc": normal_values(key_of[10], (2 * STATE,), 0.5, 3.0, (), jnp.float32),
        "norm_gain": jnp.clip(1.0 + 0.1 * jax.random.normal(key_of[11], (INNER,), jnp.float32), 0.5, 1.5),
        "w_out": normal_values(key_of[12], (INNER, D), INNER ** -0.5, 0.078125, ((0, 8), (1, 16))),
        "d_out": heavy_noise(key_of[13], (STREAM_LENGTH, D), 1.0, 6.0, ((0, 16), (1, 8)), (0, 1, 16, 2.0)),
    }


HIGH = lax.Precision.HIGHEST
EPSILON = 1e-05

def causal_conv(padded, weights, biases):
    kernel_taps = weights.shape[0]
    out_rows = padded.shape[0] - kernel_taps + 1
    summed = jnp.zeros((out_rows, padded.shape[1]), jnp.float32) + biases[None, :]
    for offset in range(kernel_taps):
        summed = summed + weights[offset][None, :] * padded[offset:offset + out_rows]
    return jax.nn.silu(summed)

def ssd_local(values, projected, raw_steps, a_log, dt_bias, d_skip, block, saving):
    row_count, channels = values.shape
    head_count = a_log.shape[0]
    head_size = channels // head_count
    state_size = projected.shape[1] // 2
    step_sizes = jax.nn.softplus(raw_steps + dt_bias[None, :])
    decay_logarithm = -step_sizes * jnp.exp(a_log)[None, :]
    shaped = values.reshape(row_count, head_count, head_size)
    scaled = shaped * step_sizes[:, :, None]
    block_count = row_count // block
    causal_mask = (jnp.arange(block)[:, None] >= jnp.arange(block)[None, :])[:, :, None]

    def one_block(carried_state, pieces):
        own_values, own_scaled, own_decay, own_proj = pieces
        input_map = own_proj[:, :state_size]
        output_map = own_proj[:, state_size:]
        running = jnp.cumsum(own_decay, axis=0)
        scores = jnp.dot(output_map, input_map.T, precision=HIGH)
        spread = running[:, None, :] - running[None, :, :]
        weights = jnp.exp(jnp.where(causal_mask, spread, -jnp.inf)) * scores[:, :, None]
        within = jnp.einsum('tsh,shp->thp', weights, own_scaled, precision=HIGH)
        reads = jnp.einsum('tn,hpn->thp', output_map, carried_state, precision=HIGH)
        from_state = jnp.exp(running)[:, :, None] * reads
        to_end = jnp.exp(running[-1][None, :] - running)
        fresh = jnp.einsum('shp,sn->hpn', to_end[:, :, None] * own_scaled, input_map, precision=HIGH)
        next_state = jnp.exp(running[-1])[:, None, None] * carried_state + fresh
        block_out = within + from_state + d_skip[None, :, None] * own_values
        return (next_state, block_out)
    step_fn = jax.checkpoint(one_block) if saving else one_block
    pieces = (shaped.reshape(block_count, block, head_count, head_size), scaled.reshape(block_count, block, head_count, head_size), decay_logarithm.reshape(block_count, block, head_count), projected.reshape(block_count, block, 2 * state_size))
    initial = jnp.zeros((head_count, head_size, state_size), jnp.float32)
    final_state, outputs = lax.scan(step_fn, initial, pieces)
    return (outputs.reshape(row_count, channels), final_state, lax.optimization_barrier(jnp.sum(decay_logarithm, axis=0)))

def reference(inner_x, gate_z, proj_bc, dt_raw, a_log, dt_bias, d_skip, conv_x, bias_x, conv_bc, bias_bc, norm_gain, w_out, d_out):
    kernel_taps = conv_x.shape[0]

    def region(values, projected, raw_steps):
        pad_values = jnp.concatenate([jnp.zeros((kernel_taps - 1, values.shape[1]), jnp.float32), values], 0)
        pad_proj = jnp.concatenate([jnp.zeros((kernel_taps - 1, projected.shape[1]), jnp.float32), projected], 0)
        conv_values = causal_conv(pad_values, conv_x, bias_x)
        conv_proj = causal_conv(pad_proj, conv_bc, bias_bc)
        mixed_out, final_state, decay_total = ssd_local(conv_values, conv_proj, raw_steps, a_log, dt_bias, d_skip, BLOCK, True)
        return mixed_out
    mixed_out, region_pull = jax.vjp(region, inner_x.astype(jnp.float32), proj_bc.astype(jnp.float32), dt_raw.astype(jnp.float32))
    gate_value = gate_z.astype(jnp.float32)
    gate_sigma = jax.nn.sigmoid(gate_value)
    gate_silu = jax.nn.silu(gate_value)
    gated_out = mixed_out * gate_silu
    inv_rms = lax.rsqrt(lax.optimization_barrier(jnp.sum(gated_out * gated_out, axis=1)) / INNER + EPSILON)
    normed = (gated_out * inv_rms[:, None] * norm_gain[None, :]).astype(jnp.bfloat16)
    group_size = INNER // N_TP

    def add_group(running_sum, group_index):
        normed_part = lax.dynamic_slice_in_dim(normed, group_index * group_size, group_size, 1)
        weight_part = lax.dynamic_slice_in_dim(w_out, group_index * group_size, group_size, 0)
        term = jnp.dot(normed_part, weight_part, preferred_element_type=jnp.float32)
        quantized_copy = lax.optimization_barrier(term.astype(jnp.bfloat16))
        return (running_sum + quantized_copy.astype(jnp.float32), None)
    summed, discarded_item = lax.scan(add_group, jnp.zeros((STREAM_LENGTH, D), jnp.float32), jnp.arange(N_TP, dtype=jnp.int32))
    output = summed.astype(jnp.bfloat16)
    grad_normed = lax.dot_general(d_out, w_out, (((1,), (1,)), ((), ())), preferred_element_type=jnp.float32)
    grad_w = lax.dot_general(normed, d_out, (((0,), (0,)), ((), ())), preferred_element_type=jnp.float32)
    scaled_grad = grad_normed * norm_gain[None, :]
    inner_sum = lax.optimization_barrier(jnp.sum(scaled_grad * gated_out, axis=1))
    grad_gated = inv_rms[:, None] * scaled_grad - gated_out * (inv_rms ** 3 * inner_sum / INNER)[:, None]
    grad_z = grad_gated * mixed_out * gate_sigma * (1.0 + gate_value * (1.0 - gate_sigma))
    grad_mixed = grad_gated * gate_silu
    grad_values, grad_proj, grad_steps = region_pull(grad_mixed)
    return (output, grad_values, grad_z, grad_proj, grad_steps, grad_w)
```

```python
import functools

import jax
import jax.numpy as jnp
from jax import lax
from jax.experimental import pallas as pl
from jax.experimental.pallas import tpu as pltpu
from jax.sharding import PartitionSpec as P

MESH = pl.DeviceIdType.MESH
F32 = jnp.float32
BF16 = jnp.bfloat16
HIGH = lax.Precision.HIGHEST
EPSILON = 1e-05
NN = ((1,), (0,))
NT = ((1,), (1,))
Q = 128
PAIR = 128
HEAD = 64
LANES = 128


def mm(a, b, dims=NN):
    return lax.dot_general(a.astype(BF16), b.astype(BF16), (dims, ((), ())), preferred_element_type=F32)


def mmh(a, b, dims=NN):
    return lax.dot_general(
        a.astype(F32), b.astype(F32), (dims, ((), ())), precision=HIGH, preferred_element_type=F32
    )


def halves(v):
    high = v.astype(BF16)
    return high, (v - high.astype(F32)).astype(BF16)


def mm3(a, b, dims=NN):
    a0, a1 = halves(a)
    b0, b1 = halves(b)
    return mm(a0, b0, dims) + (mm(a1, b0, dims) + mm(a0, b1, dims))


def iota(shape, dim):
    return lax.broadcasted_iota(jnp.int32, shape, dim)


def sigmoid(v):
    return 1.0 / (1.0 + jnp.exp(-v))


def softplus(v):
    return jnp.maximum(v, 0.0) + jnp.log1p(jnp.exp(-jnp.abs(v)))


def pair_stack(v):
    lane = iota(v.shape, 1)
    return jnp.concatenate(
        [jnp.where(lane < HEAD, v, 0.0), jnp.where(lane >= HEAD, v, 0.0)], axis=0
    )


def kernel(
    sizes,
    ix,
    gz,
    bc,
    raw,
    wt,
    dt,
    cw,
    bx,
    cwb,
    bb,
    gain,
    al,
    db,
    ds,
    alc,
    dbc,
    o_out,
    o_gx,
    o_gz,
    o_gbc,
    o_gdt,
    o_gw,
    wfull,
    dfull,
    hx,
    hb,
    dsend,
    dbuf,
    st,
    lx,
    lt,
    u,
    x,
    ub,
    bcv,
    fr,
    sst,
    cf,
    y,
    gated,
    gn,
    gm,
    nb,
    dxs,
    dus,
    dub,
    rcur,
    se,
    sr,
    en,
    sin,
    re,
    rr,
    ren,
    rin,
    ts,
    tr,
    pb,
    pr,
    gb,
    gr,
    qs,
    qr,
    qa,
    arow,
    acol,
    dga,
    sm_h,
    sm_d,
    sm_w,
    sm_g,
    sm_s,
    sm_b,
    sm_r,
    sm_q,
    sm_t,
    sm_o,
    sm_v,
    sm_p,
    sm_a,
):
    n_seq, n_tp, inner = sizes
    rows, ch = ix.shape
    nc = rows // Q
    heads = ch // HEAD
    pairs = ch // PAIR
    ns = bc.shape[1] // 2
    me, my = lax.axis_index("seq"), lax.axis_index("tp")
    wrows = wt.shape[0]
    drows = dt.shape[0]
    nrow = ns // n_seq

    scope = []

    def phase(name):
        if scope:
            scope.pop().__exit__(None, None, None)
        if name:
            scope.append(jax.named_scope(name))
            scope[0].__enter__()

    def seq_peer(k):
        return lax.rem(me + k, n_seq)

    def tp_peer(k):
        return lax.rem(my + k, n_tp)

    phase("barrier")
    barrier = pltpu.get_barrier_semaphore()
    for k in range(1, n_seq):
        pl.semaphore_signal(barrier, inc=1, device_id={"seq": seq_peer(k)}, device_id_type=MESH)
    for k in range(1, n_tp):
        pl.semaphore_signal(barrier, inc=1, device_id={"tp": tp_peer(k)}, device_id_type=MESH)
    pl.semaphore_wait(barrier, n_seq + n_tp - 2)

    def remote(src, dst, sems, k, axis, peer):
        return pltpu.make_async_remote_copy(
            src_ref=src,
            dst_ref=dst,
            send_sem=sems.at[0, k],
            recv_sem=sems.at[1, k],
            device_id={axis: peer},
            device_id_type=MESH,
        )

    phase("start")
    nxt, prv = seq_peer(1), seq_peer(n_seq - 1)
    halo_x = remote(ix.at[pl.ds(rows - 16, 16)], hx, sm_h, 0, "seq", nxt)
    halo_b = remote(bc.at[pl.ds(rows - 16, 16)], hb, sm_h, 1, "seq", nxt)
    halo_x.start()
    halo_b.start()

    def w_copy(k):
        return remote(wt, wfull.at[pl.ds(me * wrows, wrows)], sm_w, k, "seq", seq_peer(k))

    def d_copy(k):
        return remote(dt, dfull.at[pl.ds(my * drows, drows)], sm_g, k, "tp", tp_peer(k))

    for k in range(1, n_tp):
        d_copy(k).start()
    own_w = pltpu.make_async_copy(wt, wfull.at[pl.ds(me * wrows, wrows)], sm_w.at[0, 0])
    own_d = pltpu.make_async_copy(dt, dfull.at[pl.ds(my * drows, drows)], sm_g.at[0, 0])
    own_w.start()
    own_d.start()

    phase("steps")
    spread = (iota((LANES, ch), 1) // HEAD == iota((LANES, ch), 0)).astype(F32)
    spread_h = spread[:heads]
    negexp = -jnp.exp(al[...])
    neg_x = mmh(jnp.broadcast_to(negexp, (8, heads)), spread_h)[0:1]
    dtb_x = mmh(jnp.broadcast_to(db[...], (8, heads)), spread_h)[0:1]
    skip_x = mmh(jnp.broadcast_to(ds[...], (8, heads)), spread_h)[0:1]
    tri = (iota((Q, Q), 0) >= iota((Q, Q), 1)).astype(F32)
    tri_u = (iota((Q, Q), 0) <= iota((Q, Q), 1)).astype(F32)
    strict = (iota((Q, Q), 0) > iota((Q, Q), 1)).astype(F32)

    ident = (iota((16, heads), 0) == iota((16, heads), 1)).astype(F32)

    def steps(c, total):
        sl = pl.ds(pl.multiple_of(c * Q, Q), Q)
        r = raw[sl, :]
        s = softplus(mm(r, spread_h) + dtb_x)
        ld = s * neg_x
        cum = mmh(tri, ld)
        st[sl, :] = s
        lx[sl, :] = cum
        s_t = softplus(mm(ident, r, NT) + dbc[...])
        lt[c] = mmh(s_t * -jnp.exp(alc[...]), tri_u)
        return total + cum[Q - 1 : Q, :]

    total = lax.fori_loop(0, nc, steps, jnp.zeros((1, ch), F32))
    pick = (iota((ch, LANES), 0) == iota((ch, LANES), 1) * HEAD).astype(F32)
    dsend[...] = mmh(jnp.broadcast_to(total, (8, ch)), pick)

    def t_copy(k):
        return remote(dsend, dbuf.at[me], sm_d, k, "seq", seq_peer(k))

    dbuf[me] = dsend[...]
    for k in range(1, n_seq):
        t_copy(k).start()

    phase("wait_halo")
    halo_x.wait_recv()
    halo_b.wait_recv()

    phase("convs")
    def conv_of(ref, halo, weights, bias, c):
        base = pl.multiple_of(c * Q, Q)
        own = ref[pl.ds(base, Q), :].astype(F32)
        before = pl.multiple_of(jnp.maximum(c * Q - 16, 0), 16)
        prev = ref[pl.ds(before, 16), :].astype(F32)
        edge = jnp.where(me > 0, halo[...].astype(F32), 0.0)
        head = jnp.where(c > 0, prev, edge)[8:16]
        ext = jnp.concatenate([head, own], axis=0)
        acc = bias[...] + weights[3:4, :] * own
        for k in range(3):
            acc = acc + weights[k : k + 1, :] * pltpu.roll(ext, Q + 8 - (5 + k), 0)[:Q]
        return acc

    def convs(c, carry):
        sl = pl.ds(pl.multiple_of(c * Q, Q), Q)
        vb = conv_of(bc, hb, cwb, bb, c)
        ub[sl, :] = vb
        pbc = vb * sigmoid(vb)
        bcv[sl, :] = pbc
        vx = conv_of(ix, hx, cw, bx, c)
        u[sl, :] = vx
        xv = vx * sigmoid(vx)
        x[sl, :] = xv
        cum = lx[sl, :]
        to_end = jnp.exp(cum[Q - 1 : Q, :] - cum)
        b_t = jnp.transpose(pbc[:, :ns])
        fresh = mm3(b_t, xv * st[sl, :] * to_end)
        fr[c] = fresh
        return jnp.exp(cum[Q - 1 : Q, :]) * carry + fresh

    end = lax.fori_loop(0, nc, convs, jnp.zeros((ns, ch), F32))
    se[...] = end.reshape(n_seq, nrow, ch)

    phase("send_s")
    def s_copy(k):
        return remote(se.at[seq_peer(k)], sr.at[me], sm_s, k, "seq", seq_peer(k))

    def sb_copy(k):
        return remote(en.at[seq_peer(k)], sin.at[me], sm_b, k, "seq", seq_peer(k))

    for k in range(1, n_seq):
        s_copy(k).start()
    sr[me] = se[me]
    for k in range(1, n_seq):
        w_copy(k).start()

    upper = iota((Q, Q), 0) >= iota((Q, Q), 1)
    lower = iota((Q, Q), 0) <= iota((Q, Q), 1)

    phase("inside")
    def inside(c, carry):
        sl = pl.ds(pl.multiple_of(c * Q, Q), Q)
        scores = mm3(bcv[sl, ns:], bcv[sl, :ns], NT)
        for p in range(pairs):
            ps = slice(p * PAIR, (p + 1) * PAIR)
            both = []
            for h in (2 * p, 2 * p + 1):
                diff = lx[sl, h * HEAD : h * HEAD + 1] - lt[c, h : h + 1, :]
                decay = jnp.exp(jnp.where(upper, diff, -1e30))
                both.append(decay * scores)
            y[sl, ps] = mm3(jnp.concatenate(both, axis=1), pair_stack(x[sl, ps] * st[sl, ps]))
        return carry

    lax.fori_loop(0, nc, inside, 0)

    phase("wait_s")
    for k in range(1, n_seq):
        t_copy(k).wait_recv()
    for k in range(1, n_seq):
        s_copy(k).wait_recv()
    phase("scan")
    spread_d = mmh(dbuf[...].reshape(n_seq * 8, LANES), spread)

    acc = jnp.zeros((nrow, ch), F32)
    for j in range(n_seq):
        en[j] = acc
        acc = jnp.exp(spread_d[8 * j : 8 * j + 1]) * acc + sr[j]
    for k in range(1, n_seq):
        sb_copy(k).start()
    sin[me] = en[me]

    phase("wait_wd")
    own_d.wait()
    for k in range(1, n_tp):
        d_copy(k).wait_recv()
    own_w.wait()
    for k in range(1, n_seq):
        w_copy(k).wait_recv()

    phase("gn")
    width = wrows * n_seq
    kb = 512

    def gn_block(b, carry):
        kk = pl.ds(pl.multiple_of(b * kb, kb), kb)
        part = mm(jnp.transpose(dfull[kk, :]), wfull[kk, :])

        @pl.when(b == 0)
        def _():
            gn[...] = part

        @pl.when(b > 0)
        def _():
            gn[...] += part

        return carry

    lax.fori_loop(0, width // kb, gn_block, 0)

    phase("wait_sb")
    for k in range(1, n_seq):
        sb_copy(k).wait_recv()

    phase("combine")
    lane = iota((Q, LANES), 1)

    def combine(c, state):
        sl = pl.ds(pl.multiple_of(c * Q, Q), Q)
        sst[c] = state
        cum = lx[sl, :]
        mixed = y[sl, :] + jnp.exp(cum) * mm3(bcv[sl, ns:], state) + skip_x * x[sl, :]
        y[sl, :] = mixed
        zv = gz[sl, :].astype(F32)
        gv = mixed * zv * sigmoid(zv)
        gated[sl, :] = gv
        sq = jnp.sum(gv * gv, axis=1, keepdims=True)
        ip = jnp.sum(gn[sl, :] * gain[...] * gv, axis=1, keepdims=True)
        both = jnp.where(lane == 0, sq, jnp.where(lane == 1, ip, 0.0))
        ts[:, pl.ds(pl.multiple_of(c * Q, Q), Q)] = jnp.transpose(both)[:8]
        return jnp.exp(cum[Q - 1 : Q, :]) * state + fr[c]

    lax.fori_loop(0, nc, combine, sin[...].reshape(ns, ch))

    phase("wait_t")
    def r_copy(k):
        return remote(ts, tr.at[my], sm_t, k, "tp", tp_peer(k))

    for k in range(1, n_tp):
        r_copy(k).start()
    tr[my] = ts[...]
    for k in range(1, n_tp):
        r_copy(k).wait_recv()
    phase("norm")
    tsum = tr[0]
    for j in range(1, n_tp):
        tsum = tsum + tr[j]
    gn_pad = jnp.concatenate([tsum, jnp.zeros((Q - 8, rows), F32)], axis=0)
    ts2 = [jnp.transpose(gn_pad[:, c * Q : (c + 1) * Q]) for c in range(nc)]

    for c in range(nc):
        sl = pl.ds(c * Q, Q)
        inv = lax.rsqrt(ts2[c][:, 0:1] / inner + EPSILON)
        coef = inv * inv * inv * ts2[c][:, 1:2] / inner
        gv = gated[sl, :]
        nb[sl, :] = (gv * inv * gain[...]).astype(BF16)
        gg = inv * (gn[sl, :] * gain[...]) - gv * coef
        zv = gz[sl, :].astype(F32)
        sg = sigmoid(zv)
        o_gz[sl, :] = gg * y[sl, :] * sg * (1.0 + zv * (1.0 - sg))
        gmv = gg * zv * sg
        gm[sl, :] = gmv
        c_t = jnp.transpose(bcv[sl, ns:])
        cf[c] = mm3(c_t, gmv * jnp.exp(lx[sl, :]))

    racc = cf[nc - 1]
    for c in reversed(range(nc - 1)):
        racc = cf[c] + jnp.exp(lx[pl.ds(c * Q + Q - 1, 1), :]) * racc
    re[...] = racc.reshape(n_seq, nrow, ch)

    phase("send_v")
    def v_copy(k):
        return remote(re.at[seq_peer(k)], rr.at[me], sm_r, k, "seq", seq_peer(k))

    def vb_copy(k):
        return remote(ren.at[seq_peer(k)], rin.at[me], sm_q, k, "seq", seq_peer(k))

    for k in range(1, n_seq):
        v_copy(k).start()
    rr[me] = re[me]

    phase("outmm")
    def o_copy(k):
        return remote(pb.at[tp_peer(k)], pr.at[my], sm_o, k, "tp", tp_peer(k))

    for k in range(1, n_tp):
        d = tp_peer(k)
        block = wfull[pl.ds(pl.multiple_of(d * drows, drows), drows), :]
        pb[d] = mm(block, nb[...], NT).astype(BF16)
        o_copy(k).start()
    block = wfull[pl.ds(pl.multiple_of(my * drows, drows), drows), :]
    pr[my] = mm(block, nb[...], NT).astype(BF16)

    phase("wait_v")
    for k in range(1, n_seq):
        v_copy(k).wait_recv()
    acc = jnp.zeros((nrow, ch), F32)
    for j in reversed(range(n_seq)):
        ren[j] = acc
        acc = jnp.exp(spread_d[8 * j : 8 * j + 1]) * acc + rr[j]
    for k in range(1, n_seq):
        vb_copy(k).start()
    rin[me] = ren[me]

    phase("gradw")
    def g_copy(k):
        return remote(gb.at[seq_peer(k)], gr.at[me], sm_v, k, "seq", seq_peer(k))

    for k in range(1, n_seq):
        d = seq_peer(k)
        block = dfull[pl.ds(pl.multiple_of(d * wrows, wrows), wrows), :]
        gb[d] = mm(block, nb[...]).astype(BF16)
        g_copy(k).start()
    block = dfull[pl.ds(pl.multiple_of(me * wrows, wrows), wrows), :]
    gr[me] = mm(block, nb[...]).astype(BF16)

    phase("wait_vb")
    for k in range(1, n_seq):
        vb_copy(k).wait_recv()
    phase("back")
    rcur[...] = rin[...].reshape(ns, ch)

    to_head = (iota((ch, LANES), 0) // HEAD == iota((ch, LANES), 1)).astype(F32)
    neg_c = jnp.concatenate([negexp, jnp.zeros((1, LANES - heads), F32)], axis=1)
    blk = rows // n_tp

    def back(i, carry):
        c = nc - 1 - i
        sl = pl.ds(pl.multiple_of(c * Q, Q), Q)
        bmap, cmap = bcv[sl, :ns], bcv[sl, ns:]
        scores = mm3(cmap, bmap, NT)
        scores_t = mm3(bmap, cmap, NT)
        arow[...] = jnp.zeros((Q, LANES), F32)
        acol[...] = jnp.zeros((LANES, Q), F32)
        dga[...] = jnp.zeros((Q, Q), F32)
        for p in range(pairs):
            ps = slice(p * PAIR, (p + 1) * PAIR)
            g2 = gm[sl, ps]
            cross = mm3(g2, pair_stack(x[sl, ps] * st[sl, ps]), NT)
            both = []
            for i_h, h in enumerate((2 * p, 2 * p + 1)):
                diff = lx[sl, h * HEAD : h * HEAD + 1] - lt[c, h : h + 1, :]
                weighted = jnp.exp(jnp.where(upper, diff, -1e30)) * cross[:, i_h * Q : (i_h + 1) * Q]
                dga[...] += weighted
                term = weighted * scores
                arow[...] += jnp.where(lane == h, jnp.sum(term, axis=1, keepdims=True), 0.0)
                acol[h : h + 1, :] = jnp.sum(term, axis=0, keepdims=True)
                diff_t = lt[c, h : h + 1, :] - lx[sl, h * HEAD : h * HEAD + 1]
                decay_t = jnp.exp(jnp.where(lower, diff_t, -1e30))
                both.append((decay_t * scores_t).astype(BF16))
            dxs[:, ps] = mm(jnp.concatenate(both, axis=1), pair_stack(g2))
        cum = lx[sl, :]
        last = cum[Q - 1 : Q, :]
        grown = jnp.exp(cum)
        to_end = jnp.exp(last - cum)
        rv = rcur[...]
        sv = sst[c]
        gv = gm[sl, :]
        xv = x[sl, :]
        sx = st[sl, :]
        gg = gv * grown
        d_in = mm(bmap, rv) * to_end
        dxt = dxs[...] + d_in
        xt = xv * sx
        per_head = mmh(
            jnp.concatenate([gg * mm(cmap, sv), xt * d_in, xv * dxt], axis=0), to_head
        )
        fixed = mmh(
            jnp.broadcast_to(jnp.sum(rv * sv, axis=0, keepdims=True) * jnp.exp(last), (8, ch)), to_head
        )[0:1]
        swing = per_head[:Q] + arow[...] - jnp.transpose(acol[...])
        dld = mmh(tri_u, swing) + mmh(strict, per_head[Q : 2 * Q]) + fixed
        dstep = per_head[2 * Q :] + dld * neg_c
        slope = sigmoid(raw[sl, :].astype(F32) + db[...])
        o_gdt[sl, :] = dstep[:, :heads] * slope
        dgv = dga[...]
        d_b = mm3(jnp.transpose(dgv), cmap) + mm3(xt * to_end, rv, NT)
        d_c = mm3(dgv, bmap) + mm3(gg, sv, NT)
        per = Q // blk
        qs[pl.ds(c * per, per), :, :ns] = d_b.reshape(per, blk, ns)
        qs[pl.ds(c * per, per), :, ns:] = d_c.reshape(per, blk, ns)
        uv = u[sl, :]
        su = sigmoid(uv)
        dus[sl, :] = (sx * dxt + skip_x * gv) * (su * (1.0 + uv * (1.0 - su)))
        rcur[...] = cf[c] + jnp.exp(last) * rv
        return carry

    lax.fori_loop(0, nc, back, 0)

    phase("wait_q")
    def q_copy(k):
        return remote(qs.at[tp_peer(k)], qr.at[my], sm_p, k, "tp", tp_peer(k))

    def a_copy(k):
        return remote(qa.at[my], qa.at[my], sm_a, k, "tp", tp_peer(k))

    edge_x = remote(dus.at[pl.ds(0, 8)], dus.at[pl.ds(rows, 8)], sm_h, 2, "seq", prv)
    edge_b = remote(dub.at[pl.ds(0, 8)], dub.at[pl.ds(rows, 8)], sm_h, 3, "seq", prv)
    for k in range(1, n_tp):
        q_copy(k).start()
    qr[my] = qs[my]
    edge_x.start()
    for k in range(1, n_tp):
        q_copy(k).wait_recv()
    phase("qsum")
    qsum = qr[0].astype(F32)
    for j in range(1, n_tp):
        qsum = qsum + qr[j].astype(F32)
    qa[my] = qsum.astype(BF16)
    for k in range(1, n_tp):
        a_copy(k).start()

    edge_x.wait_recv()

    phase("convbx")
    def conv_back(ref, weights, out, c):
        base = pl.multiple_of(c * Q, Q)
        ext = ref[pl.ds(base, Q + 8), :]
        tail = jnp.where((c < nc - 1) | (me < n_seq - 1), ext[Q:], 0.0)
        ext = jnp.concatenate([ext[:Q], tail], axis=0)
        acc = weights[3:4, :] * ext[:Q]
        for k in range(3):
            acc = acc + weights[k : k + 1, :] * pltpu.roll(ext, Q + 8 - (3 - k), 0)[:Q]
        out[pl.ds(base, Q), :] = acc

    def conv_back_x(c, carry):
        conv_back(dus, cw, o_gx, c)
        return carry

    lax.fori_loop(0, nc, conv_back_x, 0)

    phase("wait_a")
    for k in range(1, n_tp):
        a_copy(k).wait_recv()
    phase("dub")
    ubv = ub[...]
    sb = sigmoid(ubv)
    dub[pl.ds(0, rows), :] = qa[...].reshape(rows, 2 * ns).astype(F32) * (sb * (1.0 + ubv * (1.0 - sb)))
    edge_b.start()

    phase("wait_o")
    for k in range(1, n_tp):
        o_copy(k).wait_recv()
    phase("osum")
    osum = pr[0].astype(F32)
    for j in range(1, n_tp):
        osum = osum + pr[j].astype(F32)
    o_out[...] = osum.astype(BF16)

    phase("convbb")
    edge_b.wait_recv()

    def conv_back_b(c, carry):
        conv_back(dub, cwb, o_gbc, c)
        return carry

    lax.fori_loop(0, nc, conv_back_b, 0)

    phase("wait_g")
    for k in range(1, n_seq):
        g_copy(k).wait_recv()
    phase("gsum")
    gsum = gr[0].astype(F32)
    for j in range(1, n_seq):
        gsum = gsum + gr[j].astype(F32)
    o_gw[...] = gsum

    phase("drain")
    halo_x.wait_send()
    halo_b.wait_send()
    edge_x.wait_send()
    edge_b.wait_send()
    for k in range(1, n_seq):
        for copy in (t_copy, w_copy, s_copy, sb_copy, v_copy, vb_copy, g_copy):
            copy(k).wait_send()
    for k in range(1, n_tp):
        for copy in (d_copy, r_copy, o_copy, q_copy, a_copy):
            copy(k).wait_send()
    phase("")


def solution(mesh):
    n_seq, n_tp = mesh.shape["seq"], mesh.shape["tp"]

    def shards(
        inner_x,
        gate_z,
        proj_bc,
        dt_raw,
        a_log,
        dt_bias,
        d_skip,
        conv_x,
        bias_x,
        conv_bc,
        bias_bc,
        norm_gain,
        w_out,
        d_out,
    ):
        rows, ch = inner_x.shape
        heads = a_log.shape[0]
        ns2 = proj_bc.shape[1]
        ns = ns2 // 2
        nc = rows // Q
        nrow = ns // n_seq
        wrows, drows = w_out.shape[1], d_out.shape[1]
        width = wrows * n_seq
        w_t = w_out.T
        d_t = d_out.T

        def column(v):
            return jnp.pad(v, (0, 16 - heads))[:, None]

        vm = functools.partial(pl.BlockSpec, memory_space=pltpu.VMEM)
        big = pltpu.VMEM((rows, ch), F32)
        chunk_states = pltpu.VMEM((nc, ns, ch), F32)
        slices = pltpu.VMEM((n_seq, nrow, ch), F32)
        sem_s = pltpu.SemaphoreType.DMA((2, n_seq))
        sem_t = pltpu.SemaphoreType.DMA((2, n_tp))
        scratch = [
            pltpu.VMEM((width, ch), BF16),
            pltpu.VMEM((width, rows), BF16),
            pltpu.VMEM((16, ch), BF16),
            pltpu.VMEM((16, ns2), BF16),
            pltpu.VMEM((8, LANES), F32),
            pltpu.VMEM((n_seq, 8, LANES), F32),
            big,
            big,
            pltpu.VMEM((nc, 16, Q), F32),
            big,
            big,
            pltpu.VMEM((rows, ns2), F32),
            pltpu.VMEM((rows, ns2), F32),
            chunk_states,
            chunk_states,
            chunk_states,
            big,
            big,
            big,
            big,
            pltpu.VMEM((rows, ch), BF16),
            pltpu.VMEM((Q, ch), F32),
            pltpu.VMEM((rows + 8, ch), F32),
            pltpu.VMEM((rows + 8, ns2), F32),
            pltpu.VMEM((ns, ch), F32),
            slices,
            slices,
            slices,
            slices,
            slices,
            slices,
            slices,
            slices,
            pltpu.VMEM((8, rows), F32),
            pltpu.VMEM((n_tp, 8, rows), F32),
            pltpu.VMEM((n_tp, drows, rows), BF16),
            pltpu.VMEM((n_tp, drows, rows), BF16),
            pltpu.VMEM((n_seq, wrows, ch), BF16),
            pltpu.VMEM((n_seq, wrows, ch), BF16),
            pltpu.VMEM((n_tp, rows // n_tp, ns2), F32),
            pltpu.VMEM((n_tp, rows // n_tp, ns2), F32),
            pltpu.VMEM((n_tp, rows // n_tp, ns2), BF16),
            pltpu.VMEM((Q, LANES), F32),
            pltpu.VMEM((LANES, Q), F32),
            pltpu.VMEM((Q, Q), F32),
            pltpu.SemaphoreType.DMA((2, 4)),
            sem_s,
            sem_s,
            sem_t,
            sem_s,
            sem_s,
            sem_s,
            sem_s,
            sem_t,
            sem_t,
            sem_s,
            sem_t,
            sem_t,
        ]
        out_t, g_x, g_z, g_bc, g_dt, g_w = pl.pallas_call(
            functools.partial(kernel, (n_seq, n_tp, ch * n_tp)),
            out_shape=[
                jax.ShapeDtypeStruct((drows, rows), BF16),
                jax.ShapeDtypeStruct((rows, ch), F32),
                jax.ShapeDtypeStruct((rows, ch), F32),
                jax.ShapeDtypeStruct((rows, ns2), F32),
                jax.ShapeDtypeStruct((rows, heads), F32),
                jax.ShapeDtypeStruct((wrows, ch), F32),
            ],
            in_specs=[vm()] * 16,
            out_specs=[vm()] * 6,
            scratch_shapes=scratch,
            compiler_params=pltpu.CompilerParams(
                collective_id=0, has_side_effects=True, vmem_limit_bytes=67_043_328
            ),
            name="mixer",
        )(
            inner_x,
            gate_z,
            proj_bc,
            dt_raw,
            w_t,
            d_t,
            conv_x,
            bias_x[None, :],
            conv_bc,
            bias_bc[None, :],
            norm_gain[None, :],
            a_log[None, :],
            dt_bias[None, :],
            d_skip[None, :],
            column(a_log),
            column(dt_bias),
        )
        return out_t.T, g_x, g_z, g_bc, g_dt, g_w.T

    in_specs = (
        P("seq", "tp"),
        P("seq", "tp"),
        P("seq", None),
        P("seq", "tp"),
        P("tp"),
        P("tp"),
        P("tp"),
        P(None, "tp"),
        P("tp"),
        P(),
        P(),
        P("tp"),
        P("tp", "seq"),
        P("seq", "tp"),
    )
    out_specs = (
        P("seq", "tp"),
        P("seq", "tp"),
        P("seq", "tp"),
        P("seq", None),
        P("seq", "tp"),
        P("tp", "seq"),
    )
    return jax.shard_map(
        shards, mesh=mesh, in_specs=in_specs, out_specs=out_specs, check_vma=False
    )
```

```python
import functools

import jax
import jax.numpy as jnp
from jax import lax
from jax.experimental import pallas as pl
from jax.experimental.pallas import tpu as pltpu
from jax.sharding import PartitionSpec as P

MESH = pl.DeviceIdType.MESH
F32 = jnp.float32
BF16 = jnp.bfloat16
HIGH = lax.Precision.HIGHEST
EPSILON = 1e-05
NN = ((1,), (0,))
NT = ((1,), (1,))
Q = 128
PAIR = 128
HEAD = 64
LANES = 128


def mm(a, b, dims=NN):
    return lax.dot_general(a.astype(BF16), b.astype(BF16), (dims, ((), ())), preferred_element_type=F32)


def mmh(a, b, dims=NN):
    return lax.dot_general(
        a.astype(F32), b.astype(F32), (dims, ((), ())), precision=HIGH, preferred_element_type=F32
    )


def halves(v):
    high = v.astype(BF16)
    return high, (v - high.astype(F32)).astype(BF16)


def mm3(a, b, dims=NN):
    a0, a1 = halves(a)
    b0, b1 = halves(b)
    return mm(a0, b0, dims) + (mm(a1, b0, dims) + mm(a0, b1, dims))


def iota(shape, dim):
    return lax.broadcasted_iota(jnp.int32, shape, dim)


def sigmoid(v):
    return 1.0 / (1.0 + jnp.exp(-v))


def softplus(v):
    return jnp.maximum(v, 0.0) + jnp.log1p(jnp.exp(-jnp.abs(v)))


def pair_stack(v):
    lane = iota(v.shape, 1)
    return jnp.concatenate(
        [jnp.where(lane < HEAD, v, 0.0), jnp.where(lane >= HEAD, v, 0.0)], axis=0
    )


def kernel(
    sizes,
    ix,
    gz,
    bc,
    raw,
    wt,
    dt,
    cw,
    bx,
    cwb,
    bb,
    gain,
    al,
    db,
    ds,
    o_out,
    o_gx,
    o_gz,
    o_gbc,
    o_gdt,
    o_gw,
    wfull,
    dfull,
    hx,
    hb,
    dsend,
    dbuf,
    st,
    lx,
    lt,
    u,
    x,
    ub,
    bcv,
    fr,
    sst,
    cf,
    y,
    gated,
    gn,
    gm,
    nb,
    dxs,
    dus,
    dub,
    rcur,
    se,
    sr,
    en,
    sin,
    re,
    rr,
    ren,
    rin,
    ts,
    tr,
    pb,
    pp,
    po1,
    po2,
    gb,
    ga1,
    ga2,
    ga3,
    ga4,
    gb1,
    gb2,
    gb3,
    gb4,
    qs,
    qr,
    qa,
    arow,
    acol,
    dga,
    ssq,
    sm_l,
    sm_h,
    sm_d,
    sm_w,
    sm_g,
    sm_s,
    sm_b,
    sm_r,
    sm_q,
    sm_t,
    sm_o,
    sm_v,
    sm_p,
    sm_a,
):
    n_seq, n_tp, inner = sizes
    rows, ch = ix.shape
    nc = rows // Q
    heads = raw.shape[0]
    pairs = ch // PAIR
    ns = bc.shape[1] // 2
    me, my = lax.axis_index("seq"), lax.axis_index("tp")
    wrows = wt.shape[0]
    drows = dt.shape[0]
    nrow = ns // n_seq

    scope = []

    def phase(name):
        if scope:
            scope.pop().__exit__(None, None, None)
        if name:
            scope.append(jax.named_scope(name))
            scope[0].__enter__()

    side = 4
    zi, xi = lax.div(me, side), lax.rem(me, side)
    yi, core = lax.div(my, 2), lax.rem(my, 2)

    def step(v, k):
        return lax.rem(v + k + side, side)

    x_up, x_dn = step(xi, 1), step(xi, -1)
    z_up, z_dn = step(zi, 1), step(zi, -1)
    y_up, y_dn = step(yi, 1), step(yi, -1)
    x_far, z_far, y_far = step(xi, 2), step(zi, 2), step(yi, 2)
    to_xu, to_xd = zi * side + x_up, zi * side + x_dn
    to_zu, to_zd = z_up * side + xi, z_dn * side + xi
    to_yu, to_yd = y_up * 2 + core, y_dn * 2 + core
    mate = yi * 2 + 1 - core

    def seq_peer(k):
        return lax.rem(me + k, n_seq)

    def tp_peer(k):
        return lax.rem(my + k, n_tp)

    phase("barrier")
    barrier = pltpu.get_barrier_semaphore()
    for k in range(1, n_seq):
        pl.semaphore_signal(barrier, inc=1, device_id={"seq": seq_peer(k)}, device_id_type=MESH)
    for k in range(1, n_tp):
        pl.semaphore_signal(barrier, inc=1, device_id={"tp": tp_peer(k)}, device_id_type=MESH)
    pl.semaphore_wait(barrier, n_seq + n_tp - 2)

    def remote(src, dst, sems, k, axis, peer):
        return pltpu.make_async_remote_copy(
            src_ref=src,
            dst_ref=dst,
            send_sem=sems.at[0, k],
            recv_sem=sems.at[1, k],
            device_id={axis: peer},
            device_id_type=MESH,
        )

    phase("start")
    nxt, prv = seq_peer(1), seq_peer(n_seq - 1)
    halo_x = remote(ix.at[pl.ds(rows - 16, 16)], hx, sm_h, 0, "seq", nxt)
    halo_b = remote(bc.at[pl.ds(rows - 16, 16)], hb, sm_h, 1, "seq", nxt)
    halo_x.start()
    halo_b.start()

    half = wrows // 2
    near = 48
    ra, rb = pl.ds(0, half), pl.ds(half, half)
    ra1, ra2 = pl.ds(0, near), pl.ds(near, half - near)
    rb1, rb2 = pl.ds(half, near), pl.ds(half + near, half - near)
    lo, hi, every = pl.ds(0, 2), pl.ds(2, 2), pl.ds(0, side)

    def w_view(z, x, r):
        return wfull.at[z, x, r]

    def w_move(i, peer, z, x, r, src=None):
        return remote(w_view(z, x, r) if src is None else src, w_view(z, x, r), sm_w, i, "seq", peer)

    w_copies = [
        w_move(0, to_xu, zi, xi, ra, wt.at[ra]),
        w_move(1, to_xd, zi, xi, ra, wt.at[ra]),
        w_move(2, to_zu, zi, xi, rb, wt.at[rb]),
        w_move(3, to_zd, zi, xi, rb, wt.at[rb]),
        w_move(4, to_xu, zi, x_dn, ra1),
        w_move(5, to_xd, zi, x_up, ra2),
        w_move(6, to_zu, z_dn, xi, rb1),
        w_move(7, to_zd, z_up, xi, rb2),
        w_move(8, to_zu, zi, every, ra),
        w_move(9, to_zd, zi, every, ra),
        w_move(10, to_xu, every, xi, rb),
        w_move(11, to_xd, every, xi, rb),
        w_move(12, to_zu, z_dn, lo, ra),
        w_move(13, to_zd, z_up, hi, ra),
        w_move(14, to_xu, lo, x_dn, rb),
        w_move(15, to_xd, hi, x_up, rb),
    ]

    dhalf = drows // 2

    def d_view(y, c, off=0, size=drows):
        return dfull.at[pl.ds(pl.multiple_of((y * 2 + c) * drows + off, 32), size)]

    def d_move(i, peer, y, c, off=0, size=drows, src=None):
        view = d_view(y, c, off, size)
        return remote(view if src is None else src, view, sm_g, i, "tp", peer)

    d_copies = [
        d_move(0, to_yu, yi, core, src=dt),
        d_move(1, to_yd, yi, core, src=dt),
        d_move(2, mate, yi, core, src=dt),
        d_move(3, to_yu, y_dn, core, 0, dhalf),
        d_move(4, to_yd, y_up, core, dhalf, dhalf),
        d_move(5, mate, y_dn, core),
        d_move(6, mate, y_up, core),
        d_move(7, mate, y_far, core),
    ]

    def start(copies, first, last):
        for copy in copies[first:last]:
            copy.start()

    def arrived(copies, first, last):
        for copy in copies[first:last]:
            copy.wait_recv()

    start(w_copies, 0, 4)
    start(d_copies, 0, 3)
    own_w = pltpu.make_async_copy(wt, wfull.at[zi, xi], sm_l.at[0])
    own_d = pltpu.make_async_copy(dt, d_view(yi, core), sm_l.at[1])
    own_w.start()
    own_d.start()

    phase("steps")
    spread = (iota((LANES, ch), 1) // HEAD == iota((LANES, ch), 0)).astype(F32)
    spread_h = spread[:heads]
    ident = (iota((heads, heads), 0) == iota((heads, heads), 1)).astype(F32)
    negexp = -jnp.exp(al[...])
    neg_x = mmh(jnp.broadcast_to(negexp, (8, heads)), spread_h)[0:1]
    dtb_x = mmh(jnp.broadcast_to(db[...], (8, heads)), spread_h)[0:1]
    skip_x = mmh(jnp.broadcast_to(ds[...], (8, heads)), spread_h)[0:1]
    tri = (iota((Q, Q), 0) >= iota((Q, Q), 1)).astype(F32)
    tri_u = (iota((Q, Q), 0) <= iota((Q, Q), 1)).astype(F32)
    strict = (iota((Q, Q), 0) > iota((Q, Q), 1)).astype(F32)

    def column(v):
        return mmh(ident, jnp.broadcast_to(v, (8, heads)), NT)[:, 0:1]

    def in_line(ref):
        return jnp.concatenate([ref[i : i + 1] for i in range(ref.shape[0])], axis=1)

    dt_col, neg_col = column(db[...]), column(negexp)
    bias_line, gain_line = in_line(bx), in_line(gain)

    def steps(c, total):
        sl = pl.ds(pl.multiple_of(c * Q, Q), Q)
        r = raw[:, sl].astype(F32)
        r_t = jnp.transpose(jnp.concatenate([r, jnp.zeros((LANES - heads, Q), F32)], axis=0))
        s = softplus(mm(r_t, spread) + dtb_x)
        cum = mmh(tri, s * neg_x)
        st[sl, :] = s
        lx[sl, :] = cum
        lt[c] = mmh(softplus(r + dt_col) * neg_col, tri_u)
        return total + cum[Q - 1 : Q, :]

    total = lax.fori_loop(0, nc, steps, jnp.zeros((1, ch), F32))
    pick = (iota((ch, LANES), 0) == iota((ch, LANES), 1) * HEAD).astype(F32)
    dsend[...] = mmh(jnp.broadcast_to(total, (8, ch)), pick)

    def t_copy(k):
        return remote(dsend, dbuf.at[me], sm_d, k, "seq", seq_peer(k))

    dbuf[me] = dsend[...]
    for k in range(1, n_seq):
        t_copy(k).start()

    phase("wait_w1")
    arrived(w_copies, 0, 4)
    start(w_copies, 4, 8)
    phase("wait_halo")
    halo_x.wait_recv()
    halo_b.wait_recv()

    phase("convs")
    def conv_of(ref, halo, weights, bias, c):
        base = pl.multiple_of(c * Q, Q)
        own = ref[pl.ds(base, Q), :].astype(F32)
        before = pl.multiple_of(jnp.maximum(c * Q - 16, 0), 16)
        prev = ref[pl.ds(before, 16), :].astype(F32)
        edge = jnp.where(me > 0, halo[...].astype(F32), 0.0)
        head = jnp.where(c > 0, prev, edge)[8:16]
        ext = jnp.concatenate([head, own], axis=0)
        acc = bias + weights[3:4, :] * own
        for k in range(3):
            acc = acc + weights[k : k + 1, :] * pltpu.roll(ext, Q + 8 - (5 + k), 0)[:Q]
        return acc

    def convs(c, carry):
        sl = pl.ds(pl.multiple_of(c * Q, Q), Q)
        vb = conv_of(bc, hb, cwb, bb[...], c)
        ub[sl, :] = vb
        pbc = vb * sigmoid(vb)
        bcv[sl, :] = pbc
        vx = conv_of(ix, hx, cw, bias_line, c)
        u[sl, :] = vx
        xv = vx * sigmoid(vx)
        x[sl, :] = xv
        cum = lx[sl, :]
        to_end = jnp.exp(cum[Q - 1 : Q, :] - cum)
        b_t = jnp.transpose(pbc[:, :ns])
        fresh = mm3(b_t, xv * st[sl, :] * to_end)
        fr[c] = fresh
        return jnp.exp(cum[Q - 1 : Q, :]) * carry + fresh

    end = lax.fori_loop(0, nc, convs, jnp.zeros((ns, ch), F32))
    se[...] = end.reshape(n_seq, nrow, ch)

    phase("send_s")
    def s_copy(k):
        return remote(se.at[seq_peer(k)], sr.at[me], sm_s, k, "seq", seq_peer(k))

    def sb_copy(k):
        return remote(en.at[seq_peer(k)], sin.at[me], sm_b, k, "seq", seq_peer(k))

    for k in range(1, n_seq):
        s_copy(k).start()
    sr[me] = se[me]
    phase("wait_w2")
    own_w.wait()
    arrived(w_copies, 4, 8)
    start(w_copies, 8, 12)
    phase("wait_d1")
    arrived(d_copies, 0, 2)
    start(d_copies, 3, 7)

    upper = iota((Q, Q), 0) >= iota((Q, Q), 1)
    lower = iota((Q, Q), 0) <= iota((Q, Q), 1)

    phase("inside")
    def inside(c, carry):
        sl = pl.ds(pl.multiple_of(c * Q, Q), Q)
        scores = mm3(bcv[sl, ns:], bcv[sl, :ns], NT)
        for p in range(pairs):
            ps = slice(p * PAIR, (p + 1) * PAIR)
            both = []
            for h in (2 * p, 2 * p + 1):
                diff = lx[sl, h * HEAD : h * HEAD + 1] - lt[c, h : h + 1, :]
                decay = jnp.exp(jnp.where(upper, diff, -1e30))
                both.append(decay * scores)
            y[sl, ps] = mm3(jnp.concatenate(both, axis=1), pair_stack(x[sl, ps] * st[sl, ps]))
        return carry

    lax.fori_loop(0, nc, inside, 0)

    phase("wait_s")
    for k in range(1, n_seq):
        t_copy(k).wait_recv()
    for k in range(1, n_seq):
        s_copy(k).wait_recv()
    phase("scan")
    spread_d = mmh(dbuf[...].reshape(n_seq * 8, LANES), spread)

    acc = jnp.zeros((nrow, ch), F32)
    for j in range(n_seq):
        en[j] = acc
        acc = jnp.exp(spread_d[8 * j : 8 * j + 1]) * acc + sr[j]
    for k in range(1, n_seq):
        sb_copy(k).start()
    sin[me] = en[me]

    phase("wait_d2")
    own_d.wait()
    arrived(d_copies, 3, 5)
    start(d_copies, 7, 8)
    phase("wait_w3")
    arrived(w_copies, 8, 12)
    start(w_copies, 12, 16)
    phase("wait_sb")
    for k in range(1, n_seq):
        sb_copy(k).wait_recv()
    phase("combine")
    lane = iota((Q, LANES), 1)

    def combine(c, state):
        sl = pl.ds(pl.multiple_of(c * Q, Q), Q)
        sst[c] = state
        cum = lx[sl, :]
        mixed = y[sl, :] + jnp.exp(cum) * mm3(bcv[sl, ns:], state) + skip_x * x[sl, :]
        y[sl, :] = mixed
        zv = gz[sl, :].astype(F32)
        gv = mixed * zv * sigmoid(zv)
        gated[sl, :] = gv
        ssq[sl, :] = jnp.sum(gv * gv, axis=1, keepdims=True)
        return jnp.exp(cum[Q - 1 : Q, :]) * state + fr[c]

    lax.fori_loop(0, nc, combine, sin[...].reshape(ns, ch))
    phase("wait_wd")
    arrived(d_copies, 2, 3)
    arrived(d_copies, 5, 8)
    arrived(w_copies, 12, 16)
    phase("gn")
    kb = wrows * side

    def gn_block(b, carry):
        kk = pl.ds(pl.multiple_of(b * kb, kb), kb)
        part = mm(jnp.transpose(dfull[kk, :]), wfull[b].reshape(kb, ch))

        @pl.when(b == 0)
        def _():
            gn[...] = part

        @pl.when(b > 0)
        def _():
            gn[...] += part

        return carry

    lax.fori_loop(0, side, gn_block, 0)
    phase("sums")

    def sums(c, carry):
        sl = pl.ds(pl.multiple_of(c * Q, Q), Q)
        scaled = gn[sl, :] * gain_line
        gn[sl, :] = scaled
        ip = jnp.sum(scaled * gated[sl, :], axis=1, keepdims=True)
        both = jnp.where(lane == 0, ssq[sl, :], jnp.where(lane == 1, ip, 0.0))
        ts[:, sl] = jnp.transpose(both)[:8]
        return carry

    lax.fori_loop(0, nc, sums, 0)
    phase("wait_t")
    def r_copy(k):
        return remote(ts, tr.at[my], sm_t, k, "tp", tp_peer(k))

    for k in range(1, n_tp):
        r_copy(k).start()
    tr[my] = ts[...]
    for k in range(1, n_tp):
        r_copy(k).wait_recv()
    phase("norm")
    tsum = tr[0]
    for j in range(1, n_tp):
        tsum = tsum + tr[j]
    gn_pad = jnp.concatenate([tsum, jnp.zeros((Q - 8, rows), F32)], axis=0)
    ts2 = [jnp.transpose(gn_pad[:, c * Q : (c + 1) * Q]) for c in range(nc)]

    for c in range(nc):
        sl = pl.ds(c * Q, Q)
        inv = lax.rsqrt(ts2[c][:, 0:1] / inner + EPSILON)
        coef = inv * inv * inv * ts2[c][:, 1:2] / inner
        gv = gated[sl, :]
        nb[sl, :] = (gv * inv * gain_line).astype(BF16)
        gg = inv * gn[sl, :] - gv * coef
        zv = gz[sl, :].astype(F32)
        sg = sigmoid(zv)
        o_gz[sl, :] = gg * y[sl, :] * sg * (1.0 + zv * (1.0 - sg))
        gmv = gg * zv * sg
        gm[sl, :] = gmv
        c_t = jnp.transpose(bcv[sl, ns:])
        cf[c] = mm3(c_t, gmv * jnp.exp(lx[sl, :]))

    racc = cf[nc - 1]
    for c in reversed(range(nc - 1)):
        racc = cf[c] + jnp.exp(lx[pl.ds(c * Q + Q - 1, 1), :]) * racc
    re[...] = racc.reshape(n_seq, nrow, ch)

    phase("send_v")
    def v_copy(k):
        return remote(re.at[seq_peer(k)], rr.at[me], sm_r, k, "seq", seq_peer(k))

    def vb_copy(k):
        return remote(ren.at[seq_peer(k)], rin.at[me], sm_q, k, "seq", seq_peer(k))

    for k in range(1, n_seq):
        v_copy(k).start()
    rr[me] = re[me]

    phase("outmm")
    def share(y0, c0):
        block = wfull[y0, pl.ds(2 * c0, 2)].reshape(drows, ch)
        pb[y0, c0] = mm(block, nb[...], NT).astype(BF16)

    def other(j, carry):
        share(j, 1 - core)
        return carry

    def same(j, carry):
        share(j, core)
        return carry

    o_half1, o_half2 = pl.ds(0, dhalf), pl.ds(dhalf, dhalf)
    o_copies = [
        remote(pb.at[every, 1 - core], pp, sm_o, 0, "tp", mate),
        remote(pb.at[y_far, core, o_half1], po1.at[o_half1], sm_o, 1, "tp", to_yu),
        remote(pb.at[y_far, core, o_half2], po1.at[o_half2], sm_o, 2, "tp", to_yd),
        remote(pb.at[y_up, core], po2.at[0], sm_o, 3, "tp", to_yu),
        remote(pb.at[y_dn, core], po2.at[1], sm_o, 4, "tp", to_yd),
    ]
    lax.fori_loop(0, side, other, 0)
    start(o_copies, 0, 1)
    lax.fori_loop(0, side, same, 0)

    phase("wait_v")
    for k in range(1, n_seq):
        v_copy(k).wait_recv()
    acc = jnp.zeros((nrow, ch), F32)
    for j in reversed(range(n_seq)):
        ren[j] = acc
        acc = jnp.exp(spread_d[8 * j : 8 * j + 1]) * acc + rr[j]
    for k in range(1, n_seq):
        vb_copy(k).start()
    rin[me] = ren[me]

    phase("gradw")
    g_copies = [
        remote(gb.at[z_far, lo, ra], ga1.at[lo], sm_v, 0, "seq", to_zu),
        remote(gb.at[z_far, hi, ra], ga1.at[hi], sm_v, 1, "seq", to_zd),
        remote(gb.at[lo, x_far, rb], gb1.at[lo], sm_v, 2, "seq", to_xu),
        remote(gb.at[hi, x_far, rb], gb1.at[hi], sm_v, 3, "seq", to_xd),
        remote(gb.at[z_up, every, ra], ga2.at[0], sm_v, 4, "seq", to_zu),
        remote(gb.at[z_dn, every, ra], ga2.at[1], sm_v, 5, "seq", to_zd),
        remote(gb.at[every, x_up, rb], gb2.at[0], sm_v, 6, "seq", to_xu),
        remote(gb.at[every, x_dn, rb], gb2.at[1], sm_v, 7, "seq", to_xd),
        remote(gb.at[zi, x_far, ra1], ga3.at[ra1], sm_v, 8, "seq", to_xu),
        remote(gb.at[zi, x_far, ra2], ga3.at[ra2], sm_v, 9, "seq", to_xd),
        remote(gb.at[z_far, xi, rb1], gb3.at[ra1], sm_v, 10, "seq", to_zu),
        remote(gb.at[z_far, xi, rb2], gb3.at[ra2], sm_v, 11, "seq", to_zd),
        remote(gb.at[zi, x_up, ra], ga4.at[0], sm_v, 12, "seq", to_xu),
        remote(gb.at[zi, x_dn, ra], ga4.at[1], sm_v, 13, "seq", to_xd),
        remote(gb.at[z_up, xi, rb], gb4.at[0], sm_v, 14, "seq", to_zu),
        remote(gb.at[z_dn, xi, rb], gb4.at[1], sm_v, 15, "seq", to_zd),
    ]

    def plus(ref, index, *others):
        total = ref[index].astype(F32)
        for part in others:
            total = total + part.astype(F32)
        ref[index] = total.astype(BF16)

    def g_block(k, carry):
        b = step(zi, 2 + k)
        rows_of = pl.ds(pl.multiple_of(b * kb, kb), kb)
        gb[b] = mm(dfull[rows_of, :], nb[...]).astype(BF16).reshape(side, wrows, ch)

        @pl.when(k == 0)
        def _():
            start(g_copies, 0, 2)

        return carry

    lax.fori_loop(0, side, g_block, 0)
    start(g_copies, 2, 4)

    def g_second():
        arrived(g_copies, 0, 4)
        for j in range(2):
            plus(gb, (z_up, j, ra), ga1[j])
            plus(gb, (z_dn, 2 + j, ra), ga1[2 + j])
            plus(gb, (j, x_up, rb), gb1[j])
            plus(gb, (2 + j, x_dn, rb), gb1[2 + j])
        start(g_copies, 4, 8)

    def g_third():
        arrived(g_copies, 4, 8)
        for j in range(side):
            plus(gb, (zi, j, ra), ga2[0, j], ga2[1, j])
            plus(gb, (j, xi, rb), gb2[0, j], gb2[1, j])
        start(g_copies, 8, 12)

    def g_fourth():
        arrived(g_copies, 8, 12)
        plus(gb, (zi, x_up, ra1), ga3[ra1])
        plus(gb, (zi, x_dn, ra2), ga3[ra2])
        plus(gb, (z_up, xi, rb1), gb3[ra1])
        plus(gb, (z_dn, xi, rb2), gb3[ra2])
        start(g_copies, 12, 16)

    def g_last():
        arrived(g_copies, 12, 16)
        o_gw[ra, :] = gb[zi, xi, ra].astype(F32) + ga4[0].astype(F32) + ga4[1].astype(F32)
        o_gw[rb, :] = gb[zi, xi, rb].astype(F32) + gb4[0].astype(F32) + gb4[1].astype(F32)

    def o_second():
        arrived(o_copies, 0, 1)
        for j in range(side):
            plus(pb, (j, core), pp[j])
        start(o_copies, 1, 3)

    def o_third():
        arrived(o_copies, 1, 3)
        plus(pb, (y_up, core, o_half1), po1[o_half1])
        plus(pb, (y_dn, core, o_half2), po1[o_half2])
        start(o_copies, 3, 5)

    def o_last():
        arrived(o_copies, 3, 5)
        total = pb[yi, core].astype(F32) + po2[0].astype(F32) + po2[1].astype(F32)
        o_out[...] = total.astype(BF16)

    phase("o_second")
    o_second()

    phase("wait_vb")
    for k in range(1, n_seq):
        vb_copy(k).wait_recv()
    phase("back")
    rcur[...] = rin[...].reshape(ns, ch)

    to_head = (iota((ch, LANES), 0) // HEAD == iota((ch, LANES), 1)).astype(F32)
    neg_c = jnp.concatenate([negexp, jnp.zeros((1, LANES - heads), F32)], axis=1)
    blk = rows // n_tp

    def back(i, carry):
        c = nc - 1 - i
        sl = pl.ds(pl.multiple_of(c * Q, Q), Q)
        bmap, cmap = bcv[sl, :ns], bcv[sl, ns:]
        scores = mm3(cmap, bmap, NT)
        scores_t = mm3(bmap, cmap, NT)
        arow[...] = jnp.zeros((Q, LANES), F32)
        acol[...] = jnp.zeros((LANES, Q), F32)
        dga[...] = jnp.zeros((Q, Q), F32)
        for p in range(pairs):
            ps = slice(p * PAIR, (p + 1) * PAIR)
            g2 = gm[sl, ps]
            cross = mm3(g2, pair_stack(x[sl, ps] * st[sl, ps]), NT)
            both = []
            for i_h, h in enumerate((2 * p, 2 * p + 1)):
                diff = lx[sl, h * HEAD : h * HEAD + 1] - lt[c, h : h + 1, :]
                weighted = jnp.exp(jnp.where(upper, diff, -1e30)) * cross[:, i_h * Q : (i_h + 1) * Q]
                dga[...] += weighted
                term = weighted * scores
                arow[...] += jnp.where(lane == h, jnp.sum(term, axis=1, keepdims=True), 0.0)
                acol[h : h + 1, :] = jnp.sum(term, axis=0, keepdims=True)
                diff_t = lt[c, h : h + 1, :] - lx[sl, h * HEAD : h * HEAD + 1]
                decay_t = jnp.exp(jnp.where(lower, diff_t, -1e30))
                both.append((decay_t * scores_t).astype(BF16))
            dxs[:, ps] = mm(jnp.concatenate(both, axis=1), pair_stack(g2))
        cum = lx[sl, :]
        last = cum[Q - 1 : Q, :]
        grown = jnp.exp(cum)
        to_end = jnp.exp(last - cum)
        rv = rcur[...]
        sv = sst[c]
        gv = gm[sl, :]
        xv = x[sl, :]
        sx = st[sl, :]
        gg = gv * grown
        d_in = mm(bmap, rv) * to_end
        dxt = dxs[...] + d_in
        xt = xv * sx
        per_head = mmh(
            jnp.concatenate([gg * mm(cmap, sv), xt * d_in, xv * dxt], axis=0), to_head
        )
        fixed = mmh(
            jnp.broadcast_to(jnp.sum(rv * sv, axis=0, keepdims=True) * jnp.exp(last), (8, ch)), to_head
        )[0:1]
        swing = per_head[:Q] + arow[...] - jnp.transpose(acol[...])
        dld = mmh(tri_u, swing) + mmh(strict, per_head[Q : 2 * Q]) + fixed
        dstep = per_head[2 * Q :] + dld * neg_c
        slope = sigmoid(raw[:, sl].astype(F32) + dt_col)
        o_gdt[:, sl] = jnp.transpose(dstep)[:heads] * slope
        dgv = dga[...]
        d_b = mm3(jnp.transpose(dgv), cmap) + mm3(xt * to_end, rv, NT)
        d_c = mm3(dgv, bmap) + mm3(gg, sv, NT)
        per = Q // blk
        qs[pl.ds(c * per, per), :, :ns] = d_b.reshape(per, blk, ns)
        qs[pl.ds(c * per, per), :, ns:] = d_c.reshape(per, blk, ns)
        uv = u[sl, :]
        su = sigmoid(uv)
        dus[sl, :] = (sx * dxt + skip_x * gv) * (su * (1.0 + uv * (1.0 - su)))
        rcur[...] = cf[c] + jnp.exp(last) * rv

        @pl.when(i == 0)
        def _():
            o_third()

        @pl.when(i == 1)
        def _():
            g_second()

        return carry

    lax.fori_loop(0, nc, back, 0)

    phase("wait_q")
    def q_copy(k):
        return remote(qs.at[tp_peer(k)], qr.at[my], sm_p, k, "tp", tp_peer(k))

    def a_copy(k):
        return remote(qa.at[my], qa.at[my], sm_a, k, "tp", tp_peer(k))

    edge_x = remote(dus.at[pl.ds(0, 8)], dus.at[pl.ds(rows, 8)], sm_h, 2, "seq", prv)
    edge_b = remote(dub.at[pl.ds(0, 8)], dub.at[pl.ds(rows, 8)], sm_h, 3, "seq", prv)
    for k in range(1, n_tp):
        q_copy(k).start()
    qr[my] = qs[my]
    edge_x.start()
    phase("g_third")
    g_third()
    phase("wait_q2")
    for k in range(1, n_tp):
        q_copy(k).wait_recv()
    phase("qsum")
    qsum = qr[0].astype(F32)
    for j in range(1, n_tp):
        qsum = qsum + qr[j].astype(F32)
    qa[my] = qsum.astype(BF16)
    for k in range(1, n_tp):
        a_copy(k).start()

    phase("o_last")
    o_last()
    phase("g_fourth")
    g_fourth()
    phase("wait_e")
    edge_x.wait_recv()

    phase("convbx")
    def conv_back(ref, weights, out, c):
        base = pl.multiple_of(c * Q, Q)
        ext = ref[pl.ds(base, Q + 8), :]
        tail = jnp.where((c < nc - 1) | (me < n_seq - 1), ext[Q:], 0.0)
        ext = jnp.concatenate([ext[:Q], tail], axis=0)
        acc = weights[3:4, :] * ext[:Q]
        for k in range(3):
            acc = acc + weights[k : k + 1, :] * pltpu.roll(ext, Q + 8 - (3 - k), 0)[:Q]
        out[pl.ds(base, Q), :] = acc

    def conv_back_x(c, carry):
        conv_back(dus, cw, o_gx, c)
        return carry

    lax.fori_loop(0, nc, conv_back_x, 0)

    phase("wait_a")
    for k in range(1, n_tp):
        a_copy(k).wait_recv()
    phase("dub")
    ubv = ub[...]
    sb = sigmoid(ubv)
    dub[pl.ds(0, rows), :] = qa[...].reshape(rows, 2 * ns).astype(F32) * (sb * (1.0 + ubv * (1.0 - sb)))
    edge_b.start()

    phase("convbb")
    edge_b.wait_recv()

    def conv_back_b(c, carry):
        conv_back(dub, cwb, o_gbc, c)
        return carry

    lax.fori_loop(0, nc, conv_back_b, 0)

    phase("g_last")
    g_last()

    phase("drain")
    halo_x.wait_send()
    halo_b.wait_send()
    edge_x.wait_send()
    edge_b.wait_send()
    for k in range(1, n_seq):
        for copy in (t_copy, s_copy, sb_copy, v_copy, vb_copy):
            copy(k).wait_send()
    for k in range(1, n_tp):
        for copy in (r_copy, q_copy, a_copy):
            copy(k).wait_send()
    for copy in w_copies + d_copies + o_copies + g_copies:
        copy.wait_send()
    phase("")


def solution(mesh):
    n_seq, n_tp = mesh.shape["seq"], mesh.shape["tp"]

    def shards(
        inner_x,
        gate_z,
        proj_bc,
        dt_raw,
        a_log,
        dt_bias,
        d_skip,
        conv_x,
        bias_x,
        conv_bc,
        bias_bc,
        norm_gain,
        w_out,
        d_out,
    ):
        rows, ch = inner_x.shape
        heads = a_log.shape[0]
        ns2 = proj_bc.shape[1]
        ns = ns2 // 2
        nc = rows // Q
        nrow = ns // n_seq
        wrows, drows = w_out.shape[1], d_out.shape[1]
        width = wrows * n_seq
        w_t = w_out.T
        d_t = d_out.T

        vm = functools.partial(pl.BlockSpec, memory_space=pltpu.VMEM)
        big = pltpu.VMEM((rows, ch), F32)
        chunk_states = pltpu.VMEM((nc, ns, ch), F32)
        slices = pltpu.VMEM((n_seq, nrow, ch), F32)
        sem_s = pltpu.SemaphoreType.DMA((2, n_seq))
        sem_t = pltpu.SemaphoreType.DMA((2, n_tp))
        scratch = [
            pltpu.VMEM((4, 4, wrows, ch), BF16),
            pltpu.VMEM((width, rows), BF16),
            pltpu.VMEM((16, ch), BF16),
            pltpu.VMEM((16, ns2), BF16),
            pltpu.VMEM((8, LANES), F32),
            pltpu.VMEM((n_seq, 8, LANES), F32),
            big,
            big,
            pltpu.VMEM((nc, heads, Q), F32),
            big,
            big,
            pltpu.VMEM((rows, ns2), F32),
            pltpu.VMEM((rows, ns2), F32),
            chunk_states,
            chunk_states,
            chunk_states,
            big,
            big,
            big,
            big,
            pltpu.VMEM((rows, ch), BF16),
            pltpu.VMEM((Q, ch), F32),
            pltpu.VMEM((rows + 8, ch), F32),
            pltpu.VMEM((rows + 8, ns2), F32),
            pltpu.VMEM((ns, ch), F32),
            slices,
            slices,
            slices,
            slices,
            slices,
            slices,
            slices,
            slices,
            pltpu.VMEM((8, rows), F32),
            pltpu.VMEM((n_tp, 8, rows), F32),
            pltpu.VMEM((4, 2, drows, rows), BF16),
            pltpu.VMEM((4, drows, rows), BF16),
            pltpu.VMEM((drows, rows), BF16),
            pltpu.VMEM((2, drows, rows), BF16),
            pltpu.VMEM((4, 4, wrows, ch), BF16),
            *[
                pltpu.VMEM(shape, BF16)
                for shape in 2
                * [
                    (4, wrows // 2, ch),
                    (2, 4, wrows // 2, ch),
                    (wrows // 2, ch),
                    (2, wrows // 2, ch),
                ]
            ],
            pltpu.VMEM((n_tp, rows // n_tp, ns2), F32),
            pltpu.VMEM((n_tp, rows // n_tp, ns2), F32),
            pltpu.VMEM((n_tp, rows // n_tp, ns2), BF16),
            pltpu.VMEM((Q, LANES), F32),
            pltpu.VMEM((LANES, Q), F32),
            pltpu.VMEM((Q, Q), F32),
            pltpu.VMEM((rows, 1), F32),
            pltpu.SemaphoreType.DMA((2,)),
            pltpu.SemaphoreType.DMA((2, 4)),
            sem_s,
            sem_s,
            sem_t,
            sem_s,
            sem_s,
            sem_s,
            sem_s,
            sem_t,
            sem_t,
            sem_s,
            sem_t,
            sem_t,
        ]
        out_t, g_x, g_z, g_bc, g_dt, g_w = pl.pallas_call(
            functools.partial(kernel, (n_seq, n_tp, ch * n_tp)),
            out_shape=[
                jax.ShapeDtypeStruct((drows, rows), BF16),
                jax.ShapeDtypeStruct((rows, ch), F32),
                jax.ShapeDtypeStruct((rows, ch), F32),
                jax.ShapeDtypeStruct((rows, ns2), F32),
                jax.ShapeDtypeStruct((heads, rows), F32),
                jax.ShapeDtypeStruct((wrows, ch), F32),
            ],
            in_specs=[vm()] * 14,
            out_specs=[vm()] * 6,
            scratch_shapes=scratch,
            compiler_params=pltpu.CompilerParams(
                collective_id=0, has_side_effects=True, vmem_limit_bytes=67_043_328
            ),
            name="mixer",
        )(
            inner_x,
            gate_z,
            proj_bc,
            dt_raw.T,
            w_t,
            d_t,
            conv_x,
            bias_x.reshape(-1, LANES),
            conv_bc,
            bias_bc[None, :],
            norm_gain.reshape(-1, LANES),
            a_log[None, :],
            dt_bias[None, :],
            d_skip[None, :],
        )
        return out_t.T, g_x, g_z, g_bc, g_dt.T, g_w.T

    in_specs = (
        P("seq", "tp"),
        P("seq", "tp"),
        P("seq", None),
        P("seq", "tp"),
        P("tp"),
        P("tp"),
        P("tp"),
        P(None, "tp"),
        P("tp"),
        P(),
        P(),
        P("tp"),
        P("tp", "seq"),
        P("seq", "tp"),
    )
    out_specs = (
        P("seq", "tp"),
        P("seq", "tp"),
        P("seq", "tp"),
        P("seq", None),
        P("seq", "tp"),
        P("tp", "seq"),
    )
    return jax.shard_map(
        shards, mesh=mesh, in_specs=in_specs, out_specs=out_specs, check_vma=False
    )
```

```python
import functools

import jax
import jax.numpy as jnp
from jax import lax
from jax.experimental import pallas as pl
from jax.experimental.pallas import tpu as pltpu
from jax.sharding import PartitionSpec as P

MESH = pl.DeviceIdType.MESH
F32 = jnp.float32
BF16 = jnp.bfloat16
HIGH = lax.Precision.HIGHEST
EPSILON = 1e-05
NN = ((1,), (0,))
NT = ((1,), (1,))
Q = 128
PAIR = 128
HEAD = 64
LANES = 128


def mm(a, b, dims=NN):
    return lax.dot_general(a.astype(BF16), b.astype(BF16), (dims, ((), ())), preferred_element_type=F32)


def mmh(a, b, dims=NN):
    return lax.dot_general(
        a.astype(F32), b.astype(F32), (dims, ((), ())), precision=HIGH, preferred_element_type=F32
    )


def halves(v):
    high = v.astype(BF16)
    return high, (v - high.astype(F32)).astype(BF16)


def mm3(a, b, dims=NN):
    a0, a1 = halves(a)
    b0, b1 = halves(b)
    return mm(a0, b0, dims) + (mm(a1, b0, dims) + mm(a0, b1, dims))


def parts(v, count):
    out = []
    for _ in range(count):
        piece = v.astype(BF16)
        out.append(piece)
        v = v - piece.astype(F32)
    return out


def iota(shape, dim):
    return lax.broadcasted_iota(jnp.int32, shape, dim)


def sigmoid(v):
    return 1.0 / (1.0 + jnp.exp(-v))


def softplus(v):
    return jnp.maximum(v, 0.0) + jnp.log1p(jnp.exp(-jnp.abs(v)))


def pair_stack(v):
    lane = iota(v.shape, 1)
    return jnp.concatenate(
        [jnp.where(lane < HEAD, v, 0.0), jnp.where(lane >= HEAD, v, 0.0)], axis=0
    )


def kernel(
    sizes,
    ix_in,
    gz_in,
    bc_in,
    raw_in,
    wt,
    dt,
    cw_in,
    bx_in,
    cwb_in,
    bb_in,
    gain_in,
    al_in,
    db_in,
    ds_in,
    out_hbm,
    gx_hbm,
    gz_hbm,
    gbc_hbm,
    gdt_hbm,
    gw_hbm,
    o_out,
    o_gx,
    o_gz,
    o_gbc,
    o_gdt,
    o_gw,
    ix,
    gz,
    bc,
    raw,
    cw,
    bx,
    cwb,
    bb,
    gain,
    al,
    db,
    ds,
    wfull,
    dfull,
    hx,
    hb,
    dsend,
    dbuf,
    st,
    lx,
    lt,
    u,
    x,
    ub,
    bcv,
    fr,
    sst,
    cf,
    y,
    gated,
    gn,
    gm,
    nb,
    dus,
    dub,
    rcur,
    se,
    sr,
    en,
    sin,
    re,
    rr,
    ren,
    rin,
    ts,
    tr,
    pb,
    pp,
    po1,
    po2,
    gb,
    ga1,
    ga2,
    ga3,
    ga4,
    gb1,
    gb2,
    gb3,
    gb4,
    qs,
    qm,
    qr,
    rst,
    qa,
    arow,
    acol,
    dga,
    invs,
    swings,
    dmap,
    edge,
    sm_m,
    sm_e,
    sm_l,
    sm_h,
    sm_d,
    sm_w,
    sm_g,
    sm_s,
    sm_b,
    sm_r,
    sm_q,
    sm_t,
    sm_o,
    sm_v,
    sm_p,
    sm_a,
):
    n_seq, n_tp, inner = sizes
    rows, ch = ix.shape
    nc = rows // Q
    heads = raw.shape[0]
    pairs = ch // PAIR
    ns = bc.shape[1] // 2
    me, my = lax.axis_index("seq"), lax.axis_index("tp")
    wrows = wt.shape[0]
    drows = 2 * dt.shape[1]
    nrow = ns // n_seq

    scope = []

    def phase(name):
        if scope:
            scope.pop().__exit__(None, None, None)
        if name:
            scope.append(jax.named_scope(name))
            scope[0].__enter__()

    side = 4
    zi, xi = lax.div(me, side), lax.rem(me, side)
    yi, core = lax.div(my, 2), lax.rem(my, 2)

    def step(v, k):
        return lax.rem(v + k + side, side)

    x_up, x_dn = step(xi, 1), step(xi, -1)
    z_up, z_dn = step(zi, 1), step(zi, -1)
    y_up, y_dn = step(yi, 1), step(yi, -1)
    x_far, z_far, y_far = step(xi, 2), step(zi, 2), step(yi, 2)
    to_xu, to_xd = zi * side + x_up, zi * side + x_dn
    to_zu, to_zd = z_up * side + xi, z_dn * side + xi
    to_yu, to_yd = y_up * 2 + core, y_dn * 2 + core
    mate = yi * 2 + 1 - core

    def seq_peer(k):
        return lax.rem(me + k, n_seq)

    def tp_peer(k):
        return lax.rem(my + k, n_tp)

    phase("barrier1")
    barrier = pltpu.get_barrier_semaphore()
    for k in range(1, n_seq):
        pl.semaphore_signal(barrier, inc=1, device_id={"seq": seq_peer(k)}, device_id_type=MESH)
    for k in range(1, n_tp):
        pl.semaphore_signal(barrier, inc=1, device_id={"tp": tp_peer(k)}, device_id_type=MESH)

    def remote(src, dst, sems, k, axis, peer):
        return pltpu.make_async_remote_copy(
            src_ref=src,
            dst_ref=dst,
            send_sem=sems.at[0, k],
            recv_sem=sems.at[1, k],
            device_id={axis: peer},
            device_id_type=MESH,
        )

    nxt, prv = seq_peer(1), seq_peer(n_seq - 1)

    @pl.when(my > 0)
    def _():
        pl.semaphore_signal(barrier, inc=1, device_id={"seq": nxt, "tp": 0}, device_id_type=MESH)

    staged = [
        (raw_in, raw),
        (al_in, al),
        (db_in, db),
        (ds_in, ds),
        (wt, wfull.at[zi, xi]),
        (dt, dfull.at[yi, pl.ds(2 * core, 2)]),
        (ix_in, ix),
        (bc_in, bc),
        (cw_in, cw),
        (bx_in, bx),
        (cwb_in, cwb),
        (bb_in, bb),
        (gain_in, gain),
        (gz_in, gz),
    ]
    loads = [pltpu.make_async_copy(a, b, sm_l.at[i]) for i, (a, b) in enumerate(staged)]
    for load in loads:
        load.start()
    results = [(o_gz, gz_hbm), (o_out, out_hbm), (o_gx, gx_hbm), (o_gw, gw_hbm), (o_gbc, gbc_hbm), (o_gdt, gdt_hbm)]
    stores = [pltpu.make_async_copy(a, b, sm_l.at[14 + i]) for i, (a, b) in enumerate(results)]
    phase("staging")
    for load in loads[:9]:
        load.wait()
    phase("barrier")
    pl.semaphore_wait(barrier, n_seq + n_tp - 2 + jnp.where(my == 0, n_tp - 1, 0))

    phase("start")
    halo_x = remote(ix.at[pl.ds(rows - 16, 16)], hx, sm_h, 0, "seq", nxt)
    halo_b = remote(bc.at[pl.ds(rows - 16, 16)], hb, sm_h, 1, "seq", nxt)
    halo_x.start()
    halo_b.start()

    half = wrows // 2
    near = 48
    ra, rb = pl.ds(0, half), pl.ds(half, half)
    ra1, ra2 = pl.ds(0, near), pl.ds(near, half - near)
    rb1, rb2 = pl.ds(half, near), pl.ds(half + near, half - near)
    lo, hi, every = pl.ds(0, 2), pl.ds(2, 2), pl.ds(0, side)

    def w_view(z, x, r):
        return wfull.at[z, x, r]

    def w_move(i, peer, z, x, r, src=None):
        return remote(w_view(z, x, r) if src is None else src, w_view(z, x, r), sm_w, i, "seq", peer)

    w_copies = [
        w_move(0, to_xu, zi, xi, ra),
        w_move(1, to_xd, zi, xi, ra),
        w_move(2, to_zu, zi, xi, rb),
        w_move(3, to_zd, zi, xi, rb),
        w_move(4, to_zu, zi, xi, ra),
        w_move(5, to_zd, zi, xi, ra),
        w_move(6, to_xu, zi, xi, rb),
        w_move(7, to_xd, zi, xi, rb),
        w_move(8, to_xu, zi, x_dn, ra1),
        w_move(9, to_xd, zi, x_up, ra2),
        w_move(10, to_zu, z_dn, xi, rb1),
        w_move(11, to_zd, z_up, xi, rb2),
        w_move(12, to_zu, zi, x_up, ra),
        w_move(13, to_zd, zi, x_up, ra),
        w_move(14, to_xu, z_up, xi, rb),
        w_move(15, to_xd, z_up, xi, rb),
        w_move(16, to_zu, zi, x_dn, ra),
        w_move(17, to_zd, zi, x_dn, ra),
        w_move(18, to_xu, z_dn, xi, rb),
        w_move(19, to_xd, z_dn, xi, rb),
        w_move(20, to_zu, zi, x_far, ra),
        w_move(21, to_zd, zi, x_far, ra),
        w_move(22, to_xu, z_far, xi, rb),
        w_move(23, to_xd, z_far, xi, rb),
        w_move(24, to_zu, z_dn, lo, ra),
        w_move(25, to_zd, z_up, hi, ra),
        w_move(26, to_xu, lo, x_dn, rb),
        w_move(27, to_xd, hi, x_up, rb),
    ]

    dhalf = drows // 2

    def d_view(y, c, off=0, size=drows):
        if size == drows:
            return dfull.at[y, pl.ds(2 * c, 2)]
        return dfull.at[y, 2 * c + off // size]

    def d_move(i, peer, y, c, off=0, size=drows, src=None):
        view = d_view(y, c, off, size)
        return remote(view if src is None else src, view, sm_g, i, "tp", peer)

    d_copies = [
        d_move(0, to_yu, yi, core),
        d_move(1, to_yd, yi, core),
        d_move(2, mate, yi, core),
        d_move(3, to_yu, y_dn, core, 0, dhalf),
        d_move(4, to_yd, y_up, core, dhalf, dhalf),
        d_move(5, mate, y_dn, core),
        d_move(6, mate, y_up, core),
        d_move(7, mate, y_far, core),
    ]

    def start(copies, first, last):
        for copy in copies[first:last]:
            copy.start()

    def arrived(copies, first, last):
        for copy in copies[first:last]:
            copy.wait_recv()

    start(w_copies, 0, 8)
    start(d_copies, 0, 3)

    phase("steps")
    def spread_of(first):
        return (iota((LANES, ch), 1) // HEAD + first == iota((LANES, ch), 0)).astype(BF16)

    ident = (iota((heads, heads), 0) == iota((heads, heads), 1)).astype(F32)
    spread_s = jnp.concatenate([spread_of(0)] * 3, axis=0)
    spread_l = jnp.concatenate([spread_of(16)] * 3, axis=0)
    spread_h = spread_of(0)[:heads].astype(F32)
    negexp = -jnp.exp(al[...])
    skip_x = mmh(jnp.broadcast_to(ds[...], (8, heads)), spread_h)[0:1]
    tri_u = (iota((Q, Q), 0) <= iota((Q, Q), 1)).astype(F32)

    def column(v):
        return mmh(ident, jnp.broadcast_to(v, (8, heads)), NT)[:, 0:1]

    def in_line(ref):
        return jnp.concatenate([ref[i : i + 1] for i in range(ref.shape[0])], axis=1)

    dt_col, neg_col = column(db[...]), column(negexp)

    for load in loads[9:]:
        load.wait()
    bias_line, gain_line = in_line(bx), in_line(gain)

    def steps(c, total):
        sl = pl.ds(pl.multiple_of(c * Q, Q), Q)
        s_c = softplus(raw[:, sl].astype(F32) + dt_col)
        cum = mmh(s_c * neg_col, tri_u)
        lt[c] = cum
        stacked = jnp.concatenate(
            [
                s_c,
                jnp.zeros((16 - heads, Q), F32),
                cum,
                jnp.zeros((LANES - 16 - heads, Q), F32),
            ],
            axis=0,
        )
        turned = jnp.transpose(stacked)
        pieces = jnp.concatenate(parts(turned, 3), axis=1)
        st[sl, :] = mm(pieces, spread_s)
        lx[sl, :] = mm(pieces, spread_l)
        return total + turned[Q - 1 : Q, :]

    total = lax.fori_loop(0, nc, steps, jnp.zeros((1, LANES), F32))
    dsend[...] = jnp.broadcast_to(total, (8, LANES))
    dbuf[me] = dsend[...]

    def t_copy(k):
        return remote(dsend, dbuf.at[me], sm_d, k, "seq", seq_peer(k))

    for k in range(1, n_seq):
        t_copy(k).start()

    phase("convs")
    def conv_of(ref, halo, weights, bias, c):
        base = pl.multiple_of(c * Q, Q)
        own = ref[pl.ds(base, Q), :].astype(F32)
        if halo is None:
            head = ref[pl.ds(pl.multiple_of(c * Q - 16, 16), 16), :].astype(F32)[8:16]
        else:
            head = jnp.where(me > 0, halo[...].astype(F32), 0.0)[8:16]
        ext = jnp.concatenate([head, own], axis=0)
        acc = bias + weights[3:4, :] * own
        for k in range(3):
            acc = acc + weights[k : k + 1, :] * pltpu.roll(ext, Q + 8 - (5 + k), 0)[:Q]
        return acc

    def convs(c, carry, edge_of=(None, None)):
        sl = pl.ds(pl.multiple_of(c * Q, Q), Q)
        vb = conv_of(bc, edge_of[0], cwb, bb[...], c)
        ub[sl, :] = vb
        pbc = vb * sigmoid(vb)
        bcv[sl, :] = pbc
        vx = conv_of(ix, edge_of[1], cw, bias_line, c)
        u[sl, :] = vx
        xv = vx * sigmoid(vx)
        x[sl, :] = xv
        cum = lx[sl, :]
        to_end = jnp.exp(cum[Q - 1 : Q, :] - cum)
        b_t = jnp.transpose(pbc[:, :ns])
        fresh = mm3(b_t, xv * st[sl, :] * to_end)
        fr[c] = fresh
        return carry

    lax.fori_loop(1, nc, convs, 0)
    phase("wait_halo")
    halo_x.wait_recv()
    halo_b.wait_recv()
    phase("conv0")
    convs(0, 0, (hb, hx))
    end = fr[0]
    for c in range(1, nc):
        end = jnp.exp(lx[pl.ds(c * Q + Q - 1, 1), :]) * end + fr[c]
    se[...] = end.reshape(n_seq, nrow, ch)

    phase("send_s")
    def s_copy(k):
        return remote(se.at[seq_peer(k)], sr.at[me], sm_s, k, "seq", seq_peer(k))

    def sb_copy(k):
        return remote(en.at[seq_peer(k)], sin.at[me], sm_b, k, "seq", seq_peer(k))

    for k in range(1, n_seq):
        s_copy(k).start()
    sr[me] = se[me]
    phase("wait_w1")
    arrived(w_copies, 0, 4)
    start(w_copies, 8, 20)

    upper = iota((Q, Q), 0) >= iota((Q, Q), 1)
    lower = iota((Q, Q), 0) <= iota((Q, Q), 1)

    phase("inside")
    def inside(c, carry):
        sl = pl.ds(pl.multiple_of(c * Q, Q), Q)
        scores = mm3(bcv[sl, ns:], bcv[sl, :ns], NT)
        for p in range(pairs):
            ps = slice(p * PAIR, (p + 1) * PAIR)
            both = []
            for h in (2 * p, 2 * p + 1):
                diff = lx[sl, h * HEAD : h * HEAD + 1] - lt[c, h : h + 1, :]
                decay = jnp.exp(jnp.where(upper, diff, -1e30))
                both.append(decay * scores)
            y[sl, ps] = mm3(jnp.concatenate(both, axis=1), pair_stack(x[sl, ps] * st[sl, ps]))
        return carry

    lax.fori_loop(0, nc, inside, 0)
    phase("wait_w2")
    arrived(w_copies, 8, 12)
    start(w_copies, 20, 24)
    phase("wait_d1")
    arrived(d_copies, 0, 2)
    start(d_copies, 3, 7)

    phase("wait_s")
    for k in range(1, n_seq):
        t_copy(k).wait_recv()
    for k in range(1, n_seq):
        s_copy(k).wait_recv()
    phase("scan")
    fade = jnp.exp(mm(jnp.concatenate(parts(dbuf[:, 0, :], 3), axis=1), spread_l))

    acc = jnp.zeros((nrow, ch), F32)
    for j in range(n_seq):
        en[j] = acc
        acc = fade[j : j + 1] * acc + sr[j]
    for k in range(1, n_seq):
        sb_copy(k).start()
    sin[me] = en[me]

    phase("wait_d2")
    arrived(d_copies, 3, 5)
    start(d_copies, 7, 8)
    phase("wait_w3")
    arrived(w_copies, 4, 8)
    arrived(w_copies, 12, 24)
    start(w_copies, 24, 28)
    phase("wait_sb")
    for k in range(1, n_seq):
        sb_copy(k).wait_recv()
    phase("combine")
    lane = iota((Q, LANES), 1)

    def to_row(i, c, v):
        ts[i, :, pl.ds(pl.multiple_of(c * Q, Q), Q)] = jnp.transpose(jnp.where(lane == 0, v, 0.0))[:8]

    def to_column(row, c):
        block = jnp.concatenate([row[:, c * Q : (c + 1) * Q], jnp.zeros((Q - 8, Q), F32)], axis=0)
        return jnp.transpose(block)[:, 0:1]

    def combine(c, state):
        sl = pl.ds(pl.multiple_of(c * Q, Q), Q)
        sst[c] = state
        cum = lx[sl, :]
        mixed = y[sl, :] + jnp.exp(cum) * mm3(bcv[sl, ns:], state) + skip_x * x[sl, :]
        y[sl, :] = mixed
        zv = gz[sl, :].astype(F32)
        gv = mixed * zv * sigmoid(zv)
        gated[sl, :] = gv
        to_row(0, c, jnp.sum(gv * gv, axis=1, keepdims=True))
        return jnp.exp(cum[Q - 1 : Q, :]) * state + fr[c]

    lax.fori_loop(0, nc, combine, sin[...].reshape(ns, ch))

    def r_copies(i):
        return [
            remote(ts.at[i], tr.at[i, my], sm_t, i * n_tp + k, "tp", tp_peer(k)) for k in range(1, n_tp)
        ]

    def r_total(i):
        total = tr[i, 0]
        for j in range(1, n_tp):
            total = total + tr[i, j]
        return total

    r_squares, r_inner = r_copies(0), r_copies(1)
    start(r_squares, 0, n_tp - 1)
    tr[0, my] = ts[0]

    phase("wait_d")
    arrived(d_copies, 2, 3)
    arrived(d_copies, 5, 8)
    phase("gn")
    kb = wrows * side

    def gn_add(part, first):
        @pl.when(first)
        def _():
            gn[...] = part

        @pl.when(jnp.logical_not(first))
        def _():
            gn[...] += part

    def gn_early(k, carry):
        zz, xx = step(zi, k - 1), step(xi, k - 1)
        d_rows = jnp.concatenate(
            [dfull[zz, :, ra].reshape(kb // 2, rows), dfull[:, xx, rb].reshape(kb // 2, rows)], axis=0
        )
        w_rows = jnp.concatenate(
            [wfull[zz, :, ra].reshape(kb // 2, ch), wfull[:, xx, rb].reshape(kb // 2, ch)], axis=0
        )
        gn_add(mm(jnp.transpose(d_rows), w_rows), k == 0)
        return carry

    lax.fori_loop(0, 3, gn_early, 0)

    phase("wait_ss")
    arrived(r_squares, 0, n_tp - 1)
    inv_row = lax.rsqrt(r_total(0) / inner + EPSILON)
    phase("nb")
    for c in range(nc):
        sl = pl.ds(c * Q, Q)
        inv = to_column(inv_row, c)
        invs[sl, :] = inv
        nb[sl, :] = (gated[sl, :] * inv * gain_line).astype(BF16)
    phase("gradw")
    g_copies = [
        remote(gb.at[z_far, lo, ra], ga1.at[lo], sm_v, 0, "seq", to_zu),
        remote(gb.at[z_far, hi, ra], ga1.at[hi], sm_v, 1, "seq", to_zd),
        remote(gb.at[lo, x_far, rb], gb1.at[lo], sm_v, 2, "seq", to_xu),
        remote(gb.at[hi, x_far, rb], gb1.at[hi], sm_v, 3, "seq", to_xd),
        remote(gb.at[z_up, hi, ra], ga2.at[0, hi], sm_v, 4, "seq", to_zu),
        remote(gb.at[z_dn, lo, ra], ga2.at[1, lo], sm_v, 5, "seq", to_zd),
        remote(gb.at[hi, x_up, rb], gb2.at[0, hi], sm_v, 6, "seq", to_xu),
        remote(gb.at[lo, x_dn, rb], gb2.at[1, lo], sm_v, 7, "seq", to_xd),
        remote(gb.at[z_up, lo, ra], ga2.at[0, lo], sm_v, 8, "seq", to_zu),
        remote(gb.at[z_dn, hi, ra], ga2.at[1, hi], sm_v, 9, "seq", to_zd),
        remote(gb.at[lo, x_up, rb], gb2.at[0, lo], sm_v, 10, "seq", to_xu),
        remote(gb.at[hi, x_dn, rb], gb2.at[1, hi], sm_v, 11, "seq", to_xd),
        remote(gb.at[zi, x_far, ra1], ga3.at[ra1], sm_v, 12, "seq", to_xu),
        remote(gb.at[zi, x_far, ra2], ga3.at[ra2], sm_v, 13, "seq", to_xd),
        remote(gb.at[z_far, xi, rb1], gb3.at[ra1], sm_v, 14, "seq", to_zu),
        remote(gb.at[z_far, xi, rb2], gb3.at[ra2], sm_v, 15, "seq", to_zd),
        remote(gb.at[zi, x_up, ra], ga4.at[0], sm_v, 16, "seq", to_xu),
        remote(gb.at[zi, x_dn, ra], ga4.at[1], sm_v, 17, "seq", to_xd),
        remote(gb.at[z_up, xi, rb], gb4.at[0], sm_v, 18, "seq", to_zu),
        remote(gb.at[z_dn, xi, rb], gb4.at[1], sm_v, 19, "seq", to_zd),
    ]

    def plus(ref, index, *others):
        total = ref[index].astype(F32)
        for part in others:
            total = total + part.astype(F32)
        ref[index] = total.astype(BF16)

    def g_block(k, carry):
        b = step(zi, 2 + k)
        gb[b] = mm(dfull[b].reshape(kb, rows), nb[...]).astype(BF16).reshape(side, wrows, ch)

        @pl.when(k == 0)
        def _():
            start(g_copies, 0, 2)

        return carry

    lax.fori_loop(0, side, g_block, 0)
    start(g_copies, 2, 8)

    def g_second():
        arrived(g_copies, 0, 4)
        for j in range(2):
            plus(gb, (z_up, j, ra), ga1[j])
            plus(gb, (z_dn, 2 + j, ra), ga1[2 + j])
            plus(gb, (j, x_up, rb), gb1[j])
            plus(gb, (2 + j, x_dn, rb), gb1[2 + j])
        start(g_copies, 8, 12)

    def g_third():
        arrived(g_copies, 4, 12)
        for j in range(side):
            plus(gb, (zi, j, ra), ga2[0, j], ga2[1, j])
            plus(gb, (j, xi, rb), gb2[0, j], gb2[1, j])
        start(g_copies, 12, 16)

    def g_fourth():
        arrived(g_copies, 12, 16)
        plus(gb, (zi, x_up, ra1), ga3[ra1])
        plus(gb, (zi, x_dn, ra2), ga3[ra2])
        plus(gb, (z_up, xi, rb1), gb3[ra1])
        plus(gb, (z_dn, xi, rb2), gb3[ra2])
        start(g_copies, 16, 20)

    def g_last():
        arrived(g_copies, 16, 20)
        o_gw[ra, :] = gb[zi, xi, ra].astype(F32) + ga4[0].astype(F32) + ga4[1].astype(F32)
        o_gw[rb, :] = gb[zi, xi, rb].astype(F32) + gb4[0].astype(F32) + gb4[1].astype(F32)

    def o_second():
        arrived(o_copies, 0, 1)
        for j in range(side):
            plus(pb, (j, core), pp[j])
        start(o_copies, 1, 3)

    def o_third():
        arrived(o_copies, 1, 3)
        plus(pb, (y_up, core, o_half1), po1[o_half1])
        plus(pb, (y_dn, core, o_half2), po1[o_half2])
        start(o_copies, 3, 5)

    def o_last():
        arrived(o_copies, 3, 5)
        total = pb[yi, core].astype(F32) + po2[0].astype(F32) + po2[1].astype(F32)
        o_out[...] = total.astype(BF16)
    phase("wait_w4")
    arrived(w_copies, 24, 28)
    phase("gn_last")
    gn_early(3, 0)
    phase("ip")

    def inner_sums(c, carry):
        sl = pl.ds(pl.multiple_of(c * Q, Q), Q)
        scaled = gn[sl, :] * gain_line
        gn[sl, :] = scaled
        to_row(1, c, jnp.sum(scaled * gated[sl, :], axis=1, keepdims=True))
        return carry

    lax.fori_loop(0, nc, inner_sums, 0)
    start(r_inner, 0, n_tp - 1)
    tr[1, my] = ts[1]
    phase("outmm")
    def share(y0, c0):
        block = wfull[y0, pl.ds(2 * c0, 2)].reshape(drows, ch)
        pb[y0, c0] = mm(block, nb[...], NT).astype(BF16)

    def other(j, carry):
        share(j, 1 - core)
        return carry

    def same(j, carry):
        share(j, core)
        return carry

    o_half1, o_half2 = pl.ds(0, dhalf), pl.ds(dhalf, dhalf)
    o_copies = [
        remote(pb.at[every, 1 - core], pp, sm_o, 0, "tp", mate),
        remote(pb.at[y_far, core, o_half1], po1.at[o_half1], sm_o, 1, "tp", to_yu),
        remote(pb.at[y_far, core, o_half2], po1.at[o_half2], sm_o, 2, "tp", to_yd),
        remote(pb.at[y_up, core], po2.at[0], sm_o, 3, "tp", to_yu),
        remote(pb.at[y_dn, core], po2.at[1], sm_o, 4, "tp", to_yd),
    ]
    lax.fori_loop(0, side, other, 0)
    start(o_copies, 0, 1)
    lax.fori_loop(0, side, same, 0)
    phase("wait_ip")
    arrived(r_inner, 0, n_tp - 1)
    ip_row = r_total(1) / inner * inv_row * inv_row * inv_row
    phase("norm")
    for c in range(nc):
        sl = pl.ds(c * Q, Q)
        gg = invs[sl, :] * gn[sl, :] - gated[sl, :] * to_column(ip_row, c)
        zv = gz[sl, :].astype(F32)
        sg = sigmoid(zv)
        o_gz[sl, :] = gg * y[sl, :] * sg * (1.0 + zv * (1.0 - sg))
        gmv = gg * zv * sg
        gm[sl, :] = gmv
        c_t = jnp.transpose(bcv[sl, ns:])
        cf[c] = mm3(c_t, gmv * jnp.exp(lx[sl, :]))

    racc = cf[nc - 1]
    for c in reversed(range(nc - 1)):
        racc = cf[c] + jnp.exp(lx[pl.ds(c * Q + Q - 1, 1), :]) * racc
    re[...] = racc.reshape(n_seq, nrow, ch)

    phase("send_v")
    def v_copy(k):
        return remote(re.at[seq_peer(k)], rr.at[me], sm_r, k, "seq", seq_peer(k))

    def vb_copy(k):
        return remote(ren.at[seq_peer(k)], rin.at[me], sm_q, k, "seq", seq_peer(k))

    for k in range(1, n_seq):
        v_copy(k).start()
    rr[me] = re[me]
    stores[0].start()
    phase("g_second")
    g_second()
    phase("o_second")
    o_second()
    phase("intra")
    def back_inside(c, carry):
        sl = pl.ds(pl.multiple_of(c * Q, Q), Q)
        bmap, cmap = bcv[sl, :ns], bcv[sl, ns:]
        scores = mm3(cmap, bmap, NT)
        scores_t = mm3(bmap, cmap, NT)
        arow[...] = jnp.zeros((Q, LANES), F32)
        acol[...] = jnp.zeros((LANES, Q), F32)
        dga[...] = jnp.zeros((Q, Q), F32)
        for p in range(pairs):
            ps = slice(p * PAIR, (p + 1) * PAIR)
            g2 = gm[sl, ps]
            cross = mm3(g2, pair_stack(x[sl, ps] * st[sl, ps]), NT)
            both = []
            for i_h, h in enumerate((2 * p, 2 * p + 1)):
                diff = lx[sl, h * HEAD : h * HEAD + 1] - lt[c, h : h + 1, :]
                weighted = jnp.exp(jnp.where(upper, diff, -1e30)) * cross[:, i_h * Q : (i_h + 1) * Q]
                dga[...] += weighted
                term = weighted * scores
                arow[...] += jnp.where(lane == h, jnp.sum(term, axis=1, keepdims=True), 0.0)
                acol[h : h + 1, :] = jnp.sum(term, axis=0, keepdims=True)
                decay_t = jnp.exp(jnp.where(lower, lt[c, h : h + 1, :] - lx[sl, h * HEAD : h * HEAD + 1], -1e30))
                both.append((decay_t * scores_t).astype(BF16))
            y[sl, ps] = mm(jnp.concatenate(both, axis=1), pair_stack(g2))
        dgv = dga[...]
        swings[c] = arow[...] - jnp.transpose(acol[...])
        dmap[sl, :ns] = mm3(jnp.transpose(dgv), cmap)
        dmap[sl, ns:] = mm3(dgv, bmap)
        return carry

    def back_insides(first):
        def one(i, carry):
            return back_inside(first - i, carry)

        lax.fori_loop(0, nc // 2, one, 0)

    back_insides(nc - 1)
    back_insides(nc // 2 - 1)

    phase("wait_v")
    for k in range(1, n_seq):
        v_copy(k).wait_recv()
    acc = jnp.zeros((nrow, ch), F32)
    for j in reversed(range(n_seq)):
        ren[j] = acc
        acc = fade[j : j + 1] * acc + rr[j]
    for k in range(1, n_seq):
        vb_copy(k).start()
    rin[me] = ren[me]
    phase("o_third")
    o_third()
    phase("forward_part")
    to_head = (lax.rem(iota((2 * ch, LANES), 0), ch) // HEAD == iota((2 * ch, LANES), 1)).astype(BF16)
    neg_c = jnp.concatenate([negexp, jnp.zeros((1, LANES - heads), F32)], axis=1)
    blk = Q // n_tp
    tail_sum = jnp.concatenate([tri_u.astype(BF16)] * 3, axis=1)
    head_sum = jnp.concatenate([(iota((Q, Q), 0) > iota((Q, Q), 1)).astype(BF16)] * 3, axis=1)

    def by_head(v):
        return mm(jnp.concatenate(parts(v, 2), axis=1), to_head)

    def reads(c, carry):
        sl = pl.ds(pl.multiple_of(c * Q, Q), Q)
        cmap = bcv[sl, ns:]
        sv = sst[c]
        gg = gm[sl, :] * jnp.exp(lx[sl, :])
        dmap[sl, ns:] += mm3(gg, sv, NT)
        swings[c] += by_head(gg * mm(cmap, sv))
        return carry

    lax.fori_loop(0, nc, reads, 0)
    phase("g_third")
    g_third()


    phase("wait_vb")
    for k in range(1, n_seq):
        vb_copy(k).wait_recv()
    phase("inter")
    rcur[...] = rin[...].reshape(ns, ch)
    def m_copy(c):
        return remote(qs.at[c, every, 1 - core], qm.at[c], sm_m, c, "tp", mate)

    def q_copy(c, k):
        y1 = step(yi, k)
        return remote(qs.at[c, y1, core], qr.at[c, yi], sm_p, c * side + k, "tp", y1 * 2 + core)

    def q_send(c):
        m_copy(c).wait_recv()
        for j in range(side):
            qs[c, j, core] += qm[c, j]
        for k in range(1, side):
            q_copy(c, k).start()
        qr[c, yi] = qs[c, yi, core]

    def back_b(i, carry):
        c = nc - 1 - i
        sl = pl.ds(pl.multiple_of(c * Q, Q), Q)
        cum = lx[sl, :]
        last = cum[Q - 1 : Q, :]
        rv = rcur[...]
        rst[c] = rv
        d_b = dmap[sl, :ns] + mm3(x[sl, :] * st[sl, :] * jnp.exp(last - cum), rv, NT)
        qs[c, :, :, :, :ns] = d_b.reshape(side, 2, blk, ns)
        qs[c, :, :, :, ns:] = dmap[sl, ns:].reshape(side, 2, blk, ns)
        rcur[...] = cf[c] + jnp.exp(last) * rv
        m_copy(c).start()

        @pl.when(i > 0)
        def _():
            q_send(c + 1)

        return carry

    lax.fori_loop(0, nc, back_b, 0)
    phase("g_fourth")
    g_fourth()
    phase("inter2")

    def back(i, carry):
        c = i
        sl = pl.ds(pl.multiple_of(c * Q, Q), Q)
        cum = lx[sl, :]
        last = cum[Q - 1 : Q, :]
        rv = rst[c]
        xv = x[sl, :]
        sx = st[sl, :]
        d_in = mm(bcv[sl, :ns], rv) * jnp.exp(last - cum)
        dxt = y[sl, :] + d_in
        uv = u[sl, :]
        su = sigmoid(uv)
        dus[sl, :] = (sx * dxt + skip_x * gm[sl, :]) * (su * (1.0 + uv * (1.0 - su)))
        per_head = by_head(jnp.concatenate([xv * sx * d_in, xv * dxt], axis=0))
        fixed = by_head(
            jnp.broadcast_to(jnp.sum(rv * sst[c], axis=0, keepdims=True) * jnp.exp(last), (8, ch))
        )[0:1]
        dld = (
            mm(tail_sum, jnp.concatenate(parts(swings[c], 3), axis=0))
            + mm(head_sum, jnp.concatenate(parts(per_head[:Q], 3), axis=0))
            + fixed
        )
        dstep = per_head[Q:] + dld * neg_c
        slope = sigmoid(raw[:, sl].astype(F32) + dt_col)
        o_gdt[:, sl] = jnp.transpose(dstep)[:heads] * slope

        @pl.when(i == 0)
        def _():
            q_send(0)
            edge_x.start()

        return carry

    edge_x = remote(dus.at[pl.ds(0, 8)], dus.at[pl.ds(rows, 8)], sm_h, 2, "seq", prv)
    lax.fori_loop(0, nc, back, 0)
    stores[5].start()
    phase("wait_q")

    def a_copy(k):
        return remote(qa.at[my], qa.at[my], sm_a, k, "tp", tp_peer(k))

    def edge_b(j):
        return pltpu.make_async_remote_copy(
            src_ref=edge,
            dst_ref=dub.at[pl.ds(rows, 8)],
            send_sem=sm_e.at[j],
            recv_sem=sm_h.at[1, 3],
            device_id={"seq": prv, "tp": j},
            device_id_type=MESH,
        )

    for c in range(nc):
        for k in range(1, side):
            q_copy(c, k).wait_recv()
    phase("qsum")
    qsum = qr[:, 0]
    for j in range(1, side):
        qsum = qsum + qr[:, j]
    qa[my] = qsum.astype(BF16)
    ube = ub[pl.ds(0, 8), :]
    sbe = sigmoid(ube)
    edge[...] = qsum[0, 0:8, :] * (sbe * (1.0 + ube * (1.0 - sbe)))

    @pl.when(my == 0)
    def _():
        for j in range(n_tp):
            edge_b(j).start()

    for k in range(1, n_tp):
        a_copy(k).start()

    phase("o_last")
    o_last()
    phase("wait_e")
    edge_x.wait_recv()

    phase("convbx")
    def conv_back(ref, weights, out, c):
        base = pl.multiple_of(c * Q, Q)
        ext = ref[pl.ds(base, Q + 8), :]
        tail = jnp.where((c < nc - 1) | (me < n_seq - 1), ext[Q:], 0.0)
        ext = jnp.concatenate([ext[:Q], tail], axis=0)
        acc = weights[3:4, :] * ext[:Q]
        for k in range(3):
            acc = acc + weights[k : k + 1, :] * pltpu.roll(ext, Q + 8 - (3 - k), 0)[:Q]
        out[pl.ds(base, Q), :] = acc

    def conv_back_x(c, carry):
        conv_back(dus, cw, o_gx, c)
        return carry

    lax.fori_loop(0, nc, conv_back_x, 0)

    stores[1].start()
    stores[2].start()
    phase("g_last")
    g_last()
    phase("wait_a")
    for k in range(1, n_tp):
        a_copy(k).wait_recv()
    phase("dub")
    for c in range(nc):
        sl = pl.ds(c * Q, Q)
        ubv = ub[sl, :]
        sb = sigmoid(ubv)
        dub[sl, :] = qa[:, c].reshape(Q, 2 * ns).astype(F32) * (sb * (1.0 + ubv * (1.0 - sb)))

    phase("convbb")
    edge_b(0).wait_recv()

    def conv_back_b(c, carry):
        conv_back(dub, cwb, o_gbc, c)
        return carry

    stores[3].start()
    lax.fori_loop(0, nc, conv_back_b, 0)
    stores[4].start()

    phase("drain")
    halo_x.wait_send()
    halo_b.wait_send()
    edge_x.wait_send()

    @pl.when(my == 0)
    def _():
        for j in range(n_tp):
            edge_b(j).wait_send()

    for k in range(1, n_seq):
        for copy in (t_copy, s_copy, sb_copy, v_copy, vb_copy):
            copy(k).wait_send()
    for k in range(1, n_tp):
        a_copy(k).wait_send()
    for c in range(nc):
        m_copy(c).wait_send()
        for k in range(1, side):
            q_copy(c, k).wait_send()
    for copy in r_squares + r_inner:
        copy.wait_send()
    for copy in w_copies + d_copies + o_copies + g_copies:
        copy.wait_send()
    for store in stores:
        store.wait()
    phase("")


def solution(mesh):
    n_seq, n_tp = mesh.shape["seq"], mesh.shape["tp"]

    def shards(
        inner_x,
        gate_z,
        proj_bc,
        dt_raw,
        a_log,
        dt_bias,
        d_skip,
        conv_x,
        bias_x,
        conv_bc,
        bias_bc,
        norm_gain,
        w_out,
        d_out,
    ):
        rows, ch = inner_x.shape
        heads = a_log.shape[0]
        ns2 = proj_bc.shape[1]
        ns = ns2 // 2
        nc = rows // Q
        nrow = ns // n_seq
        wrows, drows = w_out.shape[1], d_out.shape[1]
        w_t = w_out.T
        d_t = d_out.T.reshape(2, drows // 2, rows)

        big = pltpu.VMEM((rows, ch), F32)
        chunk_states = pltpu.VMEM((nc, ns, ch), F32)
        slices = pltpu.VMEM((n_seq, nrow, ch), F32)
        sem_s = pltpu.SemaphoreType.DMA((2, n_seq))
        sem_t = pltpu.SemaphoreType.DMA((2, n_tp))
        scratch = [
            pltpu.VMEM((drows, rows), BF16),
            big,
            big,
            pltpu.VMEM((rows, ns2), F32),
            pltpu.VMEM((heads, rows), F32),
            pltpu.VMEM((wrows, ch), F32),
            pltpu.VMEM((rows, ch), BF16),
            pltpu.VMEM((rows, ch), BF16),
            pltpu.VMEM((rows, ns2), BF16),
            pltpu.VMEM((heads, rows), BF16),
            pltpu.VMEM((4, ch), F32),
            pltpu.VMEM((ch // LANES, LANES), F32),
            pltpu.VMEM((4, ns2), F32),
            pltpu.VMEM((1, ns2), F32),
            pltpu.VMEM((ch // LANES, LANES), F32),
            pltpu.VMEM((1, heads), F32),
            pltpu.VMEM((1, heads), F32),
            pltpu.VMEM((1, heads), F32),
            pltpu.VMEM((4, 4, wrows, ch), BF16),
            pltpu.VMEM((4, 4, wrows, rows), BF16),
            pltpu.VMEM((16, ch), BF16),
            pltpu.VMEM((16, ns2), BF16),
            pltpu.VMEM((8, LANES), F32),
            pltpu.VMEM((n_seq, 8, LANES), F32),
            big,
            big,
            pltpu.VMEM((nc, heads, Q), F32),
            big,
            big,
            pltpu.VMEM((rows, ns2), F32),
            pltpu.VMEM((rows, ns2), F32),
            chunk_states,
            chunk_states,
            chunk_states,
            big,
            big,
            big,
            big,
            pltpu.VMEM((rows, ch), BF16),
            pltpu.VMEM((rows + 8, ch), F32),
            pltpu.VMEM((rows + 8, ns2), F32),
            pltpu.VMEM((ns, ch), F32),
            slices,
            slices,
            slices,
            slices,
            slices,
            slices,
            slices,
            slices,
            pltpu.VMEM((2, 8, rows), F32),
            pltpu.VMEM((2, n_tp, 8, rows), F32),
            pltpu.VMEM((4, 2, drows, rows), BF16),
            pltpu.VMEM((4, drows, rows), BF16),
            pltpu.VMEM((drows, rows), BF16),
            pltpu.VMEM((2, drows, rows), BF16),
            pltpu.VMEM((4, 4, wrows, ch), BF16),
            *[
                pltpu.VMEM(shape, BF16)
                for shape in 2
                * [
                    (4, wrows // 2, ch),
                    (2, 4, wrows // 2, ch),
                    (wrows // 2, ch),
                    (2, wrows // 2, ch),
                ]
            ],
            pltpu.VMEM((nc, 4, 2, Q // n_tp, ns2), F32),
            pltpu.VMEM((nc, 4, Q // n_tp, ns2), F32),
            pltpu.VMEM((nc, 4, Q // n_tp, ns2), F32),
            chunk_states,
            pltpu.VMEM((n_tp, nc, Q // n_tp, ns2), BF16),
            pltpu.VMEM((Q, LANES), F32),
            pltpu.VMEM((LANES, Q), F32),
            pltpu.VMEM((Q, Q), F32),
            pltpu.VMEM((rows, 1), F32),
            pltpu.VMEM((nc, Q, LANES), F32),
            pltpu.VMEM((rows, ns2), F32),
            pltpu.VMEM((8, ns2), F32),
            pltpu.SemaphoreType.DMA((2, nc)),
            pltpu.SemaphoreType.DMA((n_tp,)),
            pltpu.SemaphoreType.DMA((20,)),
            pltpu.SemaphoreType.DMA((2, 4)),
            sem_s,
            pltpu.SemaphoreType.DMA((2, 28)),
            sem_t,
            sem_s,
            sem_s,
            sem_s,
            sem_s,
            pltpu.SemaphoreType.DMA((2, 2 * n_tp)),
            sem_t,
            pltpu.SemaphoreType.DMA((2, 20)),
            pltpu.SemaphoreType.DMA((2, nc * n_tp)),
            sem_t,
        ]
        out_t, g_x, g_z, g_bc, g_dt, g_w = pl.pallas_call(
            functools.partial(kernel, (n_seq, n_tp, ch * n_tp)),
            out_shape=[
                jax.ShapeDtypeStruct((drows, rows), BF16),
                jax.ShapeDtypeStruct((rows, ch), F32),
                jax.ShapeDtypeStruct((rows, ch), F32),
                jax.ShapeDtypeStruct((rows, ns2), F32),
                jax.ShapeDtypeStruct((heads, rows), F32),
                jax.ShapeDtypeStruct((wrows, ch), F32),
            ],
            in_specs=[pl.BlockSpec(memory_space=pltpu.HBM)] * 14,
            out_specs=[pl.BlockSpec(memory_space=pltpu.HBM)] * 6,
            scratch_shapes=scratch,
            compiler_params=pltpu.CompilerParams(
                collective_id=0, has_side_effects=True, vmem_limit_bytes=62 * 1024 * 1024
            ),
            name="mixer",
        )(
            inner_x,
            gate_z,
            proj_bc,
            dt_raw.T,
            w_t,
            d_t,
            conv_x,
            bias_x.reshape(-1, LANES),
            conv_bc,
            bias_bc[None, :],
            norm_gain.reshape(-1, LANES),
            a_log[None, :],
            dt_bias[None, :],
            d_skip[None, :],
        )
        return out_t.T, g_x, g_z, g_bc, g_dt.T, g_w.T

    in_specs = (
        P("seq", "tp"),
        P("seq", "tp"),
        P("seq", None),
        P("seq", "tp"),
        P("tp"),
        P("tp"),
        P("tp"),
        P(None, "tp"),
        P("tp"),
        P(),
        P(),
        P("tp"),
        P("tp", "seq"),
        P("seq", "tp"),
    )
    out_specs = (
        P("seq", "tp"),
        P("seq", "tp"),
        P("seq", "tp"),
        P("seq", None),
        P("seq", "tp"),
        P("tp", "seq"),
    )
    return jax.shard_map(
        shards, mesh=mesh, in_specs=in_specs, out_specs=out_specs, check_vma=False
    )
```

```python
import functools

import jax
import jax.numpy as jnp
from jax import lax
from jax.experimental import pallas as pl
from jax.experimental.pallas import tpu as pltpu
from jax.sharding import PartitionSpec as P

MESH = pl.DeviceIdType.MESH
F32 = jnp.float32
BF16 = jnp.bfloat16
HIGH = lax.Precision.HIGHEST
EPSILON = 1e-05
NN = ((1,), (0,))
NT = ((1,), (1,))
Q = 128
PAIR = 128
HEAD = 64
LANES = 128


def mm(a, b, dims=NN):
    return lax.dot_general(a.astype(BF16), b.astype(BF16), (dims, ((), ())), preferred_element_type=F32)


def mmh(a, b, dims=NN):
    return lax.dot_general(
        a.astype(F32), b.astype(F32), (dims, ((), ())), precision=HIGH, preferred_element_type=F32
    )


def halves(v):
    high = v.astype(BF16)
    return high, (v - high.astype(F32)).astype(BF16)


def mm3(a, b, dims=NN):
    a0, a1 = halves(a)
    b0, b1 = halves(b)
    return mm(a0, b0, dims) + (mm(a1, b0, dims) + mm(a0, b1, dims))


def parts(v, count):
    out = []
    for _ in range(count):
        piece = v.astype(BF16)
        out.append(piece)
        v = v - piece.astype(F32)
    return out


def iota(shape, dim):
    return lax.broadcasted_iota(jnp.int32, shape, dim)


def sigmoid(v):
    return 1.0 / (1.0 + jnp.exp(-v))


def softplus(v):
    return jnp.maximum(v, 0.0) + jnp.log1p(jnp.exp(-jnp.abs(v)))


def pair_stack(v):
    lane = iota(v.shape, 1)
    return jnp.concatenate(
        [jnp.where(lane < HEAD, v, 0.0), jnp.where(lane >= HEAD, v, 0.0)], axis=0
    )


def kernel(
    sizes,
    ix_in,
    gz_in,
    bc_in,
    raw_in,
    wt,
    dt,
    cw_in,
    bx_in,
    cwb_in,
    bb_in,
    gain_in,
    al_in,
    db_in,
    ds_in,
    out_hbm,
    gx_hbm,
    gz_hbm,
    gbc_hbm,
    gdt_hbm,
    gw_hbm,
    o_out,
    o_gx,
    o_gz,
    o_gbc,
    o_gdt,
    o_gw,
    ix,
    gz,
    bc,
    raw,
    cw,
    bx,
    cwb,
    bb,
    gain,
    al,
    db,
    ds,
    wfull,
    dfull,
    hx,
    hb,
    dsend,
    dbuf,
    st,
    lx,
    lt,
    u,
    x,
    ub,
    bcv,
    fr,
    sst,
    cf,
    y,
    gated,
    gn,
    gm,
    nb,
    dus,
    dub,
    rcur,
    se,
    sr,
    en,
    sin,
    re,
    rr,
    ren,
    rin,
    ts,
    tr,
    pb,
    pp,
    po1,
    po2,
    gb,
    ga1,
    ga2,
    ga3,
    ga4,
    gb1,
    gb2,
    gb3,
    gb4,
    qs,
    qm,
    qr,
    rst,
    qa,
    arow,
    acol,
    dga,
    invs,
    swings,
    dmap,
    edge,
    sm_m,
    sm_e,
    sm_l,
    sm_h,
    sm_d,
    sm_w,
    sm_g,
    sm_s,
    sm_b,
    sm_r,
    sm_q,
    sm_t,
    sm_o,
    sm_v,
    sm_p,
    sm_a,
):
    n_seq, n_tp, inner = sizes
    rows, ch = ix.shape
    nc = rows // Q
    heads = raw.shape[0]
    pairs = ch // PAIR
    ns = bc.shape[1] // 2
    me, my = lax.axis_index("seq"), lax.axis_index("tp")
    wrows = wt.shape[0]
    drows = 2 * dt.shape[1]
    nrow = ns // n_seq

    scope = []

    def phase(name):
        if scope:
            scope.pop().__exit__(None, None, None)
        if name:
            scope.append(jax.named_scope(name))
            scope[0].__enter__()

    side = 4
    zi, xi = lax.div(me, side), lax.rem(me, side)
    yi, core = lax.div(my, 2), lax.rem(my, 2)

    def step(v, k):
        return lax.rem(v + k + side, side)

    x_up, x_dn = step(xi, 1), step(xi, -1)
    z_up, z_dn = step(zi, 1), step(zi, -1)
    y_up, y_dn = step(yi, 1), step(yi, -1)
    x_far, z_far, y_far = step(xi, 2), step(zi, 2), step(yi, 2)
    to_xu, to_xd = zi * side + x_up, zi * side + x_dn
    to_zu, to_zd = z_up * side + xi, z_dn * side + xi
    to_yu, to_yd = y_up * 2 + core, y_dn * 2 + core
    mate = yi * 2 + 1 - core

    def hops(pair):
        return sum(min(v, side - v) for v in pair)

    others = [(a, b) for a in range(side) for b in range(side) if a or b]
    others.sort(key=lambda pair: -hops(pair))

    def seq_peer(k):
        a, b = others[k - 1]
        return step(zi, a) * side + step(xi, b)

    def tp_peer(k):
        return lax.rem(my + k, n_tp)

    phase("barrier1")
    barrier = pltpu.get_barrier_semaphore()
    for k in range(1, n_seq):
        pl.semaphore_signal(barrier, inc=1, device_id={"seq": seq_peer(k)}, device_id_type=MESH)
    for k in range(1, n_tp):
        pl.semaphore_signal(barrier, inc=1, device_id={"tp": tp_peer(k)}, device_id_type=MESH)

    def remote(src, dst, sems, k, axis, peer):
        return pltpu.make_async_remote_copy(
            src_ref=src,
            dst_ref=dst,
            send_sem=sems.at[0, k],
            recv_sem=sems.at[1, k],
            device_id={axis: peer},
            device_id_type=MESH,
        )

    nxt, prv = lax.rem(me + 1, n_seq), lax.rem(me + n_seq - 1, n_seq)

    @pl.when(my > 0)
    def _():
        pl.semaphore_signal(barrier, inc=1, device_id={"seq": nxt, "tp": 0}, device_id_type=MESH)

    staged = [
        (raw_in, raw),
        (al_in, al),
        (db_in, db),
        (ds_in, ds),
        (wt, wfull.at[zi, xi]),
        (dt, dfull.at[yi, pl.ds(2 * core, 2)]),
        (ix_in, ix),
        (bc_in, bc),
        (cw_in, cw),
        (bx_in, bx),
        (cwb_in, cwb),
        (bb_in, bb),
        (gain_in, gain),
        (gz_in, gz),
    ]
    loads = [pltpu.make_async_copy(a, b, sm_l.at[i]) for i, (a, b) in enumerate(staged)]
    for load in loads:
        load.start()
    results = [(o_gz, gz_hbm), (o_out, out_hbm), (o_gx, gx_hbm), (o_gw, gw_hbm), (o_gbc, gbc_hbm), (o_gdt, gdt_hbm)]
    stores = [pltpu.make_async_copy(a, b, sm_l.at[14 + i]) for i, (a, b) in enumerate(results)]
    phase("staging")
    for load in loads[:9]:
        load.wait()
    phase("barrier")
    pl.semaphore_wait(barrier, n_seq + n_tp - 2 + jnp.where(my == 0, n_tp - 1, 0))

    phase("start")
    halo_x = remote(ix.at[pl.ds(rows - 16, 16)], hx, sm_h, 0, "seq", nxt)
    halo_b = remote(bc.at[pl.ds(rows - 16, 16)], hb, sm_h, 1, "seq", nxt)
    halo_x.start()
    halo_b.start()

    half = wrows // 2
    near = 48
    ra, rb = pl.ds(0, half), pl.ds(half, half)
    ra1, ra2 = pl.ds(0, near), pl.ds(near, half - near)
    rb1, rb2 = pl.ds(half, near), pl.ds(half + near, half - near)
    lo, hi, every = pl.ds(0, 2), pl.ds(2, 2), pl.ds(0, side)

    def w_view(z, x, r):
        return wfull.at[z, x, r]

    def w_move(i, peer, z, x, r, src=None):
        return remote(w_view(z, x, r) if src is None else src, w_view(z, x, r), sm_w, i, "seq", peer)

    w_copies = [
        w_move(0, to_xu, zi, xi, ra),
        w_move(1, to_xd, zi, xi, ra),
        w_move(2, to_zu, zi, xi, rb),
        w_move(3, to_zd, zi, xi, rb),
        w_move(4, to_zu, zi, xi, ra),
        w_move(5, to_zd, zi, xi, ra),
        w_move(6, to_xu, zi, xi, rb),
        w_move(7, to_xd, zi, xi, rb),
        w_move(8, to_xu, zi, x_dn, ra1),
        w_move(9, to_xd, zi, x_up, ra2),
        w_move(10, to_zu, z_dn, xi, rb1),
        w_move(11, to_zd, z_up, xi, rb2),
        w_move(12, to_zu, zi, x_up, ra),
        w_move(13, to_zd, zi, x_up, ra),
        w_move(14, to_xu, z_up, xi, rb),
        w_move(15, to_xd, z_up, xi, rb),
        w_move(16, to_zu, zi, x_dn, ra),
        w_move(17, to_zd, zi, x_dn, ra),
        w_move(18, to_xu, z_dn, xi, rb),
        w_move(19, to_xd, z_dn, xi, rb),
        w_move(20, to_zu, zi, x_far, ra),
        w_move(21, to_zd, zi, x_far, ra),
        w_move(22, to_xu, z_far, xi, rb),
        w_move(23, to_xd, z_far, xi, rb),
        w_move(24, to_zu, z_dn, lo, ra),
        w_move(25, to_zd, z_up, hi, ra),
        w_move(26, to_xu, lo, x_dn, rb),
        w_move(27, to_xd, hi, x_up, rb),
    ]

    dhalf = drows // 2

    def d_view(y, c, off=0, size=drows):
        if size == drows:
            return dfull.at[y, pl.ds(2 * c, 2)]
        return dfull.at[y, 2 * c + off // size]

    def d_move(i, peer, y, c, off=0, size=drows, src=None):
        view = d_view(y, c, off, size)
        return remote(view if src is None else src, view, sm_g, i, "tp", peer)

    d_copies = [
        d_move(0, to_yu, yi, core),
        d_move(1, to_yd, yi, core),
        d_move(2, mate, yi, core),
        d_move(3, to_yu, y_dn, core, 0, dhalf),
        d_move(4, to_yd, y_up, core, dhalf, dhalf),
        d_move(5, mate, y_dn, core),
        d_move(6, mate, y_up, core),
        d_move(7, mate, y_far, core),
    ]

    def start(copies, first, last):
        for copy in copies[first:last]:
            copy.start()

    def arrived(copies, first, last):
        for copy in copies[first:last]:
            copy.wait_recv()

    start(w_copies, 0, 8)
    start(d_copies, 0, 3)

    phase("steps")
    def spread_of(first):
        return (iota((LANES, ch), 1) // HEAD + first == iota((LANES, ch), 0)).astype(BF16)

    ident = (iota((heads, heads), 0) == iota((heads, heads), 1)).astype(F32)
    spread_s = jnp.concatenate([spread_of(0)] * 3, axis=0)
    spread_l = jnp.concatenate([spread_of(16)] * 3, axis=0)
    spread_h = spread_of(0)[:heads].astype(F32)
    negexp = -jnp.exp(al[...])
    skip_x = mmh(jnp.broadcast_to(ds[...], (8, heads)), spread_h)[0:1]
    tri_u = (iota((Q, Q), 0) <= iota((Q, Q), 1)).astype(F32)

    def column(v):
        return mmh(ident, jnp.broadcast_to(v, (8, heads)), NT)[:, 0:1]

    def in_line(ref):
        return jnp.concatenate([ref[i : i + 1] for i in range(ref.shape[0])], axis=1)

    dt_col, neg_col = column(db[...]), column(negexp)

    for load in loads[9:]:
        load.wait()
    bias_line, gain_line = in_line(bx), in_line(gain)

    def steps(c, total):
        sl = pl.ds(pl.multiple_of(c * Q, Q), Q)
        s_c = softplus(raw[:, sl].astype(F32) + dt_col)
        cum = mmh(s_c * neg_col, tri_u)
        lt[c] = cum
        stacked = jnp.concatenate(
            [
                s_c,
                jnp.zeros((16 - heads, Q), F32),
                cum,
                jnp.zeros((LANES - 16 - heads, Q), F32),
            ],
            axis=0,
        )
        turned = jnp.transpose(stacked)
        pieces = jnp.concatenate(parts(turned, 3), axis=1)
        st[sl, :] = mm(pieces, spread_s)
        lx[sl, :] = mm(pieces, spread_l)
        return total + turned[Q - 1 : Q, :]

    total = lax.fori_loop(0, nc, steps, jnp.zeros((1, LANES), F32))
    dsend[...] = jnp.broadcast_to(total, (8, LANES))
    dbuf[me] = dsend[...]

    def t_copy(k):
        return remote(dsend, dbuf.at[me], sm_d, k, "seq", seq_peer(k))

    for k in range(1, n_seq):
        t_copy(k).start()

    phase("convs")
    def conv_of(ref, halo, weights, bias, c):
        base = pl.multiple_of(c * Q, Q)
        own = ref[pl.ds(base, Q), :].astype(F32)
        if halo is None:
            head = ref[pl.ds(pl.multiple_of(c * Q - 16, 16), 16), :].astype(F32)[8:16]
        else:
            head = jnp.where(me > 0, halo[...].astype(F32), 0.0)[8:16]
        ext = jnp.concatenate([head, own], axis=0)
        acc = bias + weights[3:4, :] * own
        for k in range(3):
            acc = acc + weights[k : k + 1, :] * pltpu.roll(ext, Q + 8 - (5 + k), 0)[:Q]
        return acc

    def convs(c, carry, edge_of=(None, None)):
        sl = pl.ds(pl.multiple_of(c * Q, Q), Q)
        vb = conv_of(bc, edge_of[0], cwb, bb[...], c)
        ub[sl, :] = vb
        pbc = vb * sigmoid(vb)
        bcv[sl, :] = pbc
        vx = conv_of(ix, edge_of[1], cw, bias_line, c)
        u[sl, :] = vx
        xv = vx * sigmoid(vx)
        x[sl, :] = xv
        cum = lx[sl, :]
        to_end = jnp.exp(cum[Q - 1 : Q, :] - cum)
        b_t = jnp.transpose(pbc[:, :ns])
        fresh = mm3(b_t, xv * st[sl, :] * to_end)
        fr[c] = fresh
        return carry

    lax.fori_loop(1, nc, convs, 0)
    phase("wait_halo")
    halo_x.wait_recv()
    halo_b.wait_recv()
    phase("conv0")
    convs(0, 0, (hb, hx))
    end = fr[0]
    for c in range(1, nc):
        end = jnp.exp(lx[pl.ds(c * Q + Q - 1, 1), :]) * end + fr[c]
    se[...] = end.reshape(n_seq, nrow, ch)

    phase("send_s")
    def s_copy(k):
        return remote(se.at[seq_peer(k)], sr.at[me], sm_s, k, "seq", seq_peer(k))

    def sb_copy(k):
        return remote(en.at[seq_peer(k)], sin.at[me], sm_b, k, "seq", seq_peer(k))

    for k in range(1, n_seq):
        s_copy(k).start()
    sr[me] = se[me]
    phase("wait_w1")
    arrived(w_copies, 0, 4)
    start(w_copies, 8, 16)

    upper = iota((Q, Q), 0) >= iota((Q, Q), 1)
    lower = iota((Q, Q), 0) <= iota((Q, Q), 1)

    phase("inside")
    def inside(c, carry):
        sl = pl.ds(pl.multiple_of(c * Q, Q), Q)
        scores = mm3(bcv[sl, ns:], bcv[sl, :ns], NT)
        for p in range(pairs):
            ps = slice(p * PAIR, (p + 1) * PAIR)
            both = []
            for h in (2 * p, 2 * p + 1):
                diff = lx[sl, h * HEAD : h * HEAD + 1] - lt[c, h : h + 1, :]
                decay = jnp.exp(jnp.where(upper, diff, -1e30))
                both.append(decay * scores)
            y[sl, ps] = mm3(jnp.concatenate(both, axis=1), pair_stack(x[sl, ps] * st[sl, ps]))
        return carry

    lax.fori_loop(0, nc, inside, 0)
    phase("wait_d1")
    arrived(d_copies, 0, 2)
    start(d_copies, 3, 7)
    phase("wait_s")
    for k in range(1, n_seq):
        t_copy(k).wait_recv()
    for k in range(1, n_seq):
        s_copy(k).wait_recv()
    phase("scan")
    fade = jnp.exp(mm(jnp.concatenate(parts(dbuf[:, 0, :], 3), axis=1), spread_l))

    acc = jnp.zeros((nrow, ch), F32)
    for j in range(n_seq):
        en[j] = acc
        acc = fade[j : j + 1] * acc + sr[j]
    for k in range(1, n_seq):
        sb_copy(k).start()
    sin[me] = en[me]
    start(w_copies, 16, 20)
    phase("wait_w2")
    arrived(w_copies, 8, 12)
    start(w_copies, 20, 24)

    phase("wait_sb")
    for k in range(1, n_seq):
        sb_copy(k).wait_recv()
    phase("combine")
    lane = iota((Q, LANES), 1)

    def to_row(i, c, v):
        ts[i, :, pl.ds(pl.multiple_of(c * Q, Q), Q)] = jnp.transpose(jnp.where(lane == 0, v, 0.0))[:8]

    def to_column(row, c):
        block = jnp.concatenate([row[:, c * Q : (c + 1) * Q], jnp.zeros((Q - 8, Q), F32)], axis=0)
        return jnp.transpose(block)[:, 0:1]

    def combine(c, state):
        sl = pl.ds(pl.multiple_of(c * Q, Q), Q)
        sst[c] = state
        cum = lx[sl, :]
        mixed = y[sl, :] + jnp.exp(cum) * mm3(bcv[sl, ns:], state) + skip_x * x[sl, :]
        y[sl, :] = mixed
        zv = gz[sl, :].astype(F32)
        gv = mixed * zv * sigmoid(zv)
        gated[sl, :] = gv
        to_row(0, c, jnp.sum(gv * gv, axis=1, keepdims=True))
        return jnp.exp(cum[Q - 1 : Q, :]) * state + fr[c]

    lax.fori_loop(0, nc, combine, sin[...].reshape(ns, ch))

    def r_copies(i):
        return [
            remote(ts.at[i], tr.at[i, my], sm_t, i * n_tp + k, "tp", tp_peer(k)) for k in range(1, n_tp)
        ]

    def r_total(i):
        total = tr[i, 0]
        for j in range(1, n_tp):
            total = total + tr[i, j]
        return total

    r_squares, r_inner = r_copies(0), r_copies(1)
    start(r_squares, 0, n_tp - 1)
    tr[0, my] = ts[0]

    phase("wait_d2")
    arrived(d_copies, 3, 5)
    start(d_copies, 7, 8)
    phase("wait_w3")
    arrived(w_copies, 4, 8)
    arrived(w_copies, 12, 24)
    start(w_copies, 24, 28)
    phase("wait_d")
    arrived(d_copies, 2, 3)
    arrived(d_copies, 5, 8)
    phase("gn")
    kb = wrows * side

    def gn_add(part, first):
        @pl.when(first)
        def _():
            gn[...] = part

        @pl.when(jnp.logical_not(first))
        def _():
            gn[...] += part

    def gn_early(k, carry):
        zz, xx = step(zi, k - 1), step(xi, k - 1)
        d_rows = jnp.concatenate(
            [dfull[zz, :, ra].reshape(kb // 2, rows), dfull[:, xx, rb].reshape(kb // 2, rows)], axis=0
        )
        w_rows = jnp.concatenate(
            [wfull[zz, :, ra].reshape(kb // 2, ch), wfull[:, xx, rb].reshape(kb // 2, ch)], axis=0
        )
        gn_add(mm(jnp.transpose(d_rows), w_rows), k == 0)
        return carry

    lax.fori_loop(0, 3, gn_early, 0)

    phase("wait_ss")
    arrived(r_squares, 0, n_tp - 1)
    inv_row = lax.rsqrt(r_total(0) / inner + EPSILON)
    phase("nb")
    for c in range(nc):
        sl = pl.ds(c * Q, Q)
        inv = to_column(inv_row, c)
        invs[sl, :] = inv
        nb[sl, :] = (gated[sl, :] * inv * gain_line).astype(BF16)
    phase("gradw")
    g_copies = [
        remote(gb.at[z_far, lo, ra], ga1.at[lo], sm_v, 0, "seq", to_zu),
        remote(gb.at[z_far, hi, ra], ga1.at[hi], sm_v, 1, "seq", to_zd),
        remote(gb.at[lo, x_far, rb], gb1.at[lo], sm_v, 2, "seq", to_xu),
        remote(gb.at[hi, x_far, rb], gb1.at[hi], sm_v, 3, "seq", to_xd),
        remote(gb.at[z_up, hi, ra], ga2.at[0, hi], sm_v, 4, "seq", to_zu),
        remote(gb.at[z_dn, lo, ra], ga2.at[1, lo], sm_v, 5, "seq", to_zd),
        remote(gb.at[hi, x_up, rb], gb2.at[0, hi], sm_v, 6, "seq", to_xu),
        remote(gb.at[lo, x_dn, rb], gb2.at[1, lo], sm_v, 7, "seq", to_xd),
        remote(gb.at[z_up, lo, ra], ga2.at[0, lo], sm_v, 8, "seq", to_zu),
        remote(gb.at[z_dn, hi, ra], ga2.at[1, hi], sm_v, 9, "seq", to_zd),
        remote(gb.at[lo, x_up, rb], gb2.at[0, lo], sm_v, 10, "seq", to_xu),
        remote(gb.at[hi, x_dn, rb], gb2.at[1, hi], sm_v, 11, "seq", to_xd),
        remote(gb.at[zi, x_far, ra1], ga3.at[ra1], sm_v, 12, "seq", to_xu),
        remote(gb.at[zi, x_far, ra2], ga3.at[ra2], sm_v, 13, "seq", to_xd),
        remote(gb.at[z_far, xi, rb1], gb3.at[ra1], sm_v, 14, "seq", to_zu),
        remote(gb.at[z_far, xi, rb2], gb3.at[ra2], sm_v, 15, "seq", to_zd),
        remote(gb.at[zi, x_up, ra], ga4.at[0], sm_v, 16, "seq", to_xu),
        remote(gb.at[zi, x_dn, ra], ga4.at[1], sm_v, 17, "seq", to_xd),
        remote(gb.at[z_up, xi, rb], gb4.at[0], sm_v, 18, "seq", to_zu),
        remote(gb.at[z_dn, xi, rb], gb4.at[1], sm_v, 19, "seq", to_zd),
    ]

    def plus(ref, index, *others):
        total = ref[index].astype(F32)
        for part in others:
            total = total + part.astype(F32)
        ref[index] = total.astype(BF16)

    def g_block(k, carry):
        b = step(zi, 2 + k)
        gb[b] = mm(dfull[b].reshape(kb, rows), nb[...]).astype(BF16).reshape(side, wrows, ch)

        @pl.when(k == 0)
        def _():
            start(g_copies, 0, 2)

        return carry

    lax.fori_loop(0, side, g_block, 0)
    start(g_copies, 2, 8)

    def g_second():
        arrived(g_copies, 0, 4)
        for j in range(2):
            plus(gb, (z_up, j, ra), ga1[j])
            plus(gb, (z_dn, 2 + j, ra), ga1[2 + j])
            plus(gb, (j, x_up, rb), gb1[j])
            plus(gb, (2 + j, x_dn, rb), gb1[2 + j])
        start(g_copies, 8, 12)

    def g_third():
        arrived(g_copies, 4, 12)
        for j in range(side):
            plus(gb, (zi, j, ra), ga2[0, j], ga2[1, j])
            plus(gb, (j, xi, rb), gb2[0, j], gb2[1, j])
        start(g_copies, 12, 16)

    def g_fourth():
        arrived(g_copies, 12, 16)
        plus(gb, (zi, x_up, ra1), ga3[ra1])
        plus(gb, (zi, x_dn, ra2), ga3[ra2])
        plus(gb, (z_up, xi, rb1), gb3[ra1])
        plus(gb, (z_dn, xi, rb2), gb3[ra2])
        start(g_copies, 16, 20)

    def g_last():
        arrived(g_copies, 16, 20)
        o_gw[ra, :] = gb[zi, xi, ra].astype(F32) + ga4[0].astype(F32) + ga4[1].astype(F32)
        o_gw[rb, :] = gb[zi, xi, rb].astype(F32) + gb4[0].astype(F32) + gb4[1].astype(F32)

    def o_second():
        arrived(o_copies, 0, 1)
        for j in range(side):
            plus(pb, (j, core), pp[j])
        start(o_copies, 1, 3)

    def o_third():
        arrived(o_copies, 1, 3)
        plus(pb, (y_up, core, o_half1), po1[o_half1])
        plus(pb, (y_dn, core, o_half2), po1[o_half2])
        start(o_copies, 3, 5)

    def o_last():
        arrived(o_copies, 3, 5)
        total = pb[yi, core].astype(F32) + po2[0].astype(F32) + po2[1].astype(F32)
        o_out[...] = total.astype(BF16)
    phase("wait_w4")
    arrived(w_copies, 24, 28)
    phase("gn_last")
    gn_early(3, 0)
    phase("ip")

    def inner_sums(c, carry):
        sl = pl.ds(pl.multiple_of(c * Q, Q), Q)
        scaled = gn[sl, :] * gain_line
        gn[sl, :] = scaled
        to_row(1, c, jnp.sum(scaled * gated[sl, :], axis=1, keepdims=True))
        return carry

    lax.fori_loop(0, nc, inner_sums, 0)
    start(r_inner, 0, n_tp - 1)
    tr[1, my] = ts[1]
    phase("outmm")
    def share(y0, c0):
        block = wfull[y0, pl.ds(2 * c0, 2)].reshape(drows, ch)
        pb[y0, c0] = mm(block, nb[...], NT).astype(BF16)

    def other(j, carry):
        share(j, 1 - core)
        return carry

    def same(j, carry):
        share(j, core)
        return carry

    o_half1, o_half2 = pl.ds(0, dhalf), pl.ds(dhalf, dhalf)
    o_copies = [
        remote(pb.at[every, 1 - core], pp, sm_o, 0, "tp", mate),
        remote(pb.at[y_far, core, o_half1], po1.at[o_half1], sm_o, 1, "tp", to_yu),
        remote(pb.at[y_far, core, o_half2], po1.at[o_half2], sm_o, 2, "tp", to_yd),
        remote(pb.at[y_up, core], po2.at[0], sm_o, 3, "tp", to_yu),
        remote(pb.at[y_dn, core], po2.at[1], sm_o, 4, "tp", to_yd),
    ]
    lax.fori_loop(0, side, other, 0)
    start(o_copies, 0, 1)
    lax.fori_loop(0, side, same, 0)
    phase("wait_ip")
    arrived(r_inner, 0, n_tp - 1)
    ip_row = r_total(1) / inner * inv_row * inv_row * inv_row
    phase("norm")
    for c in range(nc):
        sl = pl.ds(c * Q, Q)
        gg = invs[sl, :] * gn[sl, :] - gated[sl, :] * to_column(ip_row, c)
        zv = gz[sl, :].astype(F32)
        sg = sigmoid(zv)
        o_gz[sl, :] = gg * y[sl, :] * sg * (1.0 + zv * (1.0 - sg))
        gmv = gg * zv * sg
        gm[sl, :] = gmv
        c_t = jnp.transpose(bcv[sl, ns:])
        cf[c] = mm3(c_t, gmv * jnp.exp(lx[sl, :]))

    racc = cf[nc - 1]
    for c in reversed(range(nc - 1)):
        racc = cf[c] + jnp.exp(lx[pl.ds(c * Q + Q - 1, 1), :]) * racc
    re[...] = racc.reshape(n_seq, nrow, ch)

    phase("send_v")
    def v_copy(k):
        return remote(re.at[seq_peer(k)], rr.at[me], sm_r, k, "seq", seq_peer(k))

    def vb_copy(k):
        return remote(ren.at[seq_peer(k)], rin.at[me], sm_q, k, "seq", seq_peer(k))

    for k in range(1, n_seq):
        v_copy(k).start()
    rr[me] = re[me]
    stores[0].start()
    phase("g_second")
    g_second()
    phase("o_second")
    o_second()
    phase("intra")
    def back_inside(c, carry):
        sl = pl.ds(pl.multiple_of(c * Q, Q), Q)
        bmap, cmap = bcv[sl, :ns], bcv[sl, ns:]
        scores = mm3(cmap, bmap, NT)
        scores_t = mm3(bmap, cmap, NT)
        arow[...] = jnp.zeros((Q, LANES), F32)
        acol[...] = jnp.zeros((LANES, Q), F32)
        dga[...] = jnp.zeros((Q, Q), F32)
        for p in range(pairs):
            ps = slice(p * PAIR, (p + 1) * PAIR)
            g2 = gm[sl, ps]
            cross = mm3(g2, pair_stack(x[sl, ps] * st[sl, ps]), NT)
            both = []
            for i_h, h in enumerate((2 * p, 2 * p + 1)):
                diff = lx[sl, h * HEAD : h * HEAD + 1] - lt[c, h : h + 1, :]
                weighted = jnp.exp(jnp.where(upper, diff, -1e30)) * cross[:, i_h * Q : (i_h + 1) * Q]
                dga[...] += weighted
                term = weighted * scores
                arow[...] += jnp.where(lane == h, jnp.sum(term, axis=1, keepdims=True), 0.0)
                acol[h : h + 1, :] = jnp.sum(term, axis=0, keepdims=True)
                decay_t = jnp.exp(jnp.where(lower, lt[c, h : h + 1, :] - lx[sl, h * HEAD : h * HEAD + 1], -1e30))
                both.append((decay_t * scores_t).astype(BF16))
            y[sl, ps] = mm(jnp.concatenate(both, axis=1), pair_stack(g2))
        dgv = dga[...]
        swings[c] = arow[...] - jnp.transpose(acol[...])
        dmap[sl, :ns] = mm3(jnp.transpose(dgv), cmap)
        dmap[sl, ns:] = mm3(dgv, bmap)
        return carry

    def back_insides(first):
        def one(i, carry):
            return back_inside(first - i, carry)

        lax.fori_loop(0, nc // 2, one, 0)

    back_insides(nc - 1)
    back_insides(nc // 2 - 1)

    phase("wait_v")
    for k in range(1, n_seq):
        v_copy(k).wait_recv()
    acc = jnp.zeros((nrow, ch), F32)
    for j in reversed(range(n_seq)):
        ren[j] = acc
        acc = fade[j : j + 1] * acc + rr[j]
    for k in range(1, n_seq):
        vb_copy(k).start()
    rin[me] = ren[me]
    phase("o_third")
    o_third()
    phase("forward_part")
    to_head = (lax.rem(iota((2 * ch, LANES), 0), ch) // HEAD == iota((2 * ch, LANES), 1)).astype(BF16)
    neg_c = jnp.concatenate([negexp, jnp.zeros((1, LANES - heads), F32)], axis=1)
    blk = Q // n_tp
    tail_sum = jnp.concatenate([tri_u.astype(BF16)] * 3, axis=1)
    head_sum = jnp.concatenate([(iota((Q, Q), 0) > iota((Q, Q), 1)).astype(BF16)] * 3, axis=1)

    def by_head(v):
        return mm(jnp.concatenate(parts(v, 2), axis=1), to_head)

    def reads(c, carry):
        sl = pl.ds(pl.multiple_of(c * Q, Q), Q)
        cmap = bcv[sl, ns:]
        sv = sst[c]
        cum = lx[sl, :]
        gg = gm[sl, :] * jnp.exp(cum)
        gn[sl, :] = x[sl, :] * st[sl, :] * jnp.exp(cum[Q - 1 : Q, :] - cum)
        dmap[sl, ns:] += mm3(gg, sv, NT)
        swings[c] += by_head(gg * mm(cmap, sv))
        return carry

    lax.fori_loop(0, nc, reads, 0)


    phase("g_third")
    g_third()
    phase("wait_vb")
    for k in range(1, n_seq):
        vb_copy(k).wait_recv()
    phase("inter")
    rcur[...] = rin[...].reshape(ns, ch)
    def m_copy(c):
        return remote(qs.at[c, every, 1 - core], qm.at[c], sm_m, c, "tp", mate)

    def q_copy(c, k):
        y1 = step(yi, k)
        return remote(qs.at[c, y1, core], qr.at[c, yi], sm_p, c * side + k, "tp", y1 * 2 + core)

    def q_send(c):
        m_copy(c).wait_recv()
        for j in range(side):
            qs[c, j, core] += qm[c, j]
        for k in range(1, side):
            q_copy(c, k).start()
        qr[c, yi] = qs[c, yi, core]

    def a_copy(c, k):
        return remote(qa.at[my, c], qa.at[my, c], sm_a, c * n_tp + k, "tp", tp_peer(k))

    def a_send(c):
        for k in range(1, side):
            q_copy(c, k).wait_recv()
        total = qr[c, 0] + qr[c, 1] + qr[c, 2] + qr[c, 3]
        qa[my, c] = total.astype(BF16)
        for k in range(1, n_tp):
            a_copy(c, k).start()
        return total

    def back_b(i, carry):
        c = nc - 1 - i
        sl = pl.ds(pl.multiple_of(c * Q, Q), Q)
        rv = rcur[...]
        rst[c] = rv
        d_b = dmap[sl, :ns] + mm3(gn[sl, :], rv, NT)
        qs[c, :, :, :, :ns] = d_b.reshape(side, 2, blk, ns)
        qs[c, :, :, :, ns:] = dmap[sl, ns:].reshape(side, 2, blk, ns)
        m_copy(c).start()
        rcur[...] = cf[c] + jnp.exp(lx[pl.ds(c * Q + Q - 1, 1), :]) * rv

        @pl.when(i > 0)
        def _():
            q_send(c + 1)

        return carry

    lax.fori_loop(0, nc, back_b, 0)
    phase("g_fourth")
    g_fourth()
    phase("inter2")

    def back(i, carry):
        c = i
        sl = pl.ds(pl.multiple_of(c * Q, Q), Q)
        cum = lx[sl, :]
        last = cum[Q - 1 : Q, :]
        rv = rst[c]
        xv = x[sl, :]
        sx = st[sl, :]
        d_in = mm(bcv[sl, :ns], rv) * jnp.exp(last - cum)
        dxt = y[sl, :] + d_in
        uv = u[sl, :]
        su = sigmoid(uv)
        dus[sl, :] = (sx * dxt + skip_x * gm[sl, :]) * (su * (1.0 + uv * (1.0 - su)))
        per_head = by_head(jnp.concatenate([xv * sx * d_in, xv * dxt], axis=0))
        fixed = by_head(
            jnp.broadcast_to(jnp.sum(rv * sst[c], axis=0, keepdims=True) * jnp.exp(last), (8, ch))
        )[0:1]
        dld = (
            mm(tail_sum, jnp.concatenate(parts(swings[c], 3), axis=0))
            + mm(head_sum, jnp.concatenate(parts(per_head[:Q], 3), axis=0))
            + fixed
        )
        dstep = per_head[Q:] + dld * neg_c
        slope = sigmoid(raw[:, sl].astype(F32) + dt_col)
        o_gdt[:, sl] = jnp.transpose(dstep)[:heads] * slope

        @pl.when(i == 0)
        def _():
            q_send(0)
            edge_x.start()

        @pl.when(i < nc - 1)
        def _():
            a_send(nc - 1 - i)

        return carry

    edge_x = remote(dus.at[pl.ds(0, 8)], dus.at[pl.ds(rows, 8)], sm_h, 2, "seq", prv)
    lax.fori_loop(0, nc, back, 0)
    stores[5].start()
    phase("wait_q")

    def edge_b(j):
        return pltpu.make_async_remote_copy(
            src_ref=edge,
            dst_ref=dub.at[pl.ds(rows, 8)],
            send_sem=sm_e.at[j],
            recv_sem=sm_h.at[1, 3],
            device_id={"seq": prv, "tp": j},
            device_id_type=MESH,
        )

    qsum = a_send(0)
    ube = ub[pl.ds(0, 8), :]
    sbe = sigmoid(ube)
    edge[...] = qsum[0:8, :] * (sbe * (1.0 + ube * (1.0 - sbe)))

    @pl.when(my == 0)
    def _():
        for j in range(n_tp):
            edge_b(j).start()


    phase("o_last")
    o_last()
    phase("wait_e")
    edge_x.wait_recv()

    phase("convbx")
    def conv_back(ref, weights, out, c):
        base = pl.multiple_of(c * Q, Q)
        ext = ref[pl.ds(base, Q + 8), :]
        tail = jnp.where((c < nc - 1) | (me < n_seq - 1), ext[Q:], 0.0)
        ext = jnp.concatenate([ext[:Q], tail], axis=0)
        acc = weights[3:4, :] * ext[:Q]
        for k in range(3):
            acc = acc + weights[k : k + 1, :] * pltpu.roll(ext, Q + 8 - (3 - k), 0)[:Q]
        out[pl.ds(base, Q), :] = acc

    def conv_back_x(c, carry):
        conv_back(dus, cw, o_gx, c)
        return carry

    lax.fori_loop(0, nc, conv_back_x, 0)

    stores[1].start()
    stores[2].start()
    phase("g_last")
    g_last()
    phase("wait_a")
    for c in range(nc):
        for k in range(1, n_tp):
            a_copy(c, k).wait_recv()
    phase("dub")
    for c in range(nc):
        sl = pl.ds(c * Q, Q)
        ubv = ub[sl, :]
        sb = sigmoid(ubv)
        dub[sl, :] = qa[:, c].reshape(Q, 2 * ns).astype(F32) * (sb * (1.0 + ubv * (1.0 - sb)))

    phase("convbb")
    edge_b(0).wait_recv()

    def conv_back_b(c, carry):
        conv_back(dub, cwb, o_gbc, c)
        return carry

    stores[3].start()
    lax.fori_loop(0, nc, conv_back_b, 0)
    stores[4].start()

    phase("drain")
    halo_x.wait_send()
    halo_b.wait_send()
    edge_x.wait_send()

    @pl.when(my == 0)
    def _():
        for j in range(n_tp):
            edge_b(j).wait_send()

    for k in range(1, n_seq):
        for copy in (t_copy, s_copy, sb_copy, v_copy, vb_copy):
            copy(k).wait_send()
    for c in range(nc):
        m_copy(c).wait_send()
        for k in range(1, n_tp):
            a_copy(c, k).wait_send()
        for k in range(1, side):
            q_copy(c, k).wait_send()
    for copy in r_squares + r_inner:
        copy.wait_send()
    for copy in w_copies + d_copies + o_copies + g_copies:
        copy.wait_send()
    for store in stores:
        store.wait()
    phase("")


def publish(*refs):
    count = (len(refs) - 2) // 3
    sources, targets, held = refs[:count], refs[count : 2 * count], refs[2 * count : 3 * count]
    sem_in, sem_out = refs[-2:]
    moves = []
    for source, target, place in zip(sources, targets, held):
        rows = source.shape[0]
        pieces = 4 if rows * source.shape[1] > 200_000 else 1
        for i in range(pieces):
            part = pl.ds(i * (rows // pieces), rows // pieces)
            k = len(moves)
            moves.append(
                (
                    pltpu.make_async_copy(source.at[part], place.at[part], sem_in.at[k]),
                    pltpu.make_async_copy(place.at[part], target.at[part], sem_out.at[k]),
                )
            )
    for load, _ in moves:
        load.start()
    for load, store in moves:
        load.wait()
        store.start()
    for _, store in moves:
        store.wait()


def solution(mesh):
    n_seq, n_tp = mesh.shape["seq"], mesh.shape["tp"]

    def shards(
        inner_x,
        gate_z,
        proj_bc,
        dt_raw,
        a_log,
        dt_bias,
        d_skip,
        conv_x,
        bias_x,
        conv_bc,
        bias_bc,
        norm_gain,
        w_out,
        d_out,
    ):
        rows, ch = inner_x.shape
        heads = a_log.shape[0]
        ns2 = proj_bc.shape[1]
        ns = ns2 // 2
        nc = rows // Q
        nrow = ns // n_seq
        wrows, drows = w_out.shape[1], d_out.shape[1]
        w_t = w_out.T
        d_t = d_out.T.reshape(2, drows // 2, rows)

        big = pltpu.VMEM((rows, ch), F32)
        chunk_states = pltpu.VMEM((nc, ns, ch), F32)
        slices = pltpu.VMEM((n_seq, nrow, ch), F32)
        sem_s = pltpu.SemaphoreType.DMA((2, n_seq))
        sem_t = pltpu.SemaphoreType.DMA((2, n_tp))
        scratch = [
            pltpu.VMEM((drows, rows), BF16),
            big,
            big,
            pltpu.VMEM((rows, ns2), F32),
            pltpu.VMEM((heads, rows), F32),
            pltpu.VMEM((wrows, ch), F32),
            pltpu.VMEM((rows, ch), BF16),
            pltpu.VMEM((rows, ch), BF16),
            pltpu.VMEM((rows, ns2), BF16),
            pltpu.VMEM((heads, rows), BF16),
            pltpu.VMEM((4, ch), F32),
            pltpu.VMEM((ch // LANES, LANES), F32),
            pltpu.VMEM((4, ns2), F32),
            pltpu.VMEM((1, ns2), F32),
            pltpu.VMEM((ch // LANES, LANES), F32),
            pltpu.VMEM((1, heads), F32),
            pltpu.VMEM((1, heads), F32),
            pltpu.VMEM((1, heads), F32),
            pltpu.VMEM((4, 4, wrows, ch), BF16),
            pltpu.VMEM((4, 4, wrows, rows), BF16),
            pltpu.VMEM((16, ch), BF16),
            pltpu.VMEM((16, ns2), BF16),
            pltpu.VMEM((8, LANES), F32),
            pltpu.VMEM((n_seq, 8, LANES), F32),
            big,
            big,
            pltpu.VMEM((nc, heads, Q), F32),
            big,
            big,
            pltpu.VMEM((rows, ns2), F32),
            pltpu.VMEM((rows, ns2), F32),
            chunk_states,
            chunk_states,
            chunk_states,
            big,
            big,
            big,
            big,
            pltpu.VMEM((rows, ch), BF16),
            pltpu.VMEM((rows + 8, ch), F32),
            pltpu.VMEM((rows + 8, ns2), F32),
            pltpu.VMEM((ns, ch), F32),
            slices,
            slices,
            slices,
            slices,
            slices,
            slices,
            slices,
            slices,
            pltpu.VMEM((2, 8, rows), F32),
            pltpu.VMEM((2, n_tp, 8, rows), F32),
            pltpu.VMEM((4, 2, drows, rows), BF16),
            pltpu.VMEM((4, drows, rows), BF16),
            pltpu.VMEM((drows, rows), BF16),
            pltpu.VMEM((2, drows, rows), BF16),
            pltpu.VMEM((4, 4, wrows, ch), BF16),
            *[
                pltpu.VMEM(shape, BF16)
                for shape in 2
                * [
                    (4, wrows // 2, ch),
                    (2, 4, wrows // 2, ch),
                    (wrows // 2, ch),
                    (2, wrows // 2, ch),
                ]
            ],
            pltpu.VMEM((nc, 4, 2, Q // n_tp, ns2), F32),
            pltpu.VMEM((nc, 4, Q // n_tp, ns2), F32),
            pltpu.VMEM((nc, 4, Q // n_tp, ns2), F32),
            chunk_states,
            pltpu.VMEM((n_tp, nc, Q // n_tp, ns2), BF16),
            pltpu.VMEM((Q, LANES), F32),
            pltpu.VMEM((LANES, Q), F32),
            pltpu.VMEM((Q, Q), F32),
            pltpu.VMEM((rows, 1), F32),
            pltpu.VMEM((nc, Q, LANES), F32),
            pltpu.VMEM((rows, ns2), F32),
            pltpu.VMEM((8, ns2), F32),
            pltpu.SemaphoreType.DMA((2, nc)),
            pltpu.SemaphoreType.DMA((n_tp,)),
            pltpu.SemaphoreType.DMA((20,)),
            pltpu.SemaphoreType.DMA((2, 4)),
            sem_s,
            pltpu.SemaphoreType.DMA((2, 28)),
            sem_t,
            sem_s,
            sem_s,
            sem_s,
            sem_s,
            pltpu.SemaphoreType.DMA((2, 2 * n_tp)),
            sem_t,
            pltpu.SemaphoreType.DMA((2, 20)),
            pltpu.SemaphoreType.DMA((2, nc * n_tp)),
            pltpu.SemaphoreType.DMA((2, nc * n_tp)),
        ]
        out_t, g_x, g_z, g_bc, g_dt, g_w = pl.pallas_call(
            functools.partial(kernel, (n_seq, n_tp, ch * n_tp)),
            out_shape=[
                jax.ShapeDtypeStruct((drows, rows), BF16),
                jax.ShapeDtypeStruct((rows, ch), F32),
                jax.ShapeDtypeStruct((rows, ch), F32),
                jax.ShapeDtypeStruct((rows, ns2), F32),
                jax.ShapeDtypeStruct((heads, rows), F32),
                jax.ShapeDtypeStruct((wrows, ch), F32),
            ],
            in_specs=[pl.BlockSpec(memory_space=pltpu.HBM)] * 14,
            out_specs=[pl.BlockSpec(memory_space=pltpu.HBM)] * 6,
            scratch_shapes=scratch,
            compiler_params=pltpu.CompilerParams(
                collective_id=0, has_side_effects=True, vmem_limit_bytes=62 * 1024 * 1024
            ),
            name="mixer",
        )(
            inner_x,
            gate_z,
            proj_bc,
            dt_raw.T,
            w_t,
            d_t,
            conv_x,
            bias_x.reshape(-1, LANES),
            conv_bc,
            bias_bc[None, :],
            norm_gain.reshape(-1, LANES),
            a_log[None, :],
            dt_bias[None, :],
            d_skip[None, :],
        )
        results = (g_x, g_z, g_bc, g_w, out_t, g_dt)
        hbm = pl.BlockSpec(memory_space=pltpu.HBM)
        g_x, g_z, g_bc, g_w, out_t, g_dt = pl.pallas_call(
            publish,
            out_shape=[jax.ShapeDtypeStruct(v.shape, v.dtype) for v in results],
            in_specs=[hbm] * 6,
            out_specs=[hbm] * 6,
            scratch_shapes=[pltpu.VMEM(v.shape, v.dtype) for v in results]
            + [pltpu.SemaphoreType.DMA((16,)), pltpu.SemaphoreType.DMA((16,))],
            compiler_params=pltpu.CompilerParams(vmem_limit_bytes=62 * 1024 * 1024),
            name="publish",
        )(*results)
        return out_t.T, g_x, g_z, g_bc, g_dt.T, g_w.T

    in_specs = (
        P("seq", "tp"),
        P("seq", "tp"),
        P("seq", None),
        P("seq", "tp"),
        P("tp"),
        P("tp"),
        P("tp"),
        P(None, "tp"),
        P("tp"),
        P(),
        P(),
        P("tp"),
        P("tp", "seq"),
        P("seq", "tp"),
    )
    out_specs = (
        P("seq", "tp"),
        P("seq", "tp"),
        P("seq", "tp"),
        P("seq", None),
        P("seq", "tp"),
        P("tp", "seq"),
    )
    return jax.shard_map(
        shards, mesh=mesh, in_specs=in_specs, out_specs=out_specs, check_vma=False
    )
```

```python
import functools

import jax
import jax.numpy as jnp
from jax import lax
from jax.experimental import pallas as pl
from jax.experimental.pallas import tpu as pltpu
from jax.sharding import PartitionSpec as P

MESH = pl.DeviceIdType.MESH
F32 = jnp.float32
BF16 = jnp.bfloat16
HIGH = lax.Precision.HIGHEST
EPSILON = 1e-05
NN = ((1,), (0,))
NT = ((1,), (1,))
Q = 128
PAIR = 128
HEAD = 64
LANES = 128


def mm(a, b, dims=NN):
    return lax.dot_general(a.astype(BF16), b.astype(BF16), (dims, ((), ())), preferred_element_type=F32)


def mmh(a, b, dims=NN):
    return lax.dot_general(
        a.astype(F32), b.astype(F32), (dims, ((), ())), precision=HIGH, preferred_element_type=F32
    )


def halves(v):
    high = v.astype(BF16)
    return high, (v - high.astype(F32)).astype(BF16)


def mm3(a, b, dims=NN):
    a0, a1 = halves(a)
    b0, b1 = halves(b)
    return mm(a0, b0, dims) + (mm(a1, b0, dims) + mm(a0, b1, dims))


def parts(v, count):
    out = []
    for _ in range(count):
        piece = v.astype(BF16)
        out.append(piece)
        v = v - piece.astype(F32)
    return out


def iota(shape, dim):
    return lax.broadcasted_iota(jnp.int32, shape, dim)


def sigmoid(v):
    return 1.0 / (1.0 + jnp.exp(-v))


def softplus(v):
    return jnp.maximum(v, 0.0) + jnp.log1p(jnp.exp(-jnp.abs(v)))


def pair_stack(v):
    lane = iota(v.shape, 1)
    return jnp.concatenate(
        [jnp.where(lane < HEAD, v, 0.0), jnp.where(lane >= HEAD, v, 0.0)], axis=0
    )


def kernel(
    sizes,
    ix_in,
    gz_in,
    bc_in,
    raw_in,
    wt,
    dt,
    cw_in,
    bx_in,
    cwb_in,
    bb_in,
    gain_in,
    al_in,
    db_in,
    ds_in,
    out_hbm,
    gx_hbm,
    gz_hbm,
    gbc_hbm,
    gdt_hbm,
    gw_hbm,
    o_out,
    o_gx,
    o_gz,
    o_gbc,
    o_gdt,
    o_gw,
    ix,
    gz,
    bc,
    raw,
    cw,
    bx,
    cwb,
    bb,
    gain,
    al,
    db,
    ds,
    wfull,
    dfull,
    hx,
    hb,
    dsend,
    dbuf,
    st,
    lx,
    lt,
    u,
    x,
    ub,
    bcv,
    fr,
    sst,
    cf,
    y,
    gated,
    gn,
    gm,
    nb,
    dus,
    dub,
    rcur,
    se,
    sr,
    en,
    sin,
    re,
    rr,
    ren,
    rin,
    ts,
    tr,
    pb,
    pp,
    po1,
    po2,
    gb,
    ga1,
    ga2,
    ga3,
    ga4,
    gb1,
    gb2,
    gb3,
    gb4,
    qs,
    qm,
    qr,
    rst,
    qa,
    arow,
    acol,
    dga,
    invs,
    swings,
    dmap,
    edge,
    frow,
    packed,
    sm_m,
    sm_e,
    sm_l,
    sm_h,
    sm_d,
    sm_w,
    sm_g,
    sm_s,
    sm_b,
    sm_r,
    sm_q,
    sm_t,
    sm_o,
    sm_v,
    sm_p,
    sm_a,
):
    n_seq, n_tp, inner = sizes
    rows, ch = ix.shape
    nc = rows // Q
    heads = raw.shape[0]
    pairs = ch // PAIR
    ns = bc.shape[1] // 2
    me, my = lax.axis_index("seq"), lax.axis_index("tp")
    wrows = wt.shape[0]
    drows = 2 * dt.shape[1]
    nrow = ns // n_seq

    scope = []

    def phase(name):
        if scope:
            scope.pop().__exit__(None, None, None)
        if name:
            scope.append(jax.named_scope(name))
            scope[0].__enter__()

    side = 4
    zi, xi = lax.div(me, side), lax.rem(me, side)
    yi, core = lax.div(my, 2), lax.rem(my, 2)

    def step(v, k):
        return lax.rem(v + k + side, side)

    x_up, x_dn = step(xi, 1), step(xi, -1)
    z_up, z_dn = step(zi, 1), step(zi, -1)
    y_up, y_dn = step(yi, 1), step(yi, -1)
    x_far, z_far, y_far = step(xi, 2), step(zi, 2), step(yi, 2)
    to_xu, to_xd = zi * side + x_up, zi * side + x_dn
    to_zu, to_zd = z_up * side + xi, z_dn * side + xi
    to_xf, to_zf = zi * side + x_far, z_far * side + xi
    to_yu, to_yd = y_up * 2 + core, y_dn * 2 + core
    mate = yi * 2 + 1 - core

    def hops(pair):
        return sum(min(v, side - v) for v in pair)

    others = [(a, b) for a in range(side) for b in range(side) if a or b]
    others.sort(key=lambda pair: -hops(pair))

    def seq_peer(k):
        a, b = others[k - 1]
        return step(zi, a) * side + step(xi, b)

    def tp_peer(k):
        return lax.rem(my + k, n_tp)

    phase("barrier1")
    barrier = pltpu.get_barrier_semaphore()
    for k in range(1, n_seq):
        pl.semaphore_signal(barrier, inc=1, device_id={"seq": seq_peer(k)}, device_id_type=MESH)
    for k in range(1, n_tp):
        pl.semaphore_signal(barrier, inc=1, device_id={"tp": tp_peer(k)}, device_id_type=MESH)

    def remote(src, dst, sems, k, axis, peer):
        return pltpu.make_async_remote_copy(
            src_ref=src,
            dst_ref=dst,
            send_sem=sems.at[0, k],
            recv_sem=sems.at[1, k],
            device_id={axis: peer},
            device_id_type=MESH,
        )

    nxt, prv = lax.rem(me + 1, n_seq), lax.rem(me + n_seq - 1, n_seq)

    @pl.when(my > 0)
    def _():
        pl.semaphore_signal(barrier, inc=1, device_id={"seq": nxt, "tp": 0}, device_id_type=MESH)

    staged = [
        (raw_in, raw),
        (al_in, al),
        (db_in, db),
        (ds_in, ds),
        (wt, wfull.at[zi, xi]),
        (dt, dfull.at[yi, pl.ds(2 * core, 2)]),
        (ix_in, ix),
        (bc_in, bc),
        (cw_in, cw),
        (bx_in, bx),
        (cwb_in, cwb),
        (bb_in, bb),
        (gain_in, gain),
        (gz_in, gz),
    ]
    loads = [pltpu.make_async_copy(a, b, sm_l.at[i]) for i, (a, b) in enumerate(staged)]
    for load in loads:
        load.start()
    results = [(o_gz, gz_hbm), (o_out, out_hbm), (o_gx, gx_hbm), (o_gw, gw_hbm), (o_gbc, gbc_hbm), (o_gdt, gdt_hbm)]
    stores = [pltpu.make_async_copy(a, b, sm_l.at[14 + i]) for i, (a, b) in enumerate(results)]
    phase("staging")
    for load in loads[:9]:
        load.wait()
    phase("barrier")
    pl.semaphore_wait(barrier, n_seq + n_tp - 2 + jnp.where(my == 0, n_tp - 1, 0))

    phase("start")
    halo_x = remote(ix.at[pl.ds(rows - 16, 16)], hx, sm_h, 0, "seq", nxt)
    halo_b = remote(bc.at[pl.ds(rows - 16, 16)], hb, sm_h, 1, "seq", nxt)
    halo_x.start()
    halo_b.start()

    half = wrows // 2
    near = 48
    ra, rb = pl.ds(0, half), pl.ds(half, half)
    ra1, ra2 = pl.ds(0, near), pl.ds(near, half - near)
    rb1, rb2 = pl.ds(half, near), pl.ds(half + near, half - near)
    lo, hi, every = pl.ds(0, 2), pl.ds(2, 2), pl.ds(0, side)

    def w_view(z, x, r):
        return wfull.at[z, x, r]

    def w_move(i, peer, z, x, r, src=None):
        return remote(w_view(z, x, r) if src is None else src, w_view(z, x, r), sm_w, i, "seq", peer)

    w_copies = [
        w_move(0, to_xu, zi, xi, ra),
        w_move(1, to_xd, zi, xi, ra),
        w_move(2, to_zu, zi, xi, rb),
        w_move(3, to_zd, zi, xi, rb),
        w_move(4, to_zu, zi, xi, ra),
        w_move(5, to_zd, zi, xi, ra),
        w_move(6, to_xu, zi, xi, rb),
        w_move(7, to_xd, zi, xi, rb),
        w_move(8, to_xu, zi, x_dn, ra1),
        w_move(9, to_xd, zi, x_up, ra2),
        w_move(10, to_zu, z_dn, xi, rb1),
        w_move(11, to_zd, z_up, xi, rb2),
        w_move(12, to_zu, zi, x_up, ra),
        w_move(13, to_zd, zi, x_up, ra),
        w_move(14, to_xu, z_up, xi, rb),
        w_move(15, to_xd, z_up, xi, rb),
        w_move(16, to_zu, zi, x_dn, ra),
        w_move(17, to_zd, zi, x_dn, ra),
        w_move(18, to_xu, z_dn, xi, rb),
        w_move(19, to_xd, z_dn, xi, rb),
        w_move(20, to_zu, zi, x_far, ra),
        w_move(21, to_zd, zi, x_far, ra),
        w_move(22, to_xu, z_far, xi, rb),
        w_move(23, to_xd, z_far, xi, rb),
        w_move(24, to_zu, z_dn, lo, ra),
        w_move(25, to_zd, z_up, hi, ra),
        w_move(26, to_xu, lo, x_dn, rb),
        w_move(27, to_xd, hi, x_up, rb),
    ]

    dhalf = drows // 2

    def d_view(y, c, off=0, size=drows):
        if size == drows:
            return dfull.at[y, pl.ds(2 * c, 2)]
        return dfull.at[y, 2 * c + off // size]

    def d_move(i, peer, y, c, off=0, size=drows, src=None):
        view = d_view(y, c, off, size)
        return remote(view if src is None else src, view, sm_g, i, "tp", peer)

    d_copies = [
        d_move(0, to_yu, yi, core),
        d_move(1, to_yd, yi, core),
        d_move(2, mate, yi, core),
        d_move(3, to_yu, y_dn, core, 0, dhalf),
        d_move(4, to_yd, y_up, core, dhalf, dhalf),
        d_move(5, mate, y_dn, core),
        d_move(6, mate, y_up, core),
        d_move(7, mate, y_far, core),
    ]

    def start(copies, first, last):
        for copy in copies[first:last]:
            copy.start()

    def arrived(copies, first, last):
        for copy in copies[first:last]:
            copy.wait_recv()

    start(w_copies, 0, 8)
    start(d_copies, 0, 3)

    phase("steps")
    slot = lax.rem(iota((LANES, 2 * ch), 0), 32)
    wanted = iota((LANES, 2 * ch), 1) // HEAD
    wanted = jnp.where(wanted < heads, wanted, wanted - heads + 16)
    spread = ((slot == wanted) & (iota((LANES, 2 * ch), 0) < 96)).astype(BF16)
    spread_h = (iota((heads, ch), 1) // HEAD == iota((heads, ch), 0)).astype(F32)
    ident = (iota((heads, heads), 0) == iota((heads, heads), 1)).astype(F32)
    negexp = -jnp.exp(al[...])
    skip_x = mmh(jnp.broadcast_to(ds[...], (8, heads)), spread_h)[0:1]
    tri_u = (iota((Q, Q), 0) <= iota((Q, Q), 1)).astype(F32)

    def column(v):
        return mmh(ident, jnp.broadcast_to(v, (8, heads)), NT)[:, 0:1]

    def in_line(ref):
        return jnp.concatenate([ref[i : i + 1] for i in range(ref.shape[0])], axis=1)

    dt_col, neg_col = column(db[...]), column(negexp)

    for load in loads[9:]:
        load.wait()
    bias_line, gain_line = in_line(bx), in_line(gain)

    def steps(c, total):
        sl = pl.ds(pl.multiple_of(c * Q, Q), Q)
        s_c = softplus(raw[:, sl].astype(F32) + dt_col)
        cum = mmh(s_c * neg_col, tri_u)
        lt[c] = cum
        gap = jnp.zeros((16 - heads, Q), F32)
        pieces = []
        for a, b in zip(parts(s_c, 3), parts(cum, 3)):
            pieces += [a.astype(F32), gap, b.astype(F32), gap]
        turned = jnp.transpose(jnp.concatenate([*pieces, jnp.zeros((LANES - 96, Q), F32)], axis=0))
        packed[sl, :] = turned.astype(BF16)
        return total + turned[Q - 1 : Q, :]

    total = lax.fori_loop(0, nc, steps, jnp.zeros((1, LANES), F32))
    st[...] = mm(packed[...], spread[:, :ch])
    lx[...] = mm(packed[...], spread[:, ch:])
    dsend[...] = jnp.broadcast_to(total, (8, LANES))
    dbuf[me] = dsend[...]

    def t_copy(k):
        return remote(dsend, dbuf.at[me], sm_d, k, "seq", seq_peer(k))

    for k in range(1, n_seq):
        t_copy(k).start()

    phase("convs")
    def conv_of(ref, halo, weights, bias, c):
        base = pl.multiple_of(c * Q, Q)
        own = ref[pl.ds(base, Q), :].astype(F32)
        if halo is None:
            head = ref[pl.ds(pl.multiple_of(c * Q - 16, 16), 16), :].astype(F32)[8:16]
        else:
            head = jnp.where(me > 0, halo[...].astype(F32), 0.0)[8:16]
        ext = jnp.concatenate([head, own], axis=0)
        acc = bias + weights[3:4, :] * own
        for k in range(3):
            acc = acc + weights[k : k + 1, :] * pltpu.roll(ext, Q + 8 - (5 + k), 0)[:Q]
        return acc

    def convs(c, carry, edge_of=(None, None)):
        sl = pl.ds(pl.multiple_of(c * Q, Q), Q)
        vb = conv_of(bc, edge_of[0], cwb, bb[...], c)
        ub[sl, :] = vb
        pbc = vb * sigmoid(vb)
        bcv[sl, :] = pbc
        vx = conv_of(ix, edge_of[1], cw, bias_line, c)
        u[sl, :] = vx
        xv = vx * sigmoid(vx)
        x[sl, :] = xv
        cum = lx[sl, :]
        to_end = jnp.exp(cum[Q - 1 : Q, :] - cum)
        b_t = jnp.transpose(pbc[:, :ns])
        fresh = mm3(b_t, xv * st[sl, :] * to_end)
        fr[c] = fresh
        return carry

    lax.fori_loop(1, nc, convs, 0)
    phase("wait_halo")
    halo_x.wait_recv()
    halo_b.wait_recv()
    phase("conv0")
    convs(0, 0, (hb, hx))
    end = fr[0]
    for c in range(1, nc):
        end = jnp.exp(lx[pl.ds(c * Q + Q - 1, 1), :]) * end + fr[c]
    se[...] = end.reshape(n_seq, nrow, ch)

    phase("send_s")
    def s_copy(k):
        return remote(se.at[seq_peer(k)], sr.at[me], sm_s, k, "seq", seq_peer(k))

    def sb_copy(k):
        return remote(en.at[seq_peer(k)], sin.at[me], sm_b, k, "seq", seq_peer(k))

    for k in range(1, n_seq):
        s_copy(k).start()
    sr[me] = se[me]
    phase("wait_w1")
    arrived(w_copies, 0, 4)
    start(w_copies, 8, 16)

    upper = iota((Q, Q), 0) >= iota((Q, Q), 1)
    lower = iota((Q, Q), 0) <= iota((Q, Q), 1)

    phase("inside")
    def inside(c, carry):
        sl = pl.ds(pl.multiple_of(c * Q, Q), Q)
        scores = mm3(bcv[sl, ns:], bcv[sl, :ns], NT)
        for p in range(pairs):
            ps = slice(p * PAIR, (p + 1) * PAIR)
            both = []
            for h in (2 * p, 2 * p + 1):
                diff = lx[sl, h * HEAD : h * HEAD + 1] - lt[c, h : h + 1, :]
                decay = jnp.exp(jnp.where(upper, diff, -1e30))
                both.append(decay * scores)
            y[sl, ps] = mm3(jnp.concatenate(both, axis=1), pair_stack(x[sl, ps] * st[sl, ps]))
        return carry

    lax.fori_loop(0, nc, inside, 0)
    phase("wait_d1")
    arrived(d_copies, 0, 2)
    start(d_copies, 3, 7)
    phase("wait_s")
    for k in range(1, n_seq):
        t_copy(k).wait_recv()
    for k in range(1, n_seq):
        s_copy(k).wait_recv()
    phase("scan")
    fade = jnp.exp(sum(mm(piece, spread[:, ch:]) for piece in parts(dbuf[:, 0, :], 3)))

    acc = jnp.zeros((nrow, ch), F32)
    for j in range(n_seq):
        en[j] = acc
        acc = fade[j : j + 1] * acc + sr[j]
    for k in range(1, n_seq):
        sb_copy(k).start()
    sin[me] = en[me]
    start(w_copies, 16, 20)
    phase("wait_w2")
    arrived(w_copies, 8, 12)
    start(w_copies, 20, 24)

    phase("wait_sb")
    for k in range(1, n_seq):
        sb_copy(k).wait_recv()
    phase("combine")
    lane = iota((Q, LANES), 1)

    def to_row(i, c, v):
        ts[i, :, pl.ds(pl.multiple_of(c * Q, Q), Q)] = jnp.transpose(jnp.where(lane == 0, v, 0.0))[:8]

    def to_column(row, c):
        block = jnp.concatenate([row[:, c * Q : (c + 1) * Q], jnp.zeros((Q - 8, Q), F32)], axis=0)
        return jnp.transpose(block)[:, 0:1]

    def combine(c, state):
        sl = pl.ds(pl.multiple_of(c * Q, Q), Q)
        sst[c] = state
        cum = lx[sl, :]
        mixed = y[sl, :] + jnp.exp(cum) * mm3(bcv[sl, ns:], state) + skip_x * x[sl, :]
        y[sl, :] = mixed
        zv = gz[sl, :].astype(F32)
        gv = mixed * zv * sigmoid(zv)
        gated[sl, :] = gv
        to_row(0, c, jnp.sum(gv * gv, axis=1, keepdims=True))
        return jnp.exp(cum[Q - 1 : Q, :]) * state + fr[c]

    lax.fori_loop(0, nc, combine, sin[...].reshape(ns, ch))

    def r_copies(i):
        return [
            remote(ts.at[i], tr.at[i, my], sm_t, i * n_tp + k, "tp", tp_peer(k)) for k in range(1, n_tp)
        ]

    def r_total(i):
        total = tr[i, 0]
        for j in range(1, n_tp):
            total = total + tr[i, j]
        return total

    r_squares, r_inner = r_copies(0), r_copies(1)
    start(r_squares, 0, n_tp - 1)
    tr[0, my] = ts[0]

    phase("wait_d2")
    arrived(d_copies, 3, 5)
    start(d_copies, 7, 8)
    phase("wait_w3")
    arrived(w_copies, 4, 8)
    arrived(w_copies, 12, 24)
    start(w_copies, 24, 28)
    phase("wait_d")
    arrived(d_copies, 2, 3)
    arrived(d_copies, 5, 8)
    phase("gn")
    kb = wrows * side

    def gn_add(part, first):
        @pl.when(first)
        def _():
            gn[...] = part

        @pl.when(jnp.logical_not(first))
        def _():
            gn[...] += part

    def gn_early(k, carry):
        zz, xx = step(zi, k - 1), step(xi, k - 1)
        d_rows = jnp.concatenate(
            [dfull[zz, :, ra].reshape(kb // 2, rows), dfull[:, xx, rb].reshape(kb // 2, rows)], axis=0
        )
        w_rows = jnp.concatenate(
            [wfull[zz, :, ra].reshape(kb // 2, ch), wfull[:, xx, rb].reshape(kb // 2, ch)], axis=0
        )
        gn_add(mm(jnp.transpose(d_rows), w_rows), k == 0)
        return carry

    lax.fori_loop(0, 3, gn_early, 0)

    phase("wait_ss")
    arrived(r_squares, 0, n_tp - 1)
    inv_row = lax.rsqrt(r_total(0) / inner + EPSILON)
    phase("nb")
    for c in range(nc):
        sl = pl.ds(c * Q, Q)
        inv = to_column(inv_row, c)
        invs[sl, :] = inv
        nb[sl, :] = (gated[sl, :] * inv * gain_line).astype(BF16)
    phase("gradw")
    g_copies = [
        remote(gb.at[z_far, lo, ra], ga1.at[lo], sm_v, 0, "seq", to_zu),
        remote(gb.at[z_far, hi, ra], ga1.at[hi], sm_v, 1, "seq", to_zd),
        remote(gb.at[lo, x_far, rb], gb1.at[lo], sm_v, 2, "seq", to_xu),
        remote(gb.at[hi, x_far, rb], gb1.at[hi], sm_v, 3, "seq", to_xd),
        remote(gb.at[z_up, hi, ra], ga2.at[0, hi], sm_v, 4, "seq", to_zu),
        remote(gb.at[z_dn, lo, ra], ga2.at[1, lo], sm_v, 5, "seq", to_zd),
        remote(gb.at[hi, x_up, rb], gb2.at[0, hi], sm_v, 6, "seq", to_xu),
        remote(gb.at[lo, x_dn, rb], gb2.at[1, lo], sm_v, 7, "seq", to_xd),
        remote(gb.at[z_up, 0, ra], ga2.at[0, 0], sm_v, 8, "seq", to_zu),
        remote(gb.at[z_dn, 2, ra], ga2.at[1, 2], sm_v, 9, "seq", to_zd),
        remote(gb.at[0, x_up, rb], gb2.at[0, 0], sm_v, 10, "seq", to_xu),
        remote(gb.at[2, x_dn, rb], gb2.at[1, 2], sm_v, 11, "seq", to_xd),
        remote(gb.at[z_up, 1, ra], ga2.at[0, 1], sm_v, 20, "seq", to_zu),
        remote(gb.at[z_dn, 3, ra], ga2.at[1, 3], sm_v, 21, "seq", to_zd),
        remote(gb.at[1, x_up, rb], gb2.at[0, 1], sm_v, 22, "seq", to_xu),
        remote(gb.at[3, x_dn, rb], gb2.at[1, 3], sm_v, 23, "seq", to_xd),
        remote(gb.at[zi, x_far, ra], ga3, sm_v, 12, "seq", to_xf),
        remote(gb.at[z_far, xi, rb], gb3, sm_v, 13, "seq", to_zf),
        remote(gb.at[zi, x_up, ra], ga4.at[0], sm_v, 14, "seq", to_xu),
        remote(gb.at[zi, x_dn, ra], ga4.at[1], sm_v, 15, "seq", to_xd),
        remote(gb.at[z_up, xi, rb], gb4.at[0], sm_v, 16, "seq", to_zu),
        remote(gb.at[z_dn, xi, rb], gb4.at[1], sm_v, 17, "seq", to_zd),
    ]

    def plus(ref, index, *others):
        total = ref[index].astype(F32)
        for part in others:
            total = total + part.astype(F32)
        ref[index] = total.astype(BF16)

    def g_block(k, carry):
        b = step(zi, 2 + k)
        gb[b] = mm(dfull[b].reshape(kb, rows), nb[...]).astype(BF16).reshape(side, wrows, ch)

        @pl.when(k == 0)
        def _():
            start(g_copies, 0, 2)

        return carry

    lax.fori_loop(0, side, g_block, 0)
    start(g_copies, 2, 8)

    def g_second():
        arrived(g_copies, 0, 4)
        for j in range(2):
            plus(gb, (z_up, j, ra), ga1[j])
            plus(gb, (z_dn, 2 + j, ra), ga1[2 + j])
            plus(gb, (j, x_up, rb), gb1[j])
            plus(gb, (2 + j, x_dn, rb), gb1[2 + j])
        start(g_copies, 8, 12)

    def g_third():
        arrived(g_copies, 4, 16)
        for j in range(side):
            plus(gb, (zi, j, ra), ga2[0, j], ga2[1, j])
            plus(gb, (j, xi, rb), gb2[0, j], gb2[1, j])
        start(g_copies, 16, 22)

    def g_last():
        arrived(g_copies, 16, 22)

        def landed(own, far, near):
            return own.astype(F32) + far.astype(F32) + near[0].astype(F32) + near[1].astype(F32)

        o_gw[ra, :] = landed(gb[zi, xi, ra], ga3[...], ga4)
        o_gw[rb, :] = landed(gb[zi, xi, rb], gb3[...], gb4)

    def o_second():
        arrived(o_copies, 0, 1)
        for j in range(side):
            plus(pb, (j, core), pp[j])
        start(o_copies, 1, 3)

    def o_third():
        arrived(o_copies, 1, 3)
        plus(pb, (y_up, core, o_half1), po1[o_half1])
        plus(pb, (y_dn, core, o_half2), po1[o_half2])
        start(o_copies, 3, 5)

    def o_last():
        arrived(o_copies, 3, 5)
        total = pb[yi, core].astype(F32) + po2[0].astype(F32) + po2[1].astype(F32)
        o_out[...] = total.astype(BF16)
    phase("wait_w4")
    arrived(w_copies, 24, 28)
    phase("gn_last")
    gn_early(3, 0)
    phase("ip")

    def inner_sums(c, carry):
        sl = pl.ds(pl.multiple_of(c * Q, Q), Q)
        scaled = gn[sl, :] * gain_line
        gn[sl, :] = scaled
        to_row(1, c, jnp.sum(scaled * gated[sl, :], axis=1, keepdims=True))
        return carry

    lax.fori_loop(0, nc, inner_sums, 0)
    start(r_inner, 0, n_tp - 1)
    tr[1, my] = ts[1]
    phase("outmm")
    def share(y0, c0):
        block = wfull[y0, pl.ds(2 * c0, 2)].reshape(drows, ch)
        pb[y0, c0] = mm(block, nb[...], NT).astype(BF16)

    def other(j, carry):
        share(j, 1 - core)
        return carry

    def same(j, carry):
        share(j, core)
        return carry

    o_half1, o_half2 = pl.ds(0, dhalf), pl.ds(dhalf, dhalf)
    o_copies = [
        remote(pb.at[every, 1 - core], pp, sm_o, 0, "tp", mate),
        remote(pb.at[y_far, core, o_half1], po1.at[o_half1], sm_o, 1, "tp", to_yu),
        remote(pb.at[y_far, core, o_half2], po1.at[o_half2], sm_o, 2, "tp", to_yd),
        remote(pb.at[y_up, core], po2.at[0], sm_o, 3, "tp", to_yu),
        remote(pb.at[y_dn, core], po2.at[1], sm_o, 4, "tp", to_yd),
    ]
    lax.fori_loop(0, side, other, 0)
    start(o_copies, 0, 1)
    lax.fori_loop(0, side, same, 0)
    phase("wait_ip")
    arrived(r_inner, 0, n_tp - 1)
    ip_row = r_total(1) / inner * inv_row * inv_row * inv_row
    phase("norm")
    for c in range(nc):
        sl = pl.ds(c * Q, Q)
        gg = invs[sl, :] * gn[sl, :] - gated[sl, :] * to_column(ip_row, c)
        zv = gz[sl, :].astype(F32)
        sg = sigmoid(zv)
        o_gz[sl, :] = gg * y[sl, :] * sg * (1.0 + zv * (1.0 - sg))
        gmv = gg * zv * sg
        gm[sl, :] = gmv
        c_t = jnp.transpose(bcv[sl, ns:])
        cf[c] = mm3(c_t, gmv * jnp.exp(lx[sl, :]))

    racc = cf[nc - 1]
    for c in reversed(range(nc - 1)):
        racc = cf[c] + jnp.exp(lx[pl.ds(c * Q + Q - 1, 1), :]) * racc
    re[...] = racc.reshape(n_seq, nrow, ch)

    phase("send_v")
    def v_copy(k):
        return remote(re.at[seq_peer(k)], rr.at[me], sm_r, k, "seq", seq_peer(k))

    def vb_copy(k):
        return remote(ren.at[seq_peer(k)], rin.at[me], sm_q, k, "seq", seq_peer(k))

    for k in range(1, n_seq):
        v_copy(k).start()
    rr[me] = re[me]
    stores[0].start()
    phase("g_second")
    g_second()
    phase("o_second")
    o_second()
    phase("intra")
    def back_inside(c, carry):
        sl = pl.ds(pl.multiple_of(c * Q, Q), Q)
        bmap, cmap = bcv[sl, :ns], bcv[sl, ns:]
        scores = mm3(cmap, bmap, NT)
        scores_t = mm3(bmap, cmap, NT)
        arow[...] = jnp.zeros((Q, LANES), F32)
        acol[...] = jnp.zeros((LANES, Q), F32)
        dga[...] = jnp.zeros((Q, Q), F32)
        for p in range(pairs):
            ps = slice(p * PAIR, (p + 1) * PAIR)
            g2 = gm[sl, ps]
            cross = mm3(g2, pair_stack(x[sl, ps] * st[sl, ps]), NT)
            both = []
            for i_h, h in enumerate((2 * p, 2 * p + 1)):
                diff = lx[sl, h * HEAD : h * HEAD + 1] - lt[c, h : h + 1, :]
                weighted = jnp.exp(jnp.where(upper, diff, -1e30)) * cross[:, i_h * Q : (i_h + 1) * Q]
                dga[...] += weighted
                term = weighted * scores
                arow[...] += jnp.where(lane == h, jnp.sum(term, axis=1, keepdims=True), 0.0)
                acol[h : h + 1, :] = jnp.sum(term, axis=0, keepdims=True)
                decay_t = jnp.exp(jnp.where(lower, lt[c, h : h + 1, :] - lx[sl, h * HEAD : h * HEAD + 1], -1e30))
                both.append((decay_t * scores_t).astype(BF16))
            y[sl, ps] = mm(jnp.concatenate(both, axis=1), pair_stack(g2))
        dgv = dga[...]
        swings[c] = arow[...] - jnp.transpose(acol[...])
        dmap[sl, :ns] = mm3(jnp.transpose(dgv), cmap)
        dmap[sl, ns:] = mm3(dgv, bmap)
        return carry

    def back_insides(first):
        def one(i, carry):
            return back_inside(first - i, carry)

        lax.fori_loop(0, nc // 2, one, 0)

    back_insides(nc - 1)
    back_insides(nc // 2 - 1)

    phase("wait_v")
    for k in range(1, n_seq):
        v_copy(k).wait_recv()
    acc = jnp.zeros((nrow, ch), F32)
    for j in reversed(range(n_seq)):
        ren[j] = acc
        acc = fade[j : j + 1] * acc + rr[j]
    for k in range(1, n_seq):
        vb_copy(k).start()
    rin[me] = ren[me]
    start(g_copies, 12, 16)
    phase("o_third")
    o_third()
    phase("forward_part")
    to_head = (lax.rem(iota((2 * ch, LANES), 0), ch) // HEAD == iota((2 * ch, LANES), 1)).astype(BF16)
    neg_c = jnp.concatenate([negexp, jnp.zeros((1, LANES - heads), F32)], axis=1)
    blk = Q // n_tp
    tail_sum = jnp.concatenate([tri_u.astype(BF16)] * 3, axis=1)
    head_sum = jnp.concatenate([(iota((Q, Q), 0) > iota((Q, Q), 1)).astype(BF16)] * 3, axis=1)

    def by_head(v):
        return mm(jnp.concatenate(parts(v, 2), axis=1), to_head)

    def reads(i, later):
        c = nc - 1 - i
        sl = pl.ds(pl.multiple_of(c * Q, Q), Q)
        cmap = bcv[sl, ns:]
        sv = sst[c]
        cum = lx[sl, :]
        last = cum[Q - 1 : Q, :]
        gg = gm[sl, :] * jnp.exp(cum)
        dmap[sl, ns:] += mm3(gg, sv, NT)
        swings[c] += by_head(gg * mm(cmap, sv))
        rv = rcur[...]
        rst[c] = rv
        reach = x[sl, :] * st[sl, :] * jnp.exp(last - cum)
        dmap[sl, :ns] += mm3(reach, rv, NT)
        gn[sl, :] = reach * later
        frow[c] = jnp.broadcast_to(later, (8, ch))
        rcur[...] = cf[c] + jnp.exp(last) * rv
        return later * jnp.exp(last)

    rcur[...] = jnp.zeros((ns, ch), F32)
    lax.fori_loop(0, nc, reads, jnp.ones((1, ch), F32))
    phase("wait_vb")
    for k in range(1, n_seq):
        vb_copy(k).wait_recv()
    phase("inter")
    rcur[...] = rin[...].reshape(ns, ch)
    def m_copy(c):
        return remote(qs.at[c, every, 1 - core], qm.at[c], sm_m, c, "tp", mate)

    def q_copy(c, k):
        y1 = step(yi, k)
        return remote(qs.at[c, y1, core], qr.at[c, yi], sm_p, c * side + k, "tp", y1 * 2 + core)

    def q_send(c):
        m_copy(c).wait_recv()
        for j in range(side):
            qs[c, j, core] += qm[c, j]
        for k in range(1, side):
            q_copy(c, k).start()
        qr[c, yi] = qs[c, yi, core]

    def a_copy(c, k):
        return remote(qa.at[my, c], qa.at[my, c], sm_a, c * n_tp + k, "tp", tp_peer(k))

    def a_send(c):
        for k in range(1, side):
            q_copy(c, k).wait_recv()
        total = qr[c, 0] + qr[c, 1] + qr[c, 2] + qr[c, 3]
        qa[my, c] = total.astype(BF16)
        for k in range(1, n_tp):
            a_copy(c, k).start()
        return total

    def back_b(c, carry):
        sl = pl.ds(pl.multiple_of(c * Q, Q), Q)
        qs[c, :, :, :, :ns] = dmap[sl, :ns].reshape(side, 2, blk, ns)
        qs[c, :, :, :, ns:] = dmap[sl, ns:].reshape(side, 2, blk, ns)
        m_copy(c).start()
        return carry

    dmap[:, :ns] += mm3(gn[...], rcur[...], NT)
    lax.fori_loop(0, nc, back_b, 0)
    phase("inter2")

    def back(i, carry):
        c = i
        sl = pl.ds(pl.multiple_of(c * Q, Q), Q)
        cum = lx[sl, :]
        last = cum[Q - 1 : Q, :]
        rv = rst[c] + frow[c][0:1] * rcur[...]
        xv = x[sl, :]
        sx = st[sl, :]
        d_in = mm(bcv[sl, :ns], rv) * jnp.exp(last - cum)
        dxt = y[sl, :] + d_in
        uv = u[sl, :]
        su = sigmoid(uv)
        dus[sl, :] = (sx * dxt + skip_x * gm[sl, :]) * (su * (1.0 + uv * (1.0 - su)))
        per_head = by_head(jnp.concatenate([xv * sx * d_in, xv * dxt], axis=0))
        fixed = by_head(
            jnp.broadcast_to(jnp.sum(rv * sst[c], axis=0, keepdims=True) * jnp.exp(last), (8, ch))
        )[0:1]
        dld = (
            mm(tail_sum, jnp.concatenate(parts(swings[c], 3), axis=0))
            + mm(head_sum, jnp.concatenate(parts(per_head[:Q], 3), axis=0))
            + fixed
        )
        dstep = per_head[Q:] + dld * neg_c
        slope = sigmoid(raw[:, sl].astype(F32) + dt_col)
        o_gdt[:, sl] = jnp.transpose(dstep)[:heads] * slope

        @pl.when(i == 0)
        def _():
            for j in range(nc):
                q_send(j)
            edge_x.start()

        @pl.when(i == 1)
        def _():
            g_third()

        return carry

    edge_x = remote(dus.at[pl.ds(0, 8)], dus.at[pl.ds(rows, 8)], sm_h, 2, "seq", prv)
    lax.fori_loop(0, nc, back, 0)
    stores[5].start()
    phase("wait_q")

    def edge_b(j):
        return pltpu.make_async_remote_copy(
            src_ref=edge,
            dst_ref=dub.at[pl.ds(rows, 8)],
            send_sem=sm_e.at[j],
            recv_sem=sm_h.at[1, 3],
            device_id={"seq": prv, "tp": j},
            device_id_type=MESH,
        )

    qsum = a_send(0)
    a_send(1)
    for c in range(2, nc):
        a_send(c)
    ube = ub[pl.ds(0, 8), :]
    sbe = sigmoid(ube)
    edge[...] = qsum[0:8, :] * (sbe * (1.0 + ube * (1.0 - sbe)))

    @pl.when(my == 0)
    def _():
        for j in range(n_tp):
            edge_b(j).start()


    phase("o_last")
    o_last()
    phase("wait_e")
    edge_x.wait_recv()

    phase("convbx")
    def conv_back(ref, weights, out, c):
        base = pl.multiple_of(c * Q, Q)
        ext = ref[pl.ds(base, Q + 8), :]
        tail = jnp.where((c < nc - 1) | (me < n_seq - 1), ext[Q:], 0.0)
        ext = jnp.concatenate([ext[:Q], tail], axis=0)
        acc = weights[3:4, :] * ext[:Q]
        for k in range(3):
            acc = acc + weights[k : k + 1, :] * pltpu.roll(ext, Q + 8 - (3 - k), 0)[:Q]
        out[pl.ds(base, Q), :] = acc

    def conv_back_x(c, carry):
        conv_back(dus, cw, o_gx, c)
        return carry

    lax.fori_loop(0, nc, conv_back_x, 0)

    stores[1].start()
    stores[2].start()
    phase("g_last")
    g_last()
    phase("wait_a")
    for c in range(nc):
        for k in range(1, n_tp):
            a_copy(c, k).wait_recv()
    phase("dub")
    for c in range(nc):
        sl = pl.ds(c * Q, Q)
        ubv = ub[sl, :]
        sb = sigmoid(ubv)
        dub[sl, :] = qa[:, c].reshape(Q, 2 * ns).astype(F32) * (sb * (1.0 + ubv * (1.0 - sb)))

    phase("convbb")
    edge_b(0).wait_recv()

    def conv_back_b(c, carry):
        conv_back(dub, cwb, o_gbc, c)
        return carry

    stores[3].start()
    lax.fori_loop(0, nc, conv_back_b, 0)
    stores[4].start()

    phase("drain")
    halo_x.wait_send()
    halo_b.wait_send()
    edge_x.wait_send()

    @pl.when(my == 0)
    def _():
        for j in range(n_tp):
            edge_b(j).wait_send()

    for k in range(1, n_seq):
        for copy in (t_copy, s_copy, sb_copy, v_copy, vb_copy):
            copy(k).wait_send()
    for c in range(nc):
        m_copy(c).wait_send()
        for k in range(1, n_tp):
            a_copy(c, k).wait_send()
        for k in range(1, side):
            q_copy(c, k).wait_send()
    for copy in r_squares + r_inner:
        copy.wait_send()
    for copy in w_copies + d_copies + o_copies + g_copies:
        copy.wait_send()
    for store in stores:
        store.wait()
    phase("")


def publish(*refs):
    count = (len(refs) - 2) // 3
    sources, targets, held = refs[:count], refs[count : 2 * count], refs[2 * count : 3 * count]
    sem_in, sem_out = refs[-2:]
    moves = []
    for source, target, place in zip(sources, targets, held):
        rows = source.shape[0]
        pieces = 4 if rows * source.shape[1] > 200_000 else 1
        for i in range(pieces):
            part = pl.ds(i * (rows // pieces), rows // pieces)
            k = len(moves)
            moves.append(
                (
                    pltpu.make_async_copy(source.at[part], place.at[part], sem_in.at[k]),
                    pltpu.make_async_copy(place.at[part], target.at[part], sem_out.at[k]),
                )
            )
    for load, _ in moves:
        load.start()
    for load, store in moves:
        load.wait()
        store.start()
    for _, store in moves:
        store.wait()


def solution(mesh):
    n_seq, n_tp = mesh.shape["seq"], mesh.shape["tp"]

    def shards(
        inner_x,
        gate_z,
        proj_bc,
        dt_raw,
        a_log,
        dt_bias,
        d_skip,
        conv_x,
        bias_x,
        conv_bc,
        bias_bc,
        norm_gain,
        w_out,
        d_out,
    ):
        rows, ch = inner_x.shape
        heads = a_log.shape[0]
        ns2 = proj_bc.shape[1]
        ns = ns2 // 2
        nc = rows // Q
        nrow = ns // n_seq
        wrows, drows = w_out.shape[1], d_out.shape[1]
        w_t = w_out.T
        d_t = d_out.T.reshape(2, drows // 2, rows)

        big = pltpu.VMEM((rows, ch), F32)
        chunk_states = pltpu.VMEM((nc, ns, ch), F32)
        slices = pltpu.VMEM((n_seq, nrow, ch), F32)
        sem_s = pltpu.SemaphoreType.DMA((2, n_seq))
        sem_t = pltpu.SemaphoreType.DMA((2, n_tp))
        scratch = [
            pltpu.VMEM((drows, rows), BF16),
            big,
            big,
            pltpu.VMEM((rows, ns2), F32),
            pltpu.VMEM((heads, rows), F32),
            pltpu.VMEM((wrows, ch), F32),
            pltpu.VMEM((rows, ch), BF16),
            pltpu.VMEM((rows, ch), BF16),
            pltpu.VMEM((rows, ns2), BF16),
            pltpu.VMEM((heads, rows), BF16),
            pltpu.VMEM((4, ch), F32),
            pltpu.VMEM((ch // LANES, LANES), F32),
            pltpu.VMEM((4, ns2), F32),
            pltpu.VMEM((1, ns2), F32),
            pltpu.VMEM((ch // LANES, LANES), F32),
            pltpu.VMEM((1, heads), F32),
            pltpu.VMEM((1, heads), F32),
            pltpu.VMEM((1, heads), F32),
            pltpu.VMEM((4, 4, wrows, ch), BF16),
            pltpu.VMEM((4, 4, wrows, rows), BF16),
            pltpu.VMEM((16, ch), BF16),
            pltpu.VMEM((16, ns2), BF16),
            pltpu.VMEM((8, LANES), F32),
            pltpu.VMEM((n_seq, 8, LANES), F32),
            big,
            big,
            pltpu.VMEM((nc, heads, Q), F32),
            big,
            big,
            pltpu.VMEM((rows, ns2), F32),
            pltpu.VMEM((rows, ns2), F32),
            chunk_states,
            chunk_states,
            chunk_states,
            big,
            big,
            big,
            big,
            pltpu.VMEM((rows, ch), BF16),
            pltpu.VMEM((rows + 8, ch), F32),
            pltpu.VMEM((rows + 8, ns2), F32),
            pltpu.VMEM((ns, ch), F32),
            slices,
            slices,
            slices,
            slices,
            slices,
            slices,
            slices,
            slices,
            pltpu.VMEM((2, 8, rows), F32),
            pltpu.VMEM((2, n_tp, 8, rows), F32),
            pltpu.VMEM((4, 2, drows, rows), BF16),
            pltpu.VMEM((4, drows, rows), BF16),
            pltpu.VMEM((drows, rows), BF16),
            pltpu.VMEM((2, drows, rows), BF16),
            pltpu.VMEM((4, 4, wrows, ch), BF16),
            *[
                pltpu.VMEM(shape, BF16)
                for shape in 2
                * [
                    (4, wrows // 2, ch),
                    (2, 4, wrows // 2, ch),
                    (wrows // 2, ch),
                    (2, wrows // 2, ch),
                ]
            ],
            pltpu.VMEM((nc, 4, 2, Q // n_tp, ns2), F32),
            pltpu.VMEM((nc, 4, Q // n_tp, ns2), F32),
            pltpu.VMEM((nc, 4, Q // n_tp, ns2), F32),
            chunk_states,
            pltpu.VMEM((n_tp, nc, Q // n_tp, ns2), BF16),
            pltpu.VMEM((Q, LANES), F32),
            pltpu.VMEM((LANES, Q), F32),
            pltpu.VMEM((Q, Q), F32),
            pltpu.VMEM((rows, 1), F32),
            pltpu.VMEM((nc, Q, LANES), F32),
            pltpu.VMEM((rows, ns2), F32),
            pltpu.VMEM((8, ns2), F32),
            pltpu.VMEM((nc, 8, ch), F32),
            pltpu.VMEM((rows, LANES), BF16),
            pltpu.SemaphoreType.DMA((2, nc)),
            pltpu.SemaphoreType.DMA((n_tp,)),
            pltpu.SemaphoreType.DMA((20,)),
            pltpu.SemaphoreType.DMA((2, 4)),
            sem_s,
            pltpu.SemaphoreType.DMA((2, 28)),
            sem_t,
            sem_s,
            sem_s,
            sem_s,
            sem_s,
            pltpu.SemaphoreType.DMA((2, 2 * n_tp)),
            sem_t,
            pltpu.SemaphoreType.DMA((2, 24)),
            pltpu.SemaphoreType.DMA((2, nc * n_tp)),
            pltpu.SemaphoreType.DMA((2, nc * n_tp)),
        ]
        out_t, g_x, g_z, g_bc, g_dt, g_w = pl.pallas_call(
            functools.partial(kernel, (n_seq, n_tp, ch * n_tp)),
            out_shape=[
                jax.ShapeDtypeStruct((drows, rows), BF16),
                jax.ShapeDtypeStruct((rows, ch), F32),
                jax.ShapeDtypeStruct((rows, ch), F32),
                jax.ShapeDtypeStruct((rows, ns2), F32),
                jax.ShapeDtypeStruct((heads, rows), F32),
                jax.ShapeDtypeStruct((wrows, ch), F32),
            ],
            in_specs=[pl.BlockSpec(memory_space=pltpu.HBM)] * 14,
            out_specs=[pl.BlockSpec(memory_space=pltpu.HBM)] * 6,
            scratch_shapes=scratch,
            compiler_params=pltpu.CompilerParams(
                collective_id=0, has_side_effects=True, vmem_limit_bytes=62 * 1024 * 1024
            ),
            name="mixer",
        )(
            inner_x,
            gate_z,
            proj_bc,
            dt_raw.T,
            w_t,
            d_t,
            conv_x,
            bias_x.reshape(-1, LANES),
            conv_bc,
            bias_bc[None, :],
            norm_gain.reshape(-1, LANES),
            a_log[None, :],
            dt_bias[None, :],
            d_skip[None, :],
        )
        results = (g_x, g_z, g_bc, g_w, out_t, g_dt)
        hbm = pl.BlockSpec(memory_space=pltpu.HBM)
        g_x, g_z, g_bc, g_w, out_t, g_dt = pl.pallas_call(
            publish,
            out_shape=[jax.ShapeDtypeStruct(v.shape, v.dtype) for v in results],
            in_specs=[hbm] * 6,
            out_specs=[hbm] * 6,
            scratch_shapes=[pltpu.VMEM(v.shape, v.dtype) for v in results]
            + [pltpu.SemaphoreType.DMA((16,)), pltpu.SemaphoreType.DMA((16,))],
            compiler_params=pltpu.CompilerParams(vmem_limit_bytes=62 * 1024 * 1024),
            name="publish",
        )(*results)
        return out_t.T, g_x, g_z, g_bc, g_dt.T, g_w.T

    in_specs = (
        P("seq", "tp"),
        P("seq", "tp"),
        P("seq", None),
        P("seq", "tp"),
        P("tp"),
        P("tp"),
        P("tp"),
        P(None, "tp"),
        P("tp"),
        P(),
        P(),
        P("tp"),
        P("tp", "seq"),
        P("seq", "tp"),
    )
    out_specs = (
        P("seq", "tp"),
        P("seq", "tp"),
        P("seq", "tp"),
        P("seq", None),
        P("seq", "tp"),
        P("tp", "seq"),
    )
    return jax.shard_map(
        shards, mesh=mesh, in_specs=in_specs, out_specs=out_specs, check_vma=False
    )
```

```python
import functools

import jax
import jax.numpy as jnp
from jax import lax
from jax.experimental import pallas as pl
from jax.experimental.pallas import tpu as pltpu
from jax.sharding import PartitionSpec as P

MESH = pl.DeviceIdType.MESH
F32 = jnp.float32
BF16 = jnp.bfloat16
HIGH = lax.Precision.HIGHEST
EPSILON = 1e-05
NN = ((1,), (0,))
NT = ((1,), (1,))
Q = 128
PAIR = 128
HEAD = 64
LANES = 128


def mm(a, b, dims=NN):
    return lax.dot_general(a.astype(BF16), b.astype(BF16), (dims, ((), ())), preferred_element_type=F32)


def mmh(a, b, dims=NN):
    return lax.dot_general(
        a.astype(F32), b.astype(F32), (dims, ((), ())), precision=HIGH, preferred_element_type=F32
    )


def halves(v):
    high = v.astype(BF16)
    return high, (v - high.astype(F32)).astype(BF16)


def mm3(a, b, dims=NN):
    a0, a1 = halves(a)
    b0, b1 = halves(b)
    return mm(a0, b0, dims) + (mm(a1, b0, dims) + mm(a0, b1, dims))


def parts(v, count):
    out = []
    for _ in range(count):
        piece = v.astype(BF16)
        out.append(piece)
        v = v - piece.astype(F32)
    return out


def iota(shape, dim):
    return lax.broadcasted_iota(jnp.int32, shape, dim)


def sigmoid(v):
    return 1.0 / (1.0 + jnp.exp(-v))


def softplus(v):
    return jnp.maximum(v, 0.0) + jnp.log1p(jnp.exp(-jnp.abs(v)))


def pair_stack(v):
    lane = iota(v.shape, 1)
    return jnp.concatenate(
        [jnp.where(lane < HEAD, v, 0.0), jnp.where(lane >= HEAD, v, 0.0)], axis=0
    )


def kernel(
    sizes,
    ix_in,
    gz_in,
    bc_in,
    raw_in,
    wt,
    dt,
    cw_in,
    bx_in,
    cwb_in,
    bb_in,
    gain_in,
    al_in,
    db_in,
    ds_in,
    out_hbm,
    gx_hbm,
    gz_hbm,
    gbc_hbm,
    gdt_hbm,
    gw_hbm,
    o_out,
    o_gx,
    o_gz,
    o_gbc,
    o_gdt,
    o_gw,
    ix,
    gz,
    bc,
    raw,
    cw,
    bx,
    cwb,
    bb,
    gain,
    al,
    db,
    ds,
    wfull,
    dfull,
    hx,
    hb,
    dsend,
    dbuf,
    st,
    lx,
    lt,
    u,
    x,
    ub,
    bcv,
    fr,
    sst,
    cf,
    y,
    gated,
    gn,
    gm,
    nb,
    dus,
    dub,
    rcur,
    se,
    sr,
    en,
    sin,
    re,
    rr,
    ren,
    rin,
    ts,
    tr,
    pb,
    pp,
    po1,
    po2,
    gb,
    ga1,
    ga2,
    ga3,
    ga4,
    gb1,
    gb2,
    gb3,
    gb4,
    qs,
    qm,
    qr,
    rst,
    qa,
    arow,
    acol,
    dga,
    invs,
    swings,
    dmap,
    edge,
    frow,
    packed,
    sm_m,
    sm_e,
    sm_l,
    sm_h,
    sm_d,
    sm_w,
    sm_g,
    sm_s,
    sm_b,
    sm_r,
    sm_q,
    sm_t,
    sm_o,
    sm_v,
    sm_p,
    sm_a,
):
    n_seq, n_tp, inner = sizes
    rows, ch = ix.shape
    nc = rows // Q
    heads = raw.shape[0]
    pairs = ch // PAIR
    ns = bc.shape[1] // 2
    me, my = lax.axis_index("seq"), lax.axis_index("tp")
    wrows = wt.shape[0]
    drows = 2 * dt.shape[1]
    nrow = ns // n_seq

    scope = []

    def phase(name):
        if scope:
            scope.pop().__exit__(None, None, None)
        if name:
            scope.append(jax.named_scope(name))
            scope[0].__enter__()

    side = 4
    zi, xi = lax.div(me, side), lax.rem(me, side)
    yi, core = lax.div(my, 2), lax.rem(my, 2)

    def step(v, k):
        return lax.rem(v + k + side, side)

    x_up, x_dn = step(xi, 1), step(xi, -1)
    z_up, z_dn = step(zi, 1), step(zi, -1)
    y_up, y_dn = step(yi, 1), step(yi, -1)
    x_far, z_far, y_far = step(xi, 2), step(zi, 2), step(yi, 2)
    to_xu, to_xd = zi * side + x_up, zi * side + x_dn
    to_zu, to_zd = z_up * side + xi, z_dn * side + xi
    to_xf, to_zf = zi * side + x_far, z_far * side + xi
    to_yu, to_yd = y_up * 2 + core, y_dn * 2 + core
    mate = yi * 2 + 1 - core

    def hops(pair):
        return sum(min(v, side - v) for v in pair)

    others = [(a, b) for a in range(side) for b in range(side) if a or b]
    others.sort(key=lambda pair: -hops(pair))

    def seq_peer(k):
        a, b = others[k - 1]
        return step(zi, a) * side + step(xi, b)

    def tp_peer(k):
        return lax.rem(my + k, n_tp)

    phase("barrier1")
    barrier = pltpu.get_barrier_semaphore()
    for k in range(1, n_seq):
        pl.semaphore_signal(barrier, inc=1, device_id={"seq": seq_peer(k)}, device_id_type=MESH)
    for k in range(1, n_tp):
        pl.semaphore_signal(barrier, inc=1, device_id={"tp": tp_peer(k)}, device_id_type=MESH)

    def remote(src, dst, sems, k, axis, peer):
        return pltpu.make_async_remote_copy(
            src_ref=src,
            dst_ref=dst,
            send_sem=sems.at[0, k],
            recv_sem=sems.at[1, k],
            device_id={axis: peer},
            device_id_type=MESH,
        )

    nxt, prv = lax.rem(me + 1, n_seq), lax.rem(me + n_seq - 1, n_seq)

    @pl.when(my > 0)
    def _():
        pl.semaphore_signal(barrier, inc=1, device_id={"seq": nxt, "tp": 0}, device_id_type=MESH)

    staged = [
        (raw_in, raw),
        (al_in, al),
        (db_in, db),
        (ds_in, ds),
        (wt, wfull.at[zi, xi]),
        (dt, dfull.at[yi, pl.ds(2 * core, 2)]),
        (ix_in, ix),
        (bc_in, bc),
        (cw_in, cw),
        (bx_in, bx),
        (cwb_in, cwb),
        (bb_in, bb),
        (gain_in, gain),
        (gz_in, gz),
    ]
    loads = [pltpu.make_async_copy(a, b, sm_l.at[i]) for i, (a, b) in enumerate(staged)]
    for load in loads:
        load.start()
    results = [(o_gz, gz_hbm), (o_out, out_hbm), (o_gx, gx_hbm), (o_gw, gw_hbm), (o_gbc, gbc_hbm), (o_gdt, gdt_hbm)]
    stores = [pltpu.make_async_copy(a, b, sm_l.at[14 + i]) for i, (a, b) in enumerate(results)]
    phase("staging")
    for load in loads[:9]:
        load.wait()
    phase("barrier")
    pl.semaphore_wait(barrier, n_seq + n_tp - 2 + jnp.where(my == 0, n_tp - 1, 0))

    phase("start")
    halo_x = remote(ix.at[pl.ds(rows - 16, 16)], hx, sm_h, 0, "seq", nxt)
    halo_b = remote(bc.at[pl.ds(rows - 16, 16)], hb, sm_h, 1, "seq", nxt)
    halo_x.start()
    halo_b.start()

    half = wrows // 2
    near = 48
    ra, rb = pl.ds(0, half), pl.ds(half, half)
    ra1, ra2 = pl.ds(0, near), pl.ds(near, half - near)
    rb1, rb2 = pl.ds(half, near), pl.ds(half + near, half - near)
    lo, hi, every = pl.ds(0, 2), pl.ds(2, 2), pl.ds(0, side)

    def w_view(z, x, r):
        return wfull.at[z, x, r]

    def w_move(i, peer, z, x, r, src=None):
        return remote(w_view(z, x, r) if src is None else src, w_view(z, x, r), sm_w, i, "seq", peer)

    w_copies = [
        w_move(0, to_xu, zi, xi, ra),
        w_move(1, to_xd, zi, xi, ra),
        w_move(2, to_zu, zi, xi, rb),
        w_move(3, to_zd, zi, xi, rb),
        w_move(4, to_zu, zi, xi, ra),
        w_move(5, to_zd, zi, xi, ra),
        w_move(6, to_xu, zi, xi, rb),
        w_move(7, to_xd, zi, xi, rb),
        w_move(8, to_xu, zi, x_dn, ra1),
        w_move(9, to_xd, zi, x_up, ra2),
        w_move(10, to_zu, z_dn, xi, rb1),
        w_move(11, to_zd, z_up, xi, rb2),
        w_move(12, to_zu, zi, x_up, ra),
        w_move(13, to_zd, zi, x_up, ra),
        w_move(14, to_xu, z_up, xi, rb),
        w_move(15, to_xd, z_up, xi, rb),
        w_move(16, to_zu, zi, x_dn, ra),
        w_move(17, to_zd, zi, x_dn, ra),
        w_move(18, to_xu, z_dn, xi, rb),
        w_move(19, to_xd, z_dn, xi, rb),
        w_move(20, to_zu, zi, x_far, ra),
        w_move(21, to_zd, zi, x_far, ra),
        w_move(22, to_xu, z_far, xi, rb),
        w_move(23, to_xd, z_far, xi, rb),
        w_move(24, to_zu, z_dn, xi, ra),
        w_move(25, to_xu, zi, x_dn, rb),
        w_move(26, to_zu, z_dn, x_up, ra),
        w_move(27, to_xu, z_up, x_dn, rb),
        w_move(28, to_zd, z_up, x_dn, ra),
        w_move(29, to_xd, z_dn, x_up, rb),
        w_move(30, to_zd, z_up, x_far, ra),
        w_move(31, to_xd, z_far, x_up, rb),
    ]

    dhalf = drows // 2

    def d_view(y, c, off=0, size=drows):
        if size == drows:
            return dfull.at[y, pl.ds(2 * c, 2)]
        return dfull.at[y, 2 * c + off // size]

    def d_move(i, peer, y, c, off=0, size=drows, src=None):
        view = d_view(y, c, off, size)
        return remote(view if src is None else src, view, sm_g, i, "tp", peer)

    d_copies = [
        d_move(0, to_yu, yi, core),
        d_move(1, to_yd, yi, core),
        d_move(2, mate, yi, core),
        d_move(3, to_yu, y_dn, core, 0, dhalf),
        d_move(4, to_yd, y_up, core, dhalf, dhalf),
        d_move(5, mate, y_dn, core),
        d_move(6, mate, y_up, core),
        d_move(7, mate, y_far, core),
    ]

    def start(copies, first, last):
        for copy in copies[first:last]:
            copy.start()

    def arrived(copies, first, last):
        for copy in copies[first:last]:
            copy.wait_recv()

    start(w_copies, 0, 8)
    start(d_copies, 0, 3)

    phase("steps")
    slot = lax.rem(iota((LANES, 2 * ch), 0), 32)
    wanted = iota((LANES, 2 * ch), 1) // HEAD
    wanted = jnp.where(wanted < heads, wanted, wanted - heads + 16)
    spread = ((slot == wanted) & (iota((LANES, 2 * ch), 0) < 96)).astype(BF16)
    spread_h = (iota((heads, ch), 1) // HEAD == iota((heads, ch), 0)).astype(F32)
    ident = (iota((heads, heads), 0) == iota((heads, heads), 1)).astype(F32)
    negexp = -jnp.exp(al[...])
    skip_x = mmh(jnp.broadcast_to(ds[...], (8, heads)), spread_h)[0:1]
    tri_u = (iota((Q, Q), 0) <= iota((Q, Q), 1)).astype(F32)

    def column(v):
        return mmh(ident, jnp.broadcast_to(v, (8, heads)), NT)[:, 0:1]

    def in_line(ref):
        return jnp.concatenate([ref[i : i + 1] for i in range(ref.shape[0])], axis=1)

    dt_col, neg_col = column(db[...]), column(negexp)

    for load in loads[9:]:
        load.wait()
    bias_line, gain_line = in_line(bx), in_line(gain)

    def steps(c, total):
        sl = pl.ds(pl.multiple_of(c * Q, Q), Q)
        s_c = softplus(raw[:, sl].astype(F32) + dt_col)
        cum = mmh(s_c * neg_col, tri_u)
        lt[c] = cum
        gap = jnp.zeros((16 - heads, Q), F32)
        pieces = []
        for a, b in zip(parts(s_c, 3), parts(cum, 3)):
            pieces += [a.astype(F32), gap, b.astype(F32), gap]
        turned = jnp.transpose(jnp.concatenate([*pieces, jnp.zeros((LANES - 96, Q), F32)], axis=0))
        packed[sl, :] = turned.astype(BF16)
        return total + turned[Q - 1 : Q, :]

    total = lax.fori_loop(0, nc, steps, jnp.zeros((1, LANES), F32))
    st[...] = mm(packed[...], spread[:, :ch])
    lx[...] = mm(packed[...], spread[:, ch:])
    dsend[...] = jnp.broadcast_to(total, (8, LANES))
    dbuf[me] = dsend[...]

    def t_copy(k):
        return remote(dsend, dbuf.at[me], sm_d, k, "seq", seq_peer(k))

    for k in range(1, n_seq):
        t_copy(k).start()

    phase("convs")
    def conv_of(ref, halo, weights, bias, c):
        base = pl.multiple_of(c * Q, Q)
        own = ref[pl.ds(base, Q), :].astype(F32)
        if halo is None:
            head = ref[pl.ds(pl.multiple_of(c * Q - 16, 16), 16), :].astype(F32)[8:16]
        else:
            head = jnp.where(me > 0, halo[...].astype(F32), 0.0)[8:16]
        ext = jnp.concatenate([head, own], axis=0)
        acc = bias + weights[3:4, :] * own
        for k in range(3):
            acc = acc + weights[k : k + 1, :] * pltpu.roll(ext, Q + 8 - (5 + k), 0)[:Q]
        return acc

    def convs(c, carry, edge_of=(None, None)):
        sl = pl.ds(pl.multiple_of(c * Q, Q), Q)
        vb = conv_of(bc, edge_of[0], cwb, bb[...], c)
        ub[sl, :] = vb
        pbc = vb * sigmoid(vb)
        bcv[sl, :] = pbc
        vx = conv_of(ix, edge_of[1], cw, bias_line, c)
        u[sl, :] = vx
        xv = vx * sigmoid(vx)
        x[sl, :] = xv
        cum = lx[sl, :]
        to_end = jnp.exp(cum[Q - 1 : Q, :] - cum)
        b_t = jnp.transpose(pbc[:, :ns])
        fresh = mm3(b_t, xv * st[sl, :] * to_end)
        fr[c] = fresh
        return carry

    lax.fori_loop(1, nc, convs, 0)
    phase("wait_halo")
    halo_x.wait_recv()
    halo_b.wait_recv()
    phase("conv0")
    convs(0, 0, (hb, hx))
    end = fr[0]
    for c in range(1, nc):
        end = jnp.exp(lx[pl.ds(c * Q + Q - 1, 1), :]) * end + fr[c]
    se[...] = end.reshape(n_seq, nrow, ch)

    phase("send_s")
    def s_copy(k):
        return remote(se.at[seq_peer(k)], sr.at[me], sm_s, k, "seq", seq_peer(k))

    def sb_copy(k):
        return remote(en.at[seq_peer(k)], sin.at[me], sm_b, k, "seq", seq_peer(k))

    for k in range(1, n_seq):
        s_copy(k).start()
    sr[me] = se[me]
    phase("wait_w1")
    arrived(w_copies, 0, 4)
    start(w_copies, 8, 16)

    upper = iota((Q, Q), 0) >= iota((Q, Q), 1)
    lower = iota((Q, Q), 0) <= iota((Q, Q), 1)

    phase("inside")
    def inside(c, carry):
        sl = pl.ds(pl.multiple_of(c * Q, Q), Q)
        scores = mm3(bcv[sl, ns:], bcv[sl, :ns], NT)
        for p in range(pairs):
            ps = slice(p * PAIR, (p + 1) * PAIR)
            both = []
            for h in (2 * p, 2 * p + 1):
                diff = lx[sl, h * HEAD : h * HEAD + 1] - lt[c, h : h + 1, :]
                decay = jnp.exp(jnp.where(upper, diff, -1e30))
                both.append(decay * scores)
            y[sl, ps] = mm3(jnp.concatenate(both, axis=1), pair_stack(x[sl, ps] * st[sl, ps]))
        return carry

    lax.fori_loop(0, nc, inside, 0)
    phase("wait_d1")
    arrived(d_copies, 0, 2)
    start(d_copies, 3, 7)
    phase("wait_s")
    for k in range(1, n_seq):
        t_copy(k).wait_recv()
    for k in range(1, n_seq):
        s_copy(k).wait_recv()
    phase("scan")
    fade = jnp.exp(sum(mm(piece, spread[:, ch:]) for piece in parts(dbuf[:, 0, :], 3)))

    acc = jnp.zeros((nrow, ch), F32)
    for j in range(n_seq):
        en[j] = acc
        acc = fade[j : j + 1] * acc + sr[j]
    for k in range(1, n_seq):
        sb_copy(k).start()
    sin[me] = en[me]
    start(w_copies, 16, 20)
    phase("wait_w2")
    arrived(w_copies, 8, 12)
    start(w_copies, 20, 24)

    phase("wait_sb")
    for k in range(1, n_seq):
        sb_copy(k).wait_recv()
    arrived(d_copies, 3, 5)
    start(d_copies, 7, 8)
    phase("combine")
    lane = iota((Q, LANES), 1)

    def to_row(i, c, v):
        ts[i, :, pl.ds(pl.multiple_of(c * Q, Q), Q)] = jnp.transpose(jnp.where(lane == 0, v, 0.0))[:8]

    def to_column(row, c):
        block = jnp.concatenate([row[:, c * Q : (c + 1) * Q], jnp.zeros((Q - 8, Q), F32)], axis=0)
        return jnp.transpose(block)[:, 0:1]

    def combine(c, state):
        sl = pl.ds(pl.multiple_of(c * Q, Q), Q)
        sst[c] = state
        cum = lx[sl, :]
        mixed = y[sl, :] + jnp.exp(cum) * mm3(bcv[sl, ns:], state) + skip_x * x[sl, :]
        y[sl, :] = mixed
        zv = gz[sl, :].astype(F32)
        gv = mixed * zv * sigmoid(zv)
        gated[sl, :] = gv
        to_row(0, c, jnp.sum(gv * gv, axis=1, keepdims=True))
        return jnp.exp(cum[Q - 1 : Q, :]) * state + fr[c]

    lax.fori_loop(0, nc, combine, sin[...].reshape(ns, ch))

    def r_copies(i):
        return [
            remote(ts.at[i], tr.at[i, my], sm_t, i * n_tp + k, "tp", tp_peer(k)) for k in range(1, n_tp)
        ]

    def r_total(i):
        total = tr[i, 0]
        for j in range(1, n_tp):
            total = total + tr[i, j]
        return total

    r_squares, r_inner = r_copies(0), r_copies(1)
    start(r_squares, 0, n_tp - 1)
    tr[0, my] = ts[0]

    phase("wait_w_near")
    arrived(w_copies, 4, 8)
    arrived(w_copies, 12, 20)
    start(w_copies, 24, 30)
    phase("gn_own")
    kb = wrows * side

    moves = (0, 1, -1, 2)

    def gn_early(k):
        zz, xx = step(zi, moves[k]), step(xi, moves[k])
        d_rows = jnp.concatenate(
            [dfull[zz, :, ra].reshape(kb // 2, rows), dfull[:, xx, rb].reshape(kb // 2, rows)], axis=0
        )
        w_rows = jnp.concatenate(
            [wfull[zz, :, ra].reshape(kb // 2, ch), wfull[:, xx, rb].reshape(kb // 2, ch)], axis=0
        )
        part = mm(jnp.transpose(d_rows), w_rows)
        gn[...] = part if k == 0 else gn[...] + part

    arrived(d_copies, 2, 3)
    arrived(d_copies, 5, 7)
    arrived(d_copies, 7, 8)
    gn_early(0)
    phase("wait_w3")
    arrived(w_copies, 20, 24)
    start(w_copies, 30, 32)
    phase("gn")
    gn_early(1)
    gn_early(2)

    phase("wait_ss")
    arrived(r_squares, 0, n_tp - 1)
    inv_row = lax.rsqrt(r_total(0) / inner + EPSILON)
    phase("nb")
    for c in range(nc):
        sl = pl.ds(c * Q, Q)
        inv = to_column(inv_row, c)
        invs[sl, :] = inv
        nb[sl, :] = (gated[sl, :] * inv * gain_line).astype(BF16)
    phase("gradw")
    g_copies = [
        remote(gb.at[z_far, lo, ra], ga1.at[lo], sm_v, 0, "seq", to_zu),
        remote(gb.at[z_far, hi, ra], ga1.at[hi], sm_v, 1, "seq", to_zd),
        remote(gb.at[lo, x_far, rb], gb1.at[lo], sm_v, 2, "seq", to_xu),
        remote(gb.at[hi, x_far, rb], gb1.at[hi], sm_v, 3, "seq", to_xd),
        remote(gb.at[z_up, hi, ra], ga2.at[0, hi], sm_v, 4, "seq", to_zu),
        remote(gb.at[z_dn, lo, ra], ga2.at[1, lo], sm_v, 5, "seq", to_zd),
        remote(gb.at[hi, x_up, rb], gb2.at[0, hi], sm_v, 6, "seq", to_xu),
        remote(gb.at[lo, x_dn, rb], gb2.at[1, lo], sm_v, 7, "seq", to_xd),
        remote(gb.at[z_up, 0, ra], ga2.at[0, 0], sm_v, 8, "seq", to_zu),
        remote(gb.at[z_dn, 2, ra], ga2.at[1, 2], sm_v, 9, "seq", to_zd),
        remote(gb.at[0, x_up, rb], gb2.at[0, 0], sm_v, 10, "seq", to_xu),
        remote(gb.at[2, x_dn, rb], gb2.at[1, 2], sm_v, 11, "seq", to_xd),
        remote(gb.at[z_up, 1, ra], ga2.at[0, 1], sm_v, 20, "seq", to_zu),
        remote(gb.at[z_dn, 3, ra], ga2.at[1, 3], sm_v, 21, "seq", to_zd),
        remote(gb.at[1, x_up, rb], gb2.at[0, 1], sm_v, 22, "seq", to_xu),
        remote(gb.at[3, x_dn, rb], gb2.at[1, 3], sm_v, 23, "seq", to_xd),
        remote(gb.at[zi, x_far, ra], ga3, sm_v, 12, "seq", to_xf),
        remote(gb.at[z_far, xi, rb], gb3, sm_v, 13, "seq", to_zf),
        remote(gb.at[zi, x_up, ra], ga4.at[0], sm_v, 14, "seq", to_xu),
        remote(gb.at[zi, x_dn, ra], ga4.at[1], sm_v, 15, "seq", to_xd),
        remote(gb.at[z_up, xi, rb], gb4.at[0], sm_v, 16, "seq", to_zu),
        remote(gb.at[z_dn, xi, rb], gb4.at[1], sm_v, 17, "seq", to_zd),
    ]

    def plus(ref, index, *others):
        total = ref[index].astype(F32)
        for part in others:
            total = total + part.astype(F32)
        ref[index] = total.astype(BF16)

    def g_block(k, carry):
        b = step(zi, 2 + k)
        gb[b] = mm(dfull[b].reshape(kb, rows), nb[...]).astype(BF16).reshape(side, wrows, ch)

        @pl.when(k == 0)
        def _():
            start(g_copies, 0, 2)

        return carry

    lax.fori_loop(0, side, g_block, 0)
    start(g_copies, 2, 8)

    def g_second():
        arrived(g_copies, 0, 4)
        for j in range(2):
            plus(gb, (z_up, j, ra), ga1[j])
            plus(gb, (z_dn, 2 + j, ra), ga1[2 + j])
            plus(gb, (j, x_up, rb), gb1[j])
            plus(gb, (2 + j, x_dn, rb), gb1[2 + j])
        start(g_copies, 8, 12)

    def g_third():
        arrived(g_copies, 4, 16)
        for j in range(side):
            plus(gb, (zi, j, ra), ga2[0, j], ga2[1, j])
            plus(gb, (j, xi, rb), gb2[0, j], gb2[1, j])
        start(g_copies, 16, 22)

    def g_last():
        arrived(g_copies, 16, 22)

        def landed(own, far, near):
            return own.astype(F32) + far.astype(F32) + near[0].astype(F32) + near[1].astype(F32)

        o_gw[ra, :] = landed(gb[zi, xi, ra], ga3[...], ga4)
        o_gw[rb, :] = landed(gb[zi, xi, rb], gb3[...], gb4)

    def o_second():
        arrived(o_copies, 0, 1)
        for j in range(side):
            plus(pb, (j, core), pp[j])
        start(o_copies, 1, 3)

    def o_third():
        arrived(o_copies, 1, 3)
        plus(pb, (y_up, core, o_half1), po1[o_half1])
        plus(pb, (y_dn, core, o_half2), po1[o_half2])
        start(o_copies, 3, 5)

    def o_last():
        arrived(o_copies, 3, 5)
        total = pb[yi, core].astype(F32) + po2[0].astype(F32) + po2[1].astype(F32)
        o_out[...] = total.astype(BF16)
    phase("wait_w4")
    arrived(w_copies, 24, 32)
    phase("gn_last")
    gn_early(3)
    phase("ip")

    def inner_sums(c, carry):
        sl = pl.ds(pl.multiple_of(c * Q, Q), Q)
        scaled = gn[sl, :] * gain_line
        gn[sl, :] = scaled
        to_row(1, c, jnp.sum(scaled * gated[sl, :], axis=1, keepdims=True))
        return carry

    lax.fori_loop(0, nc, inner_sums, 0)
    start(r_inner, 0, n_tp - 1)
    tr[1, my] = ts[1]
    phase("outmm")
    def share(y0, c0):
        block = wfull[y0, pl.ds(2 * c0, 2)].reshape(drows, ch)
        pb[y0, c0] = mm(block, nb[...], NT).astype(BF16)

    def other(j, carry):
        share(j, 1 - core)
        return carry

    def same(j, carry):
        share(j, core)
        return carry

    o_half1, o_half2 = pl.ds(0, dhalf), pl.ds(dhalf, dhalf)
    o_copies = [
        remote(pb.at[every, 1 - core], pp, sm_o, 0, "tp", mate),
        remote(pb.at[y_far, core, o_half1], po1.at[o_half1], sm_o, 1, "tp", to_yu),
        remote(pb.at[y_far, core, o_half2], po1.at[o_half2], sm_o, 2, "tp", to_yd),
        remote(pb.at[y_up, core], po2.at[0], sm_o, 3, "tp", to_yu),
        remote(pb.at[y_dn, core], po2.at[1], sm_o, 4, "tp", to_yd),
    ]
    lax.fori_loop(0, side, other, 0)
    start(o_copies, 0, 1)
    lax.fori_loop(0, side, same, 0)
    phase("wait_ip")
    arrived(r_inner, 0, n_tp - 1)
    ip_row = r_total(1) / inner * inv_row * inv_row * inv_row
    phase("norm")
    for c in range(nc):
        sl = pl.ds(c * Q, Q)
        gg = invs[sl, :] * gn[sl, :] - gated[sl, :] * to_column(ip_row, c)
        zv = gz[sl, :].astype(F32)
        sg = sigmoid(zv)
        o_gz[sl, :] = gg * y[sl, :] * sg * (1.0 + zv * (1.0 - sg))
        gmv = gg * zv * sg
        gm[sl, :] = gmv
        c_t = jnp.transpose(bcv[sl, ns:])
        cf[c] = mm3(c_t, gmv * jnp.exp(lx[sl, :]))

    racc = cf[nc - 1]
    for c in reversed(range(nc - 1)):
        racc = cf[c] + jnp.exp(lx[pl.ds(c * Q + Q - 1, 1), :]) * racc
    re[...] = racc.reshape(n_seq, nrow, ch)

    phase("send_v")
    def v_copy(k):
        return remote(re.at[seq_peer(k)], rr.at[me], sm_r, k, "seq", seq_peer(k))

    def vb_copy(k):
        return remote(ren.at[seq_peer(k)], rin.at[me], sm_q, k, "seq", seq_peer(k))

    for k in range(1, n_seq):
        v_copy(k).start()
    rr[me] = re[me]
    stores[0].start()
    phase("g_second")
    g_second()
    phase("o_second")
    o_second()
    phase("intra")
    def back_inside(c, carry):
        sl = pl.ds(pl.multiple_of(c * Q, Q), Q)
        bmap, cmap = bcv[sl, :ns], bcv[sl, ns:]
        scores = mm3(cmap, bmap, NT)
        scores_t = mm3(bmap, cmap, NT)
        arow[...] = jnp.zeros((Q, LANES), F32)
        acol[...] = jnp.zeros((LANES, Q), F32)
        dga[...] = jnp.zeros((Q, Q), F32)
        for p in range(pairs):
            ps = slice(p * PAIR, (p + 1) * PAIR)
            g2 = gm[sl, ps]
            cross = mm3(g2, pair_stack(x[sl, ps] * st[sl, ps]), NT)
            both = []
            for i_h, h in enumerate((2 * p, 2 * p + 1)):
                diff = lx[sl, h * HEAD : h * HEAD + 1] - lt[c, h : h + 1, :]
                weighted = jnp.exp(jnp.where(upper, diff, -1e30)) * cross[:, i_h * Q : (i_h + 1) * Q]
                dga[...] += weighted
                term = weighted * scores
                arow[...] += jnp.where(lane == h, jnp.sum(term, axis=1, keepdims=True), 0.0)
                acol[h : h + 1, :] = jnp.sum(term, axis=0, keepdims=True)
                decay_t = jnp.exp(jnp.where(lower, lt[c, h : h + 1, :] - lx[sl, h * HEAD : h * HEAD + 1], -1e30))
                both.append((decay_t * scores_t).astype(BF16))
            y[sl, ps] = mm(jnp.concatenate(both, axis=1), pair_stack(g2))
        dgv = dga[...]
        swings[c] = arow[...] - jnp.transpose(acol[...])
        dmap[sl, :ns] = mm3(jnp.transpose(dgv), cmap)
        dmap[sl, ns:] = mm3(dgv, bmap)
        return carry

    def back_insides(first):
        def one(i, carry):
            return back_inside(first - i, carry)

        lax.fori_loop(0, nc // 2, one, 0)

    back_insides(nc - 1)
    back_insides(nc // 2 - 1)

    phase("wait_v")
    for k in range(1, n_seq):
        v_copy(k).wait_recv()
    acc = jnp.zeros((nrow, ch), F32)
    for j in reversed(range(n_seq)):
        ren[j] = acc
        acc = fade[j : j + 1] * acc + rr[j]
    for k in range(1, n_seq):
        vb_copy(k).start()
    rin[me] = ren[me]
    start(g_copies, 12, 16)
    phase("o_third")
    o_third()
    phase("forward_part")
    to_head = (lax.rem(iota((2 * ch, LANES), 0), ch) // HEAD == iota((2 * ch, LANES), 1)).astype(BF16)
    neg_c = jnp.concatenate([negexp, jnp.zeros((1, LANES - heads), F32)], axis=1)
    blk = Q // n_tp
    tail_sum = jnp.concatenate([tri_u.astype(BF16)] * 3, axis=1)
    head_sum = jnp.concatenate([(iota((Q, Q), 0) > iota((Q, Q), 1)).astype(BF16)] * 3, axis=1)

    def by_head(v):
        return mm(jnp.concatenate(parts(v, 2), axis=1), to_head)

    def reads(i, later):
        c = nc - 1 - i
        sl = pl.ds(pl.multiple_of(c * Q, Q), Q)
        cmap = bcv[sl, ns:]
        sv = sst[c]
        cum = lx[sl, :]
        last = cum[Q - 1 : Q, :]
        gg = gm[sl, :] * jnp.exp(cum)
        dmap[sl, ns:] += mm3(gg, sv, NT)
        swings[c] += by_head(gg * mm(cmap, sv))
        rv = rcur[...]
        rst[c] = rv
        reach = x[sl, :] * st[sl, :] * jnp.exp(last - cum)
        dmap[sl, :ns] += mm3(reach, rv, NT)
        gn[sl, :] = reach * later
        frow[c] = jnp.broadcast_to(later, (8, ch))
        rcur[...] = cf[c] + jnp.exp(last) * rv
        return later * jnp.exp(last)

    rcur[...] = jnp.zeros((ns, ch), F32)
    lax.fori_loop(0, nc, reads, jnp.ones((1, ch), F32))
    phase("wait_vb")
    for k in range(1, n_seq):
        vb_copy(k).wait_recv()
    phase("inter")
    rcur[...] = rin[...].reshape(ns, ch)
    def m_copy(c):
        return remote(qs.at[c, every, 1 - core], qm.at[c], sm_m, c, "tp", mate)

    def q_copy(c, k):
        y1 = step(yi, k)
        return remote(qs.at[c, y1, core], qr.at[c, yi], sm_p, c * side + k, "tp", y1 * 2 + core)

    def q_send(c):
        m_copy(c).wait_recv()
        for j in range(side):
            qs[c, j, core] += qm[c, j]
        for k in range(1, side):
            q_copy(c, k).start()
        qr[c, yi] = qs[c, yi, core]

    def a_copy(c, k):
        return remote(qa.at[my, c], qa.at[my, c], sm_a, c * n_tp + k, "tp", tp_peer(k))

    def a_send(c):
        for k in range(1, side):
            q_copy(c, k).wait_recv()
        total = qr[c, 0] + qr[c, 1] + qr[c, 2] + qr[c, 3]
        qa[my, c] = total.astype(BF16)
        for k in range(1, n_tp):
            a_copy(c, k).start()
        return total

    def back_b(c, carry):
        sl = pl.ds(pl.multiple_of(c * Q, Q), Q)
        qs[c, :, :, :, :ns] = dmap[sl, :ns].reshape(side, 2, blk, ns)
        qs[c, :, :, :, ns:] = dmap[sl, ns:].reshape(side, 2, blk, ns)
        m_copy(c).start()
        return carry

    dmap[:, :ns] += mm3(gn[...], rcur[...], NT)
    lax.fori_loop(0, nc, back_b, 0)
    phase("inter2")

    def back(i, carry):
        c = i
        sl = pl.ds(pl.multiple_of(c * Q, Q), Q)
        cum = lx[sl, :]
        last = cum[Q - 1 : Q, :]
        rv = rst[c] + frow[c][0:1] * rcur[...]
        xv = x[sl, :]
        sx = st[sl, :]
        d_in = mm(bcv[sl, :ns], rv) * jnp.exp(last - cum)
        dxt = y[sl, :] + d_in
        uv = u[sl, :]
        su = sigmoid(uv)
        dus[sl, :] = (sx * dxt + skip_x * gm[sl, :]) * (su * (1.0 + uv * (1.0 - su)))
        per_head = by_head(jnp.concatenate([xv * sx * d_in, xv * dxt], axis=0))
        fixed = by_head(
            jnp.broadcast_to(jnp.sum(rv * sst[c], axis=0, keepdims=True) * jnp.exp(last), (8, ch))
        )[0:1]
        dld = (
            mm(tail_sum, jnp.concatenate(parts(swings[c], 3), axis=0))
            + mm(head_sum, jnp.concatenate(parts(per_head[:Q], 3), axis=0))
            + fixed
        )
        dstep = per_head[Q:] + dld * neg_c
        slope = sigmoid(raw[:, sl].astype(F32) + dt_col)
        o_gdt[:, sl] = jnp.transpose(dstep)[:heads] * slope

        @pl.when(i == 0)
        def _():
            for j in range(nc):
                q_send(j)
            edge_x.start()

        @pl.when(i == 1)
        def _():
            g_third()

        return carry

    edge_x = remote(dus.at[pl.ds(0, 8)], dus.at[pl.ds(rows, 8)], sm_h, 2, "seq", prv)
    lax.fori_loop(0, nc, back, 0)
    stores[5].start()
    phase("wait_q")

    def edge_b(j):
        return pltpu.make_async_remote_copy(
            src_ref=edge,
            dst_ref=dub.at[pl.ds(rows, 8)],
            send_sem=sm_e.at[j],
            recv_sem=sm_h.at[1, 3],
            device_id={"seq": prv, "tp": j},
            device_id_type=MESH,
        )

    qsum = a_send(0)
    a_send(1)
    for c in range(2, nc):
        a_send(c)
    ube = ub[pl.ds(0, 8), :]
    sbe = sigmoid(ube)
    edge[...] = qsum[0:8, :] * (sbe * (1.0 + ube * (1.0 - sbe)))

    @pl.when(my == 0)
    def _():
        for j in range(n_tp):
            edge_b(j).start()


    phase("o_last")
    o_last()
    phase("wait_e")
    edge_x.wait_recv()

    phase("convbx")
    def conv_back(ref, weights, out, c):
        base = pl.multiple_of(c * Q, Q)
        ext = ref[pl.ds(base, Q + 8), :]
        tail = jnp.where((c < nc - 1) | (me < n_seq - 1), ext[Q:], 0.0)
        ext = jnp.concatenate([ext[:Q], tail], axis=0)
        acc = weights[3:4, :] * ext[:Q]
        for k in range(3):
            acc = acc + weights[k : k + 1, :] * pltpu.roll(ext, Q + 8 - (3 - k), 0)[:Q]
        out[pl.ds(base, Q), :] = acc

    def conv_back_x(c, carry):
        conv_back(dus, cw, o_gx, c)
        return carry

    lax.fori_loop(0, nc, conv_back_x, 0)

    stores[1].start()
    stores[2].start()
    phase("g_last")
    g_last()
    phase("wait_a")
    for c in range(nc):
        for k in range(1, n_tp):
            a_copy(c, k).wait_recv()
    phase("dub")
    for c in range(nc):
        sl = pl.ds(c * Q, Q)
        ubv = ub[sl, :]
        sb = sigmoid(ubv)
        dub[sl, :] = qa[:, c].reshape(Q, 2 * ns).astype(F32) * (sb * (1.0 + ubv * (1.0 - sb)))

    phase("convbb")
    edge_b(0).wait_recv()

    def conv_back_b(c, carry):
        conv_back(dub, cwb, o_gbc, c)
        return carry

    stores[3].start()
    lax.fori_loop(0, nc, conv_back_b, 0)
    stores[4].start()

    phase("drain")
    halo_x.wait_send()
    halo_b.wait_send()
    edge_x.wait_send()

    @pl.when(my == 0)
    def _():
        for j in range(n_tp):
            edge_b(j).wait_send()

    for k in range(1, n_seq):
        for copy in (t_copy, s_copy, sb_copy, v_copy, vb_copy):
            copy(k).wait_send()
    for c in range(nc):
        m_copy(c).wait_send()
        for k in range(1, n_tp):
            a_copy(c, k).wait_send()
        for k in range(1, side):
            q_copy(c, k).wait_send()
    for copy in r_squares + r_inner:
        copy.wait_send()
    for copy in w_copies + d_copies + o_copies + g_copies:
        copy.wait_send()
    for store in stores:
        store.wait()
    phase("")


def publish(*refs):
    count = (len(refs) - 2) // 3
    sources, targets, held = refs[:count], refs[count : 2 * count], refs[2 * count : 3 * count]
    sem_in, sem_out = refs[-2:]
    moves = []
    for source, target, place in zip(sources, targets, held):
        rows = source.shape[0]
        pieces = 4 if rows * source.shape[1] > 200_000 else 1
        for i in range(pieces):
            part = pl.ds(i * (rows // pieces), rows // pieces)
            k = len(moves)
            moves.append(
                (
                    pltpu.make_async_copy(source.at[part], place.at[part], sem_in.at[k]),
                    pltpu.make_async_copy(place.at[part], target.at[part], sem_out.at[k]),
                )
            )
    for load, _ in moves:
        load.start()
    for load, store in moves:
        load.wait()
        store.start()
    for _, store in moves:
        store.wait()


def solution(mesh):
    n_seq, n_tp = mesh.shape["seq"], mesh.shape["tp"]

    def shards(
        inner_x,
        gate_z,
        proj_bc,
        dt_raw,
        a_log,
        dt_bias,
        d_skip,
        conv_x,
        bias_x,
        conv_bc,
        bias_bc,
        norm_gain,
        w_out,
        d_out,
    ):
        rows, ch = inner_x.shape
        heads = a_log.shape[0]
        ns2 = proj_bc.shape[1]
        ns = ns2 // 2
        nc = rows // Q
        nrow = ns // n_seq
        wrows, drows = w_out.shape[1], d_out.shape[1]
        w_t = w_out.T
        d_t = d_out.T.reshape(2, drows // 2, rows)

        big = pltpu.VMEM((rows, ch), F32)
        chunk_states = pltpu.VMEM((nc, ns, ch), F32)
        slices = pltpu.VMEM((n_seq, nrow, ch), F32)
        sem_s = pltpu.SemaphoreType.DMA((2, n_seq))
        sem_t = pltpu.SemaphoreType.DMA((2, n_tp))
        scratch = [
            pltpu.VMEM((drows, rows), BF16),
            big,
            big,
            pltpu.VMEM((rows, ns2), F32),
            pltpu.VMEM((heads, rows), F32),
            pltpu.VMEM((wrows, ch), F32),
            pltpu.VMEM((rows, ch), BF16),
            pltpu.VMEM((rows, ch), BF16),
            pltpu.VMEM((rows, ns2), BF16),
            pltpu.VMEM((heads, rows), BF16),
            pltpu.VMEM((4, ch), F32),
            pltpu.VMEM((ch // LANES, LANES), F32),
            pltpu.VMEM((4, ns2), F32),
            pltpu.VMEM((1, ns2), F32),
            pltpu.VMEM((ch // LANES, LANES), F32),
            pltpu.VMEM((1, heads), F32),
            pltpu.VMEM((1, heads), F32),
            pltpu.VMEM((1, heads), F32),
            pltpu.VMEM((4, 4, wrows, ch), BF16),
            pltpu.VMEM((4, 4, wrows, rows), BF16),
            pltpu.VMEM((16, ch), BF16),
            pltpu.VMEM((16, ns2), BF16),
            pltpu.VMEM((8, LANES), F32),
            pltpu.VMEM((n_seq, 8, LANES), F32),
            big,
            big,
            pltpu.VMEM((nc, heads, Q), F32),
            big,
            big,
            pltpu.VMEM((rows, ns2), F32),
            pltpu.VMEM((rows, ns2), F32),
            chunk_states,
            chunk_states,
            chunk_states,
            big,
            big,
            big,
            big,
            pltpu.VMEM((rows, ch), BF16),
            pltpu.VMEM((rows + 8, ch), F32),
            pltpu.VMEM((rows + 8, ns2), F32),
            pltpu.VMEM((ns, ch), F32),
            slices,
            slices,
            slices,
            slices,
            slices,
            slices,
            slices,
            slices,
            pltpu.VMEM((2, 8, rows), F32),
            pltpu.VMEM((2, n_tp, 8, rows), F32),
            pltpu.VMEM((4, 2, drows, rows), BF16),
            pltpu.VMEM((4, drows, rows), BF16),
            pltpu.VMEM((drows, rows), BF16),
            pltpu.VMEM((2, drows, rows), BF16),
            pltpu.VMEM((4, 4, wrows, ch), BF16),
            *[
                pltpu.VMEM(shape, BF16)
                for shape in 2
                * [
                    (4, wrows // 2, ch),
                    (2, 4, wrows // 2, ch),
                    (wrows // 2, ch),
                    (2, wrows // 2, ch),
                ]
            ],
            pltpu.VMEM((nc, 4, 2, Q // n_tp, ns2), F32),
            pltpu.VMEM((nc, 4, Q // n_tp, ns2), F32),
            pltpu.VMEM((nc, 4, Q // n_tp, ns2), F32),
            chunk_states,
            pltpu.VMEM((n_tp, nc, Q // n_tp, ns2), BF16),
            pltpu.VMEM((Q, LANES), F32),
            pltpu.VMEM((LANES, Q), F32),
            pltpu.VMEM((Q, Q), F32),
            pltpu.VMEM((rows, 1), F32),
            pltpu.VMEM((nc, Q, LANES), F32),
            pltpu.VMEM((rows, ns2), F32),
            pltpu.VMEM((8, ns2), F32),
            pltpu.VMEM((nc, 8, ch), F32),
            pltpu.VMEM((rows, LANES), BF16),
            pltpu.SemaphoreType.DMA((2, nc)),
            pltpu.SemaphoreType.DMA((n_tp,)),
            pltpu.SemaphoreType.DMA((20,)),
            pltpu.SemaphoreType.DMA((2, 4)),
            sem_s,
            pltpu.SemaphoreType.DMA((2, 32)),
            sem_t,
            sem_s,
            sem_s,
            sem_s,
            sem_s,
            pltpu.SemaphoreType.DMA((2, 2 * n_tp)),
            sem_t,
            pltpu.SemaphoreType.DMA((2, 24)),
            pltpu.SemaphoreType.DMA((2, nc * n_tp)),
            pltpu.SemaphoreType.DMA((2, nc * n_tp)),
        ]
        out_t, g_x, g_z, g_bc, g_dt, g_w = pl.pallas_call(
            functools.partial(kernel, (n_seq, n_tp, ch * n_tp)),
            out_shape=[
                jax.ShapeDtypeStruct((drows, rows), BF16),
                jax.ShapeDtypeStruct((rows, ch), F32),
                jax.ShapeDtypeStruct((rows, ch), F32),
                jax.ShapeDtypeStruct((rows, ns2), F32),
                jax.ShapeDtypeStruct((heads, rows), F32),
                jax.ShapeDtypeStruct((wrows, ch), F32),
            ],
            in_specs=[pl.BlockSpec(memory_space=pltpu.HBM)] * 14,
            out_specs=[pl.BlockSpec(memory_space=pltpu.HBM)] * 6,
            scratch_shapes=scratch,
            compiler_params=pltpu.CompilerParams(
                collective_id=0, has_side_effects=True, vmem_limit_bytes=62 * 1024 * 1024
            ),
            name="mixer",
        )(
            inner_x,
            gate_z,
            proj_bc,
            dt_raw.T,
            w_t,
            d_t,
            conv_x,
            bias_x.reshape(-1, LANES),
            conv_bc,
            bias_bc[None, :],
            norm_gain.reshape(-1, LANES),
            a_log[None, :],
            dt_bias[None, :],
            d_skip[None, :],
        )
        results = (g_x, g_z, g_bc, g_w, out_t, g_dt)
        hbm = pl.BlockSpec(memory_space=pltpu.HBM)
        g_x, g_z, g_bc, g_w, out_t, g_dt = pl.pallas_call(
            publish,
            out_shape=[jax.ShapeDtypeStruct(v.shape, v.dtype) for v in results],
            in_specs=[hbm] * 6,
            out_specs=[hbm] * 6,
            scratch_shapes=[pltpu.VMEM(v.shape, v.dtype) for v in results]
            + [pltpu.SemaphoreType.DMA((16,)), pltpu.SemaphoreType.DMA((16,))],
            compiler_params=pltpu.CompilerParams(vmem_limit_bytes=62 * 1024 * 1024),
            name="publish",
        )(*results)
        return out_t.T, g_x, g_z, g_bc, g_dt.T, g_w.T

    in_specs = (
        P("seq", "tp"),
        P("seq", "tp"),
        P("seq", None),
        P("seq", "tp"),
        P("tp"),
        P("tp"),
        P("tp"),
        P(None, "tp"),
        P("tp"),
        P(),
        P(),
        P("tp"),
        P("tp", "seq"),
        P("seq", "tp"),
    )
    out_specs = (
        P("seq", "tp"),
        P("seq", "tp"),
        P("seq", "tp"),
        P("seq", None),
        P("seq", "tp"),
        P("tp", "seq"),
    )
    return jax.shard_map(
        shards, mesh=mesh, in_specs=in_specs, out_specs=out_specs, check_vma=False
    )
```

```python
import functools

import jax
import jax.numpy as jnp
from jax import lax
from jax.experimental import pallas as pl
from jax.experimental.pallas import tpu as pltpu
from jax.sharding import PartitionSpec as P

MESH = pl.DeviceIdType.MESH
F32 = jnp.float32
BF16 = jnp.bfloat16
HIGH = lax.Precision.HIGHEST
EPSILON = 1e-05
NN = ((1,), (0,))
NT = ((1,), (1,))
Q = 128
PAIR = 128
HEAD = 64
LANES = 128


def mm(a, b, dims=NN):
    return lax.dot_general(a.astype(BF16), b.astype(BF16), (dims, ((), ())), preferred_element_type=F32)


def mmh(a, b, dims=NN):
    return lax.dot_general(
        a.astype(F32), b.astype(F32), (dims, ((), ())), precision=HIGH, preferred_element_type=F32
    )


def halves(v):
    high = v.astype(BF16)
    return high, (v - high.astype(F32)).astype(BF16)


def mm3(a, b, dims=NN):
    a0, a1 = halves(a)
    b0, b1 = halves(b)
    return mm(a0, b0, dims) + (mm(a1, b0, dims) + mm(a0, b1, dims))


def parts(v, count):
    out = []
    for _ in range(count):
        piece = v.astype(BF16)
        out.append(piece)
        v = v - piece.astype(F32)
    return out


def iota(shape, dim):
    return lax.broadcasted_iota(jnp.int32, shape, dim)


def sigmoid(v):
    return 1.0 / (1.0 + jnp.exp(-v))


def softplus(v):
    return jnp.maximum(v, 0.0) + jnp.log1p(jnp.exp(-jnp.abs(v)))


def pair_stack(v):
    lane = iota(v.shape, 1)
    return jnp.concatenate(
        [jnp.where(lane < HEAD, v, 0.0), jnp.where(lane >= HEAD, v, 0.0)], axis=0
    )


def kernel(
    sizes,
    ix_in,
    gz_in,
    bc_in,
    raw_in,
    wt,
    dt,
    cw_in,
    bx_in,
    cwb_in,
    bb_in,
    gain_in,
    al_in,
    db_in,
    ds_in,
    out_hbm,
    gx_hbm,
    gz_hbm,
    gbc_hbm,
    gdt_hbm,
    gw_hbm,
    o_out,
    o_gx,
    o_gz,
    o_gbc,
    o_gdt,
    o_gw,
    ix,
    gz,
    bc,
    raw,
    cw,
    bx,
    cwb,
    bb,
    gain,
    al,
    db,
    ds,
    wfull,
    dfull,
    hx,
    hb,
    dsend,
    dbuf,
    st,
    lx,
    lt,
    u,
    x,
    ub,
    bcv,
    fr,
    sst,
    cf,
    y,
    gated,
    gn,
    gm,
    nb,
    dus,
    dub,
    rcur,
    se,
    sr,
    en,
    sin,
    re,
    rr,
    ren,
    rin,
    ts,
    tr,
    pb,
    pp,
    po1,
    po2,
    gb,
    ga1,
    ga2,
    ga3,
    ga4,
    gb1,
    gb2,
    gb3,
    gb4,
    qs,
    qm,
    qr,
    rst,
    qa,
    arow,
    acol,
    dga,
    invs,
    swings,
    dmap,
    edge,
    frow,
    packed,
    sm_m,
    sm_e,
    sm_l,
    sm_h,
    sm_d,
    sm_w,
    sm_g,
    sm_s,
    sm_b,
    sm_r,
    sm_q,
    sm_t,
    sm_o,
    sm_v,
    sm_p,
    sm_a,
):
    n_seq, n_tp, inner = sizes
    rows, ch = ix.shape
    nc = rows // Q
    heads = raw.shape[0]
    pairs = ch // PAIR
    ns = bc.shape[1] // 2
    me, my = lax.axis_index("seq"), lax.axis_index("tp")
    wrows = wt.shape[0]
    drows = 2 * dt.shape[1]
    nrow = ns // n_seq

    scope = []

    def phase(name):
        if scope:
            scope.pop().__exit__(None, None, None)
        if name:
            scope.append(jax.named_scope(name))
            scope[0].__enter__()

    side = 4
    zi, xi = lax.div(me, side), lax.rem(me, side)
    yi, core = lax.div(my, 2), lax.rem(my, 2)

    def step(v, k):
        return lax.rem(v + k + side, side)

    x_up, x_dn = step(xi, 1), step(xi, -1)
    z_up, z_dn = step(zi, 1), step(zi, -1)
    y_up, y_dn = step(yi, 1), step(yi, -1)
    x_far, z_far, y_far = step(xi, 2), step(zi, 2), step(yi, 2)
    to_xu, to_xd = zi * side + x_up, zi * side + x_dn
    to_zu, to_zd = z_up * side + xi, z_dn * side + xi
    to_xf, to_zf = zi * side + x_far, z_far * side + xi
    to_yu, to_yd = y_up * 2 + core, y_dn * 2 + core
    mate = yi * 2 + 1 - core

    def hops(pair):
        return sum(min(v, side - v) for v in pair)

    others = [(a, b) for a in range(side) for b in range(side) if a or b]
    others.sort(key=lambda pair: -hops(pair))

    def seq_peer(k):
        a, b = others[k - 1]
        return step(zi, a) * side + step(xi, b)

    def tp_peer(k):
        return lax.rem(my + k, n_tp)

    phase("barrier1")
    barrier = pltpu.get_barrier_semaphore()
    for k in range(1, n_seq):
        pl.semaphore_signal(barrier, inc=1, device_id={"seq": seq_peer(k)}, device_id_type=MESH)
    for k in range(1, n_tp):
        pl.semaphore_signal(barrier, inc=1, device_id={"tp": tp_peer(k)}, device_id_type=MESH)

    def remote(src, dst, sems, k, axis, peer):
        return pltpu.make_async_remote_copy(
            src_ref=src,
            dst_ref=dst,
            send_sem=sems.at[0, k],
            recv_sem=sems.at[1, k],
            device_id={axis: peer},
            device_id_type=MESH,
        )

    nxt, prv = lax.rem(me + 1, n_seq), lax.rem(me + n_seq - 1, n_seq)

    @pl.when(my > 0)
    def _():
        pl.semaphore_signal(barrier, inc=1, device_id={"seq": nxt, "tp": 0}, device_id_type=MESH)

    staged = [
        (raw_in, raw),
        (al_in, al),
        (db_in, db),
        (ds_in, ds),
        (wt, wfull.at[zi, xi]),
        (dt, dfull.at[yi, pl.ds(2 * core, 2)]),
        (ix_in, ix),
        (bc_in, bc),
        (cw_in, cw),
        (bx_in, bx),
        (cwb_in, cwb),
        (bb_in, bb),
        (gain_in, gain),
        (gz_in, gz),
    ]
    loads = [pltpu.make_async_copy(a, b, sm_l.at[i]) for i, (a, b) in enumerate(staged)]
    for load in loads:
        load.start()
    results = [(o_gz, gz_hbm), (o_out, out_hbm), (o_gx, gx_hbm), (o_gw, gw_hbm), (o_gbc, gbc_hbm), (o_gdt, gdt_hbm)]
    stores = [pltpu.make_async_copy(a, b, sm_l.at[14 + i]) for i, (a, b) in enumerate(results)]
    phase("staging")
    for load in loads[:9]:
        load.wait()
    phase("barrier")
    pl.semaphore_wait(barrier, n_seq + n_tp - 2 + jnp.where(my == 0, n_tp - 1, 0))

    phase("start")
    halo_x = remote(ix.at[pl.ds(rows - 16, 16)], hx, sm_h, 0, "seq", nxt)
    halo_b = remote(bc.at[pl.ds(rows - 16, 16)], hb, sm_h, 1, "seq", nxt)
    halo_x.start()
    halo_b.start()

    half = wrows // 2
    near = 48
    ra, rb = pl.ds(0, half), pl.ds(half, half)
    ra1, ra2 = pl.ds(0, near), pl.ds(near, half - near)
    rb1, rb2 = pl.ds(half, near), pl.ds(half + near, half - near)
    lo, hi, every = pl.ds(0, 2), pl.ds(2, 2), pl.ds(0, side)

    def w_view(z, x, r):
        return wfull.at[z, x, r]

    def w_move(i, peer, z, x, r, src=None):
        return remote(w_view(z, x, r) if src is None else src, w_view(z, x, r), sm_w, i, "seq", peer)

    w_copies = [
        w_move(0, to_xu, zi, xi, ra),
        w_move(1, to_xd, zi, xi, ra),
        w_move(2, to_zu, zi, xi, rb),
        w_move(3, to_zd, zi, xi, rb),
        w_move(4, to_zu, zi, xi, ra),
        w_move(5, to_zd, zi, xi, ra),
        w_move(6, to_xu, zi, xi, rb),
        w_move(7, to_xd, zi, xi, rb),
        w_move(8, to_xu, zi, x_dn, ra1),
        w_move(9, to_xd, zi, x_up, ra2),
        w_move(10, to_zu, z_dn, xi, rb1),
        w_move(11, to_zd, z_up, xi, rb2),
        w_move(12, to_zu, zi, x_up, ra),
        w_move(13, to_zd, zi, x_up, ra),
        w_move(14, to_xu, z_up, xi, rb),
        w_move(15, to_xd, z_up, xi, rb),
        w_move(16, to_zu, zi, x_dn, ra),
        w_move(17, to_zd, zi, x_dn, ra),
        w_move(18, to_xu, z_dn, xi, rb),
        w_move(19, to_xd, z_dn, xi, rb),
        w_move(20, to_zu, zi, x_far, ra),
        w_move(21, to_zd, zi, x_far, ra),
        w_move(22, to_xu, z_far, xi, rb),
        w_move(23, to_xd, z_far, xi, rb),
        w_move(24, to_zu, z_dn, xi, ra),
        w_move(25, to_xu, zi, x_dn, rb),
        w_move(26, to_zu, z_dn, x_up, ra),
        w_move(27, to_xu, z_up, x_dn, rb),
        w_move(28, to_zd, z_up, x_dn, ra),
        w_move(29, to_xd, z_dn, x_up, rb),
        w_move(30, to_zd, z_up, x_far, ra),
        w_move(31, to_xd, z_far, x_up, rb),
    ]

    dhalf = drows // 2

    def d_view(y, c, off=0, size=drows):
        if size == drows:
            return dfull.at[y, pl.ds(2 * c, 2)]
        return dfull.at[y, 2 * c + off // size]

    def d_move(i, peer, y, c, off=0, size=drows, src=None):
        view = d_view(y, c, off, size)
        return remote(view if src is None else src, view, sm_g, i, "tp", peer)

    d_copies = [
        d_move(0, to_yu, yi, core),
        d_move(1, to_yd, yi, core),
        d_move(2, mate, yi, core),
        d_move(3, to_yu, y_dn, core, 0, dhalf),
        d_move(4, to_yd, y_up, core, dhalf, dhalf),
        d_move(5, mate, y_dn, core),
        d_move(6, mate, y_up, core),
        d_move(7, mate, y_far, core),
    ]

    def start(copies, first, last):
        for copy in copies[first:last]:
            copy.start()

    def arrived(copies, first, last):
        for copy in copies[first:last]:
            copy.wait_recv()

    start(w_copies, 0, 8)
    start(d_copies, 0, 3)

    phase("steps")
    slot = lax.rem(iota((LANES, 2 * ch), 0), 32)
    wanted = iota((LANES, 2 * ch), 1) // HEAD
    wanted = jnp.where(wanted < heads, wanted, wanted - heads + 16)
    spread = ((slot == wanted) & (iota((LANES, 2 * ch), 0) < 96)).astype(BF16)
    spread_h = (iota((heads, ch), 1) // HEAD == iota((heads, ch), 0)).astype(F32)
    ident = (iota((heads, heads), 0) == iota((heads, heads), 1)).astype(F32)
    negexp = -jnp.exp(al[...])
    skip_x = mmh(jnp.broadcast_to(ds[...], (8, heads)), spread_h)[0:1]
    tri_u = (iota((Q, Q), 0) <= iota((Q, Q), 1)).astype(F32)

    def column(v):
        return mmh(ident, jnp.broadcast_to(v, (8, heads)), NT)[:, 0:1]

    def in_line(ref):
        return jnp.concatenate([ref[i : i + 1] for i in range(ref.shape[0])], axis=1)

    dt_col, neg_col = column(db[...]), column(negexp)

    for load in loads[9:]:
        load.wait()
    bias_line, gain_line = in_line(bx), in_line(gain)

    def steps(c, total):
        sl = pl.ds(pl.multiple_of(c * Q, Q), Q)
        s_c = softplus(raw[:, sl].astype(F32) + dt_col)
        cum = mmh(s_c * neg_col, tri_u)
        lt[c] = cum
        gap = jnp.zeros((16 - heads, Q), F32)
        pieces = []
        for a, b in zip(parts(s_c, 3), parts(cum, 3)):
            pieces += [a.astype(F32), gap, b.astype(F32), gap]
        turned = jnp.transpose(jnp.concatenate([*pieces, jnp.zeros((LANES - 96, Q), F32)], axis=0))
        packed[sl, :] = turned.astype(BF16)
        return total + turned[Q - 1 : Q, :]

    total = lax.fori_loop(0, nc, steps, jnp.zeros((1, LANES), F32))
    st[...] = mm(packed[...], spread[:, :ch])
    lx[...] = mm(packed[...], spread[:, ch:])
    dsend[...] = jnp.broadcast_to(total, (8, LANES))
    dbuf[me] = dsend[...]

    def t_copy(k):
        return remote(dsend, dbuf.at[me], sm_d, k, "seq", seq_peer(k))

    for k in range(1, n_seq):
        t_copy(k).start()

    phase("convs")
    def conv_of(ref, halo, weights, bias, c):
        base = pl.multiple_of(c * Q, Q)
        own = ref[pl.ds(base, Q), :].astype(F32)
        if halo is None:
            head = ref[pl.ds(pl.multiple_of(c * Q - 16, 16), 16), :].astype(F32)[8:16]
        else:
            head = jnp.where(me > 0, halo[...].astype(F32), 0.0)[8:16]
        ext = jnp.concatenate([head, own], axis=0)
        acc = bias + weights[3:4, :] * own
        for k in range(3):
            acc = acc + weights[k : k + 1, :] * pltpu.roll(ext, Q + 8 - (5 + k), 0)[:Q]
        return acc

    def convs(c, carry, edge_of=(None, None)):
        sl = pl.ds(pl.multiple_of(c * Q, Q), Q)
        vb = conv_of(bc, edge_of[0], cwb, bb[...], c)
        ub[sl, :] = vb
        pbc = vb * sigmoid(vb)
        bcv[sl, :] = pbc
        vx = conv_of(ix, edge_of[1], cw, bias_line, c)
        u[sl, :] = vx
        xv = vx * sigmoid(vx)
        x[sl, :] = xv
        cum = lx[sl, :]
        to_end = jnp.exp(cum[Q - 1 : Q, :] - cum)
        b_t = jnp.transpose(pbc[:, :ns])
        fresh = mm3(b_t, xv * st[sl, :] * to_end)
        fr[c] = fresh
        return carry

    lax.fori_loop(1, nc, convs, 0)
    phase("wait_halo")
    halo_x.wait_recv()
    halo_b.wait_recv()
    phase("conv0")
    convs(0, 0, (hb, hx))
    end = fr[0]
    for c in range(1, nc):
        end = jnp.exp(lx[pl.ds(c * Q + Q - 1, 1), :]) * end + fr[c]
    se[...] = end.reshape(n_seq, nrow, ch)

    phase("send_s")
    def s_copy(k):
        return remote(se.at[seq_peer(k)], sr.at[me], sm_s, k, "seq", seq_peer(k))

    def sb_copy(k):
        return remote(en.at[seq_peer(k)], sin.at[me], sm_b, k, "seq", seq_peer(k))

    for k in range(1, n_seq):
        s_copy(k).start()
    sr[me] = se[me]
    phase("wait_w1")
    arrived(w_copies, 0, 4)
    start(w_copies, 8, 16)

    upper = iota((Q, Q), 0) >= iota((Q, Q), 1)
    lower = iota((Q, Q), 0) <= iota((Q, Q), 1)

    phase("inside")
    def inside(c, carry):
        sl = pl.ds(pl.multiple_of(c * Q, Q), Q)
        scores = mm3(bcv[sl, ns:], bcv[sl, :ns], NT)
        for p in range(pairs):
            ps = slice(p * PAIR, (p + 1) * PAIR)
            both = []
            for h in (2 * p, 2 * p + 1):
                diff = lx[sl, h * HEAD : h * HEAD + 1] - lt[c, h : h + 1, :]
                decay = jnp.exp(jnp.where(upper, diff, -1e30))
                both.append(decay * scores)
            y[sl, ps] = mm3(jnp.concatenate(both, axis=1), pair_stack(x[sl, ps] * st[sl, ps]))
        return carry

    lax.fori_loop(0, nc, inside, 0)
    phase("wait_d1")
    arrived(d_copies, 0, 2)
    start(d_copies, 3, 7)
    phase("wait_s")
    for k in range(1, n_seq):
        t_copy(k).wait_recv()
    for k in range(1, n_seq):
        s_copy(k).wait_recv()
    phase("scan")
    fade = jnp.exp(sum(mm(piece, spread[:, ch:]) for piece in parts(dbuf[:, 0, :], 3)))

    acc = jnp.zeros((nrow, ch), F32)
    for j in range(n_seq):
        en[j] = acc
        acc = fade[j : j + 1] * acc + sr[j]
    for k in range(1, n_seq):
        sb_copy(k).start()
    sin[me] = en[me]
    start(w_copies, 16, 20)
    phase("wait_w2")
    arrived(w_copies, 8, 12)
    start(w_copies, 20, 24)

    phase("wait_sb")
    for k in range(1, n_seq):
        sb_copy(k).wait_recv()
    arrived(d_copies, 3, 5)
    start(d_copies, 7, 8)
    phase("combine")
    lane = iota((Q, LANES), 1)

    def to_row(i, c, v):
        ts[i, :, pl.ds(pl.multiple_of(c * Q, Q), Q)] = jnp.transpose(jnp.where(lane == 0, v, 0.0))[:8]

    def to_column(row, c):
        block = jnp.concatenate([row[:, c * Q : (c + 1) * Q], jnp.zeros((Q - 8, Q), F32)], axis=0)
        return jnp.transpose(block)[:, 0:1]

    def combine(c, state):
        sl = pl.ds(pl.multiple_of(c * Q, Q), Q)
        sst[c] = state
        cum = lx[sl, :]
        mixed = y[sl, :] + jnp.exp(cum) * mm3(bcv[sl, ns:], state) + skip_x * x[sl, :]
        y[sl, :] = mixed
        zv = gz[sl, :].astype(F32)
        gv = mixed * zv * sigmoid(zv)
        gated[sl, :] = gv
        to_row(0, c, jnp.sum(gv * gv, axis=1, keepdims=True))
        return jnp.exp(cum[Q - 1 : Q, :]) * state + fr[c]

    lax.fori_loop(0, nc, combine, sin[...].reshape(ns, ch))

    def r_copies(i):
        return [
            remote(ts.at[i], tr.at[i, my], sm_t, i * n_tp + k, "tp", tp_peer(k)) for k in range(1, n_tp)
        ]

    def r_total(i):
        total = tr[i, 0]
        for j in range(1, n_tp):
            total = total + tr[i, j]
        return total

    r_squares, r_inner = r_copies(0), r_copies(1)
    start(r_squares, 0, n_tp - 1)
    tr[0, my] = ts[0]

    phase("wait_w_near")
    arrived(w_copies, 4, 8)
    arrived(w_copies, 12, 20)
    start(w_copies, 24, 30)
    phase("gn_own")
    kb = wrows * side

    moves = (0, 1, -1, 2)

    def gn_early(k):
        zz, xx = step(zi, moves[k]), step(xi, moves[k])
        d_rows = jnp.concatenate(
            [dfull[zz, :, ra].reshape(kb // 2, rows), dfull[:, xx, rb].reshape(kb // 2, rows)], axis=0
        )
        w_rows = jnp.concatenate(
            [wfull[zz, :, ra].reshape(kb // 2, ch), wfull[:, xx, rb].reshape(kb // 2, ch)], axis=0
        )
        part = mm(jnp.transpose(d_rows), w_rows)
        gn[...] = part if k == 0 else gn[...] + part

    arrived(d_copies, 2, 3)
    arrived(d_copies, 5, 7)
    arrived(d_copies, 7, 8)
    gn_early(0)
    phase("wait_w3")
    arrived(w_copies, 20, 24)
    start(w_copies, 30, 32)
    phase("gn")
    gn_early(1)
    gn_early(2)

    phase("wait_ss")
    arrived(r_squares, 0, n_tp - 1)
    inv_row = lax.rsqrt(r_total(0) / inner + EPSILON)
    phase("nb")
    for c in range(nc):
        sl = pl.ds(c * Q, Q)
        inv = to_column(inv_row, c)
        invs[sl, :] = inv
        nb[sl, :] = (gated[sl, :] * inv * gain_line).astype(BF16)
    phase("gradw")
    g_copies = [
        remote(gb.at[z_far, lo, ra], ga1.at[lo], sm_v, 0, "seq", to_zu),
        remote(gb.at[z_far, hi, ra], ga1.at[hi], sm_v, 1, "seq", to_zd),
        remote(gb.at[lo, x_far, rb], gb1.at[lo], sm_v, 2, "seq", to_xu),
        remote(gb.at[hi, x_far, rb], gb1.at[hi], sm_v, 3, "seq", to_xd),
        remote(gb.at[z_up, hi, ra], ga2.at[0, hi], sm_v, 4, "seq", to_zu),
        remote(gb.at[z_dn, lo, ra], ga2.at[1, lo], sm_v, 5, "seq", to_zd),
        remote(gb.at[hi, x_up, rb], gb2.at[0, hi], sm_v, 6, "seq", to_xu),
        remote(gb.at[lo, x_dn, rb], gb2.at[1, lo], sm_v, 7, "seq", to_xd),
        remote(gb.at[z_up, 0, ra], ga2.at[0, 0], sm_v, 8, "seq", to_zu),
        remote(gb.at[z_dn, 2, ra], ga2.at[1, 2], sm_v, 9, "seq", to_zd),
        remote(gb.at[0, x_up, rb], gb2.at[0, 0], sm_v, 10, "seq", to_xu),
        remote(gb.at[2, x_dn, rb], gb2.at[1, 2], sm_v, 11, "seq", to_xd),
        remote(gb.at[z_up, 1, ra], ga2.at[0, 1], sm_v, 20, "seq", to_zu),
        remote(gb.at[z_dn, 3, ra], ga2.at[1, 3], sm_v, 21, "seq", to_zd),
        remote(gb.at[1, x_up, rb], gb2.at[0, 1], sm_v, 22, "seq", to_xu),
        remote(gb.at[3, x_dn, rb], gb2.at[1, 3], sm_v, 23, "seq", to_xd),
        remote(gb.at[zi, x_far, ra], ga3, sm_v, 12, "seq", to_xf),
        remote(gb.at[z_far, xi, rb], gb3, sm_v, 13, "seq", to_zf),
        remote(gb.at[zi, x_up, ra], ga4.at[0], sm_v, 14, "seq", to_xu),
        remote(gb.at[zi, x_dn, ra], ga4.at[1], sm_v, 15, "seq", to_xd),
        remote(gb.at[z_up, xi, rb], gb4.at[0], sm_v, 16, "seq", to_zu),
        remote(gb.at[z_dn, xi, rb], gb4.at[1], sm_v, 17, "seq", to_zd),
    ]

    def plus(ref, index, *others):
        total = ref[index].astype(F32)
        for part in others:
            total = total + part.astype(F32)
        ref[index] = total.astype(BF16)

    def g_block(k, carry):
        b = step(zi, 2 + k)
        gb[b] = mm(dfull[b].reshape(kb, rows), nb[...]).astype(BF16).reshape(side, wrows, ch)

        @pl.when(k == 0)
        def _():
            start(g_copies, 0, 2)

        return carry

    lax.fori_loop(0, side, g_block, 0)
    start(g_copies, 2, 8)

    def g_second():
        arrived(g_copies, 0, 4)
        for j in range(2):
            plus(gb, (z_up, j, ra), ga1[j])
            plus(gb, (z_dn, 2 + j, ra), ga1[2 + j])
            plus(gb, (j, x_up, rb), gb1[j])
            plus(gb, (2 + j, x_dn, rb), gb1[2 + j])
        start(g_copies, 8, 12)

    def g_third():
        arrived(g_copies, 4, 16)
        for j in range(side):
            plus(gb, (zi, j, ra), ga2[0, j], ga2[1, j])
            plus(gb, (j, xi, rb), gb2[0, j], gb2[1, j])
        start(g_copies, 16, 22)

    def g_last():
        arrived(g_copies, 16, 22)

        def landed(own, far, near):
            return own.astype(F32) + far.astype(F32) + near[0].astype(F32) + near[1].astype(F32)

        o_gw[ra, :] = landed(gb[zi, xi, ra], ga3[...], ga4)
        o_gw[rb, :] = landed(gb[zi, xi, rb], gb3[...], gb4)

    def o_second():
        arrived(o_copies, 0, 1)
        for j in range(side):
            plus(pb, (j, core), pp[j])
        start(o_copies, 1, 3)

    def o_third():
        arrived(o_copies, 1, 3)
        plus(pb, (y_up, core, o_half1), po1[o_half1])
        plus(pb, (y_dn, core, o_half2), po1[o_half2])
        start(o_copies, 3, 5)

    def o_last():
        arrived(o_copies, 3, 5)
        total = pb[yi, core].astype(F32) + po2[0].astype(F32) + po2[1].astype(F32)
        o_out[...] = total.astype(BF16)
    phase("wait_w4")
    arrived(w_copies, 24, 32)
    phase("gn_last")
    gn_early(3)
    phase("ip")

    def inner_sums(c, carry):
        sl = pl.ds(pl.multiple_of(c * Q, Q), Q)
        scaled = gn[sl, :] * gain_line
        gn[sl, :] = scaled
        to_row(1, c, jnp.sum(scaled * gated[sl, :], axis=1, keepdims=True))
        return carry

    lax.fori_loop(0, nc, inner_sums, 0)
    start(r_inner, 0, n_tp - 1)
    tr[1, my] = ts[1]
    phase("outmm")
    def share(y0, c0):
        block = wfull[y0, pl.ds(2 * c0, 2)].reshape(drows, ch)
        pb[y0, c0] = mm(block, nb[...], NT).astype(BF16)

    def other(j, carry):
        share(j, 1 - core)
        return carry

    def same(j, carry):
        share(j, core)
        return carry

    o_half1, o_half2 = pl.ds(0, dhalf), pl.ds(dhalf, dhalf)
    o_copies = [
        remote(pb.at[every, 1 - core], pp, sm_o, 0, "tp", mate),
        remote(pb.at[y_far, core, o_half1], po1.at[o_half1], sm_o, 1, "tp", to_yu),
        remote(pb.at[y_far, core, o_half2], po1.at[o_half2], sm_o, 2, "tp", to_yd),
        remote(pb.at[y_up, core], po2.at[0], sm_o, 3, "tp", to_yu),
        remote(pb.at[y_dn, core], po2.at[1], sm_o, 4, "tp", to_yd),
    ]
    lax.fori_loop(0, side, other, 0)
    start(o_copies, 0, 1)
    lax.fori_loop(0, side, same, 0)
    phase("wait_ip")
    arrived(r_inner, 0, n_tp - 1)
    ip_row = r_total(1) / inner * inv_row * inv_row * inv_row
    phase("norm")
    for c in range(nc):
        sl = pl.ds(c * Q, Q)
        gg = invs[sl, :] * gn[sl, :] - gated[sl, :] * to_column(ip_row, c)
        zv = gz[sl, :].astype(F32)
        sg = sigmoid(zv)
        o_gz[sl, :] = gg * y[sl, :] * sg * (1.0 + zv * (1.0 - sg))
        gmv = gg * zv * sg
        gm[sl, :] = gmv
        c_t = jnp.transpose(bcv[sl, ns:])
        cf[c] = mm3(c_t, gmv * jnp.exp(lx[sl, :]))

    racc = cf[nc - 1]
    for c in reversed(range(nc - 1)):
        racc = cf[c] + jnp.exp(lx[pl.ds(c * Q + Q - 1, 1), :]) * racc
    re[...] = racc.reshape(n_seq, nrow, ch)

    phase("send_v")
    def v_copy(k):
        return remote(re.at[seq_peer(k)], rr.at[me], sm_r, k, "seq", seq_peer(k))

    def vb_copy(k):
        return remote(ren.at[seq_peer(k)], rin.at[me], sm_q, k, "seq", seq_peer(k))

    for k in range(1, n_seq):
        v_copy(k).start()
    rr[me] = re[me]
    stores[0].start()
    phase("g_second")
    g_second()
    phase("o_second")
    o_second()
    phase("intra")
    def back_inside(c, carry):
        sl = pl.ds(pl.multiple_of(c * Q, Q), Q)
        bmap, cmap = bcv[sl, :ns], bcv[sl, ns:]
        scores = mm3(cmap, bmap, NT)
        scores_t = mm3(bmap, cmap, NT)
        arow[...] = jnp.zeros((Q, LANES), F32)
        acol[...] = jnp.zeros((LANES, Q), F32)
        dga[...] = jnp.zeros((Q, Q), F32)
        for p in range(pairs):
            ps = slice(p * PAIR, (p + 1) * PAIR)
            g2 = gm[sl, ps]
            cross = mm3(g2, pair_stack(x[sl, ps] * st[sl, ps]), NT)
            both = []
            for i_h, h in enumerate((2 * p, 2 * p + 1)):
                diff = lx[sl, h * HEAD : h * HEAD + 1] - lt[c, h : h + 1, :]
                weighted = jnp.exp(jnp.where(upper, diff, -1e30)) * cross[:, i_h * Q : (i_h + 1) * Q]
                dga[...] += weighted
                term = weighted * scores
                arow[...] += jnp.where(lane == h, jnp.sum(term, axis=1, keepdims=True), 0.0)
                acol[h : h + 1, :] = jnp.sum(term, axis=0, keepdims=True)
                decay_t = jnp.exp(jnp.where(lower, lt[c, h : h + 1, :] - lx[sl, h * HEAD : h * HEAD + 1], -1e30))
                both.append((decay_t * scores_t).astype(BF16))
            y[sl, ps] = mm(jnp.concatenate(both, axis=1), pair_stack(g2))
        dgv = dga[...]
        swings[c] = arow[...] - jnp.transpose(acol[...])
        dmap[sl, :ns] = mm3(jnp.transpose(dgv), cmap)
        dmap[sl, ns:] = mm3(dgv, bmap)
        return carry

    def back_insides(first):
        def one(i, carry):
            return back_inside(first - i, carry)

        lax.fori_loop(0, nc // 2, one, 0)

    back_insides(nc - 1)
    back_insides(nc // 2 - 1)

    phase("wait_v")
    for k in range(1, n_seq):
        v_copy(k).wait_recv()
    acc = jnp.zeros((nrow, ch), F32)
    for j in reversed(range(n_seq)):
        ren[j] = acc
        acc = fade[j : j + 1] * acc + rr[j]
    for k in range(1, n_seq):
        vb_copy(k).start()
    rin[me] = ren[me]
    start(g_copies, 12, 16)
    phase("o_third")
    o_third()
    phase("forward_part")
    to_head = (lax.rem(iota((2 * ch, LANES), 0), ch) // HEAD == iota((2 * ch, LANES), 1)).astype(BF16)
    neg_c = jnp.concatenate([negexp, jnp.zeros((1, LANES - heads), F32)], axis=1)
    blk = Q // n_tp
    tail_sum = jnp.concatenate([tri_u.astype(BF16)] * 3, axis=1)
    head_sum = jnp.concatenate([(iota((Q, Q), 0) > iota((Q, Q), 1)).astype(BF16)] * 3, axis=1)

    def by_head(v):
        return mm(jnp.concatenate(parts(v, 2), axis=1), to_head)

    def reads(i, later):
        c = nc - 1 - i
        sl = pl.ds(pl.multiple_of(c * Q, Q), Q)
        cmap = bcv[sl, ns:]
        sv = sst[c]
        cum = lx[sl, :]
        last = cum[Q - 1 : Q, :]
        gg = gm[sl, :] * jnp.exp(cum)
        dmap[sl, ns:] += mm3(gg, sv, NT)
        swings[c] += by_head(gg * mm(cmap, sv))
        rv = rcur[...]
        rst[c] = rv
        reach = x[sl, :] * st[sl, :] * jnp.exp(last - cum)
        dmap[sl, :ns] += mm3(reach, rv, NT)
        gn[sl, :] = reach * later
        frow[c] = jnp.broadcast_to(later, (8, ch))
        rcur[...] = cf[c] + jnp.exp(last) * rv
        return later * jnp.exp(last)

    rcur[...] = jnp.zeros((ns, ch), F32)
    lax.fori_loop(0, nc, reads, jnp.ones((1, ch), F32))
    phase("wait_vb")
    for k in range(1, n_seq):
        vb_copy(k).wait_recv()
    phase("inter")
    rcur[...] = rin[...].reshape(ns, ch)
    def m_copy(c):
        return remote(qs.at[c, every, 1 - core], qm.at[c], sm_m, c, "tp", mate)

    def q_copy(c, k):
        y1 = step(yi, k)
        return remote(qs.at[c, y1, core], qr.at[c, yi], sm_p, c * side + k, "tp", y1 * 2 + core)

    def q_send(c):
        m_copy(c).wait_recv()
        for j in range(side):
            qs[c, j, core] += qm[c, j]
        for k in range(1, side):
            q_copy(c, k).start()
        qr[c, yi] = qs[c, yi, core]

    def a_copy(c, k):
        return remote(qa.at[my, c], qa.at[my, c], sm_a, c * n_tp + k, "tp", tp_peer(k))

    def a_send(c):
        for k in range(1, side):
            q_copy(c, k).wait_recv()
        total = qr[c, 0] + qr[c, 1] + qr[c, 2] + qr[c, 3]
        qa[my, c] = total.astype(BF16)
        for k in range(1, n_tp):
            a_copy(c, k).start()
        return total

    def back_b(c, carry):
        sl = pl.ds(pl.multiple_of(c * Q, Q), Q)
        qs[c, :, :, :, :ns] = dmap[sl, :ns].reshape(side, 2, blk, ns)
        qs[c, :, :, :, ns:] = dmap[sl, ns:].reshape(side, 2, blk, ns)
        m_copy(c).start()
        return carry

    dmap[:, :ns] += mm3(gn[...], rcur[...], NT)
    lax.fori_loop(0, nc, back_b, 0)
    phase("inter2")

    def back(i, carry):
        c = i
        sl = pl.ds(pl.multiple_of(c * Q, Q), Q)
        cum = lx[sl, :]
        last = cum[Q - 1 : Q, :]
        rv = rst[c] + frow[c][0:1] * rcur[...]
        xv = x[sl, :]
        sx = st[sl, :]
        d_in = mm(bcv[sl, :ns], rv) * jnp.exp(last - cum)
        dxt = y[sl, :] + d_in
        uv = u[sl, :]
        su = sigmoid(uv)
        dus[sl, :] = (sx * dxt + skip_x * gm[sl, :]) * (su * (1.0 + uv * (1.0 - su)))
        per_head = by_head(jnp.concatenate([xv * sx * d_in, xv * dxt], axis=0))
        fixed = by_head(
            jnp.broadcast_to(jnp.sum(rv * sst[c], axis=0, keepdims=True) * jnp.exp(last), (8, ch))
        )[0:1]
        dld = (
            mm(tail_sum, jnp.concatenate(parts(swings[c], 3), axis=0))
            + mm(head_sum, jnp.concatenate(parts(per_head[:Q], 3), axis=0))
            + fixed
        )
        dstep = per_head[Q:] + dld * neg_c
        slope = sigmoid(raw[:, sl].astype(F32) + dt_col)
        o_gdt[:, sl] = jnp.transpose(dstep)[:heads] * slope

        @pl.when(i == 0)
        def _():
            for j in range(nc):
                q_send(j)
            edge_x.start()

        @pl.when(i == 1)
        def _():
            g_third()

        return carry

    edge_x = remote(dus.at[pl.ds(0, 8)], dus.at[pl.ds(rows, 8)], sm_h, 2, "seq", prv)
    lax.fori_loop(0, nc, back, 0)
    stores[5].start()
    phase("wait_q")

    def edge_b(j):
        return pltpu.make_async_remote_copy(
            src_ref=edge,
            dst_ref=dub.at[pl.ds(rows, 8)],
            send_sem=sm_e.at[j],
            recv_sem=sm_h.at[1, 3],
            device_id={"seq": prv, "tp": j},
            device_id_type=MESH,
        )

    qsum = a_send(0)
    a_send(1)
    for c in range(2, nc):
        a_send(c)
    ube = ub[pl.ds(0, 8), :]
    sbe = sigmoid(ube)
    edge[...] = qsum[0:8, :] * (sbe * (1.0 + ube * (1.0 - sbe)))

    @pl.when(my == 0)
    def _():
        for j in range(n_tp):
            edge_b(j).start()


    phase("o_last")
    o_last()
    phase("wait_e")
    edge_x.wait_recv()

    phase("convbx")
    def conv_back(ref, weights, out, c):
        base = pl.multiple_of(c * Q, Q)
        ext = ref[pl.ds(base, Q + 8), :]
        tail = jnp.where((c < nc - 1) | (me < n_seq - 1), ext[Q:], 0.0)
        ext = jnp.concatenate([ext[:Q], tail], axis=0)
        acc = weights[3:4, :] * ext[:Q]
        for k in range(3):
            acc = acc + weights[k : k + 1, :] * pltpu.roll(ext, Q + 8 - (3 - k), 0)[:Q]
        out[pl.ds(base, Q), :] = acc

    def conv_back_x(c, carry):
        conv_back(dus, cw, o_gx, c)
        return carry

    lax.fori_loop(0, nc, conv_back_x, 0)

    stores[1].start()
    stores[2].start()
    phase("wait_a")
    for c in range(nc):
        for k in range(1, n_tp):
            a_copy(c, k).wait_recv()
    phase("dub")
    for c in range(nc):
        sl = pl.ds(c * Q, Q)
        ubv = ub[sl, :]
        sb = sigmoid(ubv)
        dub[sl, :] = qa[:, c].reshape(Q, 2 * ns).astype(F32) * (sb * (1.0 + ubv * (1.0 - sb)))

    phase("convbb")
    edge_b(0).wait_recv()

    def conv_back_b(c, carry):
        conv_back(dub, cwb, o_gbc, c)
        return carry

    lax.fori_loop(0, nc, conv_back_b, 0)
    stores[4].start()
    g_last()
    stores[3].start()

    phase("drain")
    halo_x.wait_send()
    halo_b.wait_send()
    edge_x.wait_send()

    @pl.when(my == 0)
    def _():
        for j in range(n_tp):
            edge_b(j).wait_send()

    for k in range(1, n_seq):
        for copy in (t_copy, s_copy, sb_copy, v_copy, vb_copy):
            copy(k).wait_send()
    for c in range(nc):
        m_copy(c).wait_send()
        for k in range(1, n_tp):
            a_copy(c, k).wait_send()
        for k in range(1, side):
            q_copy(c, k).wait_send()
    for copy in r_squares + r_inner:
        copy.wait_send()
    for copy in w_copies + d_copies + o_copies + g_copies:
        copy.wait_send()
    for store in stores:
        store.wait()
    phase("")


def publish(*refs):
    count = (len(refs) - 2) // 3
    sources, targets, held = refs[:count], refs[count : 2 * count], refs[2 * count : 3 * count]
    sem_in, sem_out = refs[-2:]
    moves = []
    for source, target, place in zip(sources, targets, held):
        rows = source.shape[0]
        pieces = 4 if rows * source.shape[1] > 200_000 else 1
        for i in range(pieces):
            part = pl.ds(i * (rows // pieces), rows // pieces)
            k = len(moves)
            moves.append(
                (
                    pltpu.make_async_copy(source.at[part], place.at[part], sem_in.at[k]),
                    pltpu.make_async_copy(place.at[part], target.at[part], sem_out.at[k]),
                )
            )
    for load, _ in moves:
        load.start()
    for load, store in moves:
        load.wait()
        store.start()
    for _, store in moves:
        store.wait()


def solution(mesh):
    n_seq, n_tp = mesh.shape["seq"], mesh.shape["tp"]

    def shards(
        inner_x,
        gate_z,
        proj_bc,
        dt_raw,
        a_log,
        dt_bias,
        d_skip,
        conv_x,
        bias_x,
        conv_bc,
        bias_bc,
        norm_gain,
        w_out,
        d_out,
    ):
        rows, ch = inner_x.shape
        heads = a_log.shape[0]
        ns2 = proj_bc.shape[1]
        ns = ns2 // 2
        nc = rows // Q
        nrow = ns // n_seq
        wrows, drows = w_out.shape[1], d_out.shape[1]
        w_t = w_out.T
        d_t = d_out.T.reshape(2, drows // 2, rows)

        big = pltpu.VMEM((rows, ch), F32)
        chunk_states = pltpu.VMEM((nc, ns, ch), F32)
        slices = pltpu.VMEM((n_seq, nrow, ch), F32)
        sem_s = pltpu.SemaphoreType.DMA((2, n_seq))
        sem_t = pltpu.SemaphoreType.DMA((2, n_tp))
        scratch = [
            pltpu.VMEM((drows, rows), BF16),
            big,
            big,
            pltpu.VMEM((rows, ns2), F32),
            pltpu.VMEM((heads, rows), F32),
            pltpu.VMEM((wrows, ch), F32),
            pltpu.VMEM((rows, ch), BF16),
            pltpu.VMEM((rows, ch), BF16),
            pltpu.VMEM((rows, ns2), BF16),
            pltpu.VMEM((heads, rows), BF16),
            pltpu.VMEM((4, ch), F32),
            pltpu.VMEM((ch // LANES, LANES), F32),
            pltpu.VMEM((4, ns2), F32),
            pltpu.VMEM((1, ns2), F32),
            pltpu.VMEM((ch // LANES, LANES), F32),
            pltpu.VMEM((1, heads), F32),
            pltpu.VMEM((1, heads), F32),
            pltpu.VMEM((1, heads), F32),
            pltpu.VMEM((4, 4, wrows, ch), BF16),
            pltpu.VMEM((4, 4, wrows, rows), BF16),
            pltpu.VMEM((16, ch), BF16),
            pltpu.VMEM((16, ns2), BF16),
            pltpu.VMEM((8, LANES), F32),
            pltpu.VMEM((n_seq, 8, LANES), F32),
            big,
            big,
            pltpu.VMEM((nc, heads, Q), F32),
            big,
            big,
            pltpu.VMEM((rows, ns2), F32),
            pltpu.VMEM((rows, ns2), F32),
            chunk_states,
            chunk_states,
            chunk_states,
            big,
            big,
            big,
            big,
            pltpu.VMEM((rows, ch), BF16),
            pltpu.VMEM((rows + 8, ch), F32),
            pltpu.VMEM((rows + 8, ns2), F32),
            pltpu.VMEM((ns, ch), F32),
            slices,
            slices,
            slices,
            slices,
            slices,
            slices,
            slices,
            slices,
            pltpu.VMEM((2, 8, rows), F32),
            pltpu.VMEM((2, n_tp, 8, rows), F32),
            pltpu.VMEM((4, 2, drows, rows), BF16),
            pltpu.VMEM((4, drows, rows), BF16),
            pltpu.VMEM((drows, rows), BF16),
            pltpu.VMEM((2, drows, rows), BF16),
            pltpu.VMEM((4, 4, wrows, ch), BF16),
            *[
                pltpu.VMEM(shape, BF16)
                for shape in 2
                * [
                    (4, wrows // 2, ch),
                    (2, 4, wrows // 2, ch),
                    (wrows // 2, ch),
                    (2, wrows // 2, ch),
                ]
            ],
            pltpu.VMEM((nc, 4, 2, Q // n_tp, ns2), F32),
            pltpu.VMEM((nc, 4, Q // n_tp, ns2), F32),
            pltpu.VMEM((nc, 4, Q // n_tp, ns2), F32),
            chunk_states,
            pltpu.VMEM((n_tp, nc, Q // n_tp, ns2), BF16),
            pltpu.VMEM((Q, LANES), F32),
            pltpu.VMEM((LANES, Q), F32),
            pltpu.VMEM((Q, Q), F32),
            pltpu.VMEM((rows, 1), F32),
            pltpu.VMEM((nc, Q, LANES), F32),
            pltpu.VMEM((rows, ns2), F32),
            pltpu.VMEM((8, ns2), F32),
            pltpu.VMEM((nc, 8, ch), F32),
            pltpu.VMEM((rows, LANES), BF16),
            pltpu.SemaphoreType.DMA((2, nc)),
            pltpu.SemaphoreType.DMA((n_tp,)),
            pltpu.SemaphoreType.DMA((20,)),
            pltpu.SemaphoreType.DMA((2, 4)),
            sem_s,
            pltpu.SemaphoreType.DMA((2, 32)),
            sem_t,
            sem_s,
            sem_s,
            sem_s,
            sem_s,
            pltpu.SemaphoreType.DMA((2, 2 * n_tp)),
            sem_t,
            pltpu.SemaphoreType.DMA((2, 24)),
            pltpu.SemaphoreType.DMA((2, nc * n_tp)),
            pltpu.SemaphoreType.DMA((2, nc * n_tp)),
        ]
        out_t, g_x, g_z, g_bc, g_dt, g_w = pl.pallas_call(
            functools.partial(kernel, (n_seq, n_tp, ch * n_tp)),
            out_shape=[
                jax.ShapeDtypeStruct((drows, rows), BF16),
                jax.ShapeDtypeStruct((rows, ch), F32),
                jax.ShapeDtypeStruct((rows, ch), F32),
                jax.ShapeDtypeStruct((rows, ns2), F32),
                jax.ShapeDtypeStruct((heads, rows), F32),
                jax.ShapeDtypeStruct((wrows, ch), F32),
            ],
            in_specs=[pl.BlockSpec(memory_space=pltpu.HBM)] * 14,
            out_specs=[pl.BlockSpec(memory_space=pltpu.HBM)] * 6,
            scratch_shapes=scratch,
            compiler_params=pltpu.CompilerParams(
                collective_id=0, has_side_effects=True, vmem_limit_bytes=62 * 1024 * 1024
            ),
            name="mixer",
        )(
            inner_x,
            gate_z,
            proj_bc,
            dt_raw.T,
            w_t,
            d_t,
            conv_x,
            bias_x.reshape(-1, LANES),
            conv_bc,
            bias_bc[None, :],
            norm_gain.reshape(-1, LANES),
            a_log[None, :],
            dt_bias[None, :],
            d_skip[None, :],
        )
        results = (g_x, g_z, g_bc, g_w, out_t, g_dt)
        hbm = pl.BlockSpec(memory_space=pltpu.HBM)
        g_x, g_z, g_bc, g_w, out_t, g_dt = pl.pallas_call(
            publish,
            out_shape=[jax.ShapeDtypeStruct(v.shape, v.dtype) for v in results],
            in_specs=[hbm] * 6,
            out_specs=[hbm] * 6,
            scratch_shapes=[pltpu.VMEM(v.shape, v.dtype) for v in results]
            + [pltpu.SemaphoreType.DMA((16,)), pltpu.SemaphoreType.DMA((16,))],
            compiler_params=pltpu.CompilerParams(vmem_limit_bytes=62 * 1024 * 1024),
            name="publish",
        )(*results)
        return out_t.T, g_x, g_z, g_bc, g_dt.T, g_w.T

    in_specs = (
        P("seq", "tp"),
        P("seq", "tp"),
        P("seq", None),
        P("seq", "tp"),
        P("tp"),
        P("tp"),
        P("tp"),
        P(None, "tp"),
        P("tp"),
        P(),
        P(),
        P("tp"),
        P("tp", "seq"),
        P("seq", "tp"),
    )
    out_specs = (
        P("seq", "tp"),
        P("seq", "tp"),
        P("seq", "tp"),
        P("seq", None),
        P("seq", "tp"),
        P("tp", "seq"),
    )
    return jax.shard_map(
        shards, mesh=mesh, in_specs=in_specs, out_specs=out_specs, check_vma=False
    )
```
